128 devices in a mesh: dp: 4 (over x_lo, core), ctx: 32 (over x_hi, y, z).
Axes of the slice: x: 4 (x_hi: 2, x_lo: 2; x = x_hi * 2 + x_lo), y: 4, z: 4, core: 2. Of those that a mesh axis runs over, the one named last changes fastest.
Arguments:
- tokens: bfloat16 [4, 16384, 2048], P('dp', 'ctx'), may hold values from -6 to 6
- in_weight: bfloat16 [2048, 5120], P(None, 'dp'), may hold values from -0.125 to 0.125
- step_weight: bfloat16 [2048, 64], replicated, may hold values from -0.125 to 0.125
- step_bias: float32 [64], replicated, may hold values from -3 to 0
- decay_rate: float32 [64], replicated, may hold values from 0.0001 to 0.5
- skip_gain: float32 [64], replicated, may hold values from 0.5 to 1.5
- filter_taps: float32 [4, 5120], replicated, may hold values from -3 to 3
- filter_bias: float32 [5120], replicated, may hold values from -3 to 3
- norm_gain: float32 [4096], replicated, may hold values from 0.5 to 1.5
Outputs:
- normed: bfloat16 [4, 16384, 4096], P('dp', 'ctx')
The draws below stay inside these ranges and needn't reach their ends.
All inputs are finite; a program needn't handle non-finite values.
Results may differ from the reference program's by a relative error of at most 0.0061.
Values may be sent and summed in bfloat16 or wider, within the bound.
A program may use at most 192 MiB of HBM per device.

```python
import math
import jax
import jax.numpy as jnp
from jax import lax

D = 2048
HEADS = 64
HEAD_DIM = 64
STATE = 128
GROUPS = 4
BLOCK = 256
CONV_K = 4
BATCH = 4
SEQLEN = 16384
XBC = 5120


def steps_of(rng, dims, shards, low, largest):
    level, own = 1.0, jax.random.fold_in(rng, 6)
    for axis_at, shards_of in shards:
        steps = jnp.exp(jax.random.uniform(jax.random.fold_in(own, axis_at), (shards_of,), jnp.float32, low / len(shards), largest / len(shards)))
        level = level * jnp.repeat(steps, dims[axis_at] // shards_of).reshape([-1 if axis == axis_at else 1 for axis in range(len(dims))])
    return level


def bell_draw(key, extent, scale, bound, shards=(), held_as=jnp.bfloat16):
    values = scale * jax.random.normal(key, extent, jnp.float32)
    if shards:
        values = values * steps_of(key, extent, shards, -0.22, 0.18)
    return jnp.clip(values, -bound, bound).astype(held_as)


def setup_inputs(seed: int = 0) -> dict:
    streams_of = jax.random.split(jax.random.key(seed), 10)
    return {
        "tokens": bell_draw(streams_of[0], (BATCH, SEQLEN, D), 1.0, 6.0, ((0, 4), (1, 32))),
        "in_weight": bell_draw(streams_of[1], (D, XBC), D ** -0.5, 0.125, ((1, 4),)),
        "step_weight": bell_draw(streams_of[2], (D, HEADS), D ** -0.5, 0.125),
        "step_bias": jnp.clip(jax.random.uniform(streams_of[3], (HEADS,), jnp.float32, -3.0, 0.0), -3.0, 0.0),
        "decay_rate": jnp.clip(jnp.exp(jax.random.uniform(streams_of[4], (HEADS,), jnp.float32, math.log(0.0001), math.log(0.5))), 0.0001, 0.5),
        "skip_gain": jnp.clip(jax.random.uniform(streams_of[5], (HEADS,), jnp.float32, 0.5, 1.5), 0.5, 1.5),
        "filter_taps": bell_draw(streams_of[6], (CONV_K, XBC), CONV_K ** -0.5, 3.0, (), jnp.float32),
        "filter_bias": bell_draw(streams_of[7], (XBC,), 0.5, 3.0, (), jnp.float32),
        "norm_gain": jnp.clip(jax.random.uniform(streams_of[8], (HEADS * HEAD_DIM,), jnp.float32, 0.5, 1.5), 0.5, 1.5),
    }


def filter_rows(prefix, current, filter_taps, filter_bias):
    padded = jnp.concatenate([prefix, current], axis=0).astype(jnp.float32)
    length = current.shape[0]
    summed = filter_bias + filter_taps[0] * padded[0:length]
    for offset in range(1, filter_taps.shape[0]):
        summed = summed + filter_taps[offset] * padded[offset:offset + length]
    return summed

def ssd_group(values, input_map, output_map, step_size, decay_rate, skip_gain, block_len):
    length, head_count, head_width = values.shape
    block_count = length // block_len
    bundle = math.gcd(block_count, 8)
    bundle_count = block_count // bundle
    highest = lax.Precision.HIGHEST
    value_rows = values.reshape(block_count, block_len, head_count, head_width)
    input_rows = input_map.reshape(block_count, block_len, -1)
    output_rows = output_map.reshape(block_count, block_len, -1)
    step_rows = step_size.reshape(block_count, block_len, head_count)
    decay_sum = jnp.cumsum(-step_rows * decay_rate, axis=1)
    causal = (jnp.arange(block_len)[:, None] >= jnp.arange(block_len)[None, :])[None, :, :, None]

    def local_block(pieces):
        value_block, input_block, output_block, step_block, decay_block = pieces
        value_wide = value_block.astype(jnp.float32)
        input_wide = input_block.astype(jnp.float32)
        scores = jnp.einsum('ktn,kun->ktu', output_block.astype(jnp.float32), input_wide, precision=highest)
        decay_gap = jnp.where(causal, decay_block[:, :, None, :] - decay_block[:, None, :, :], 0.0)
        weights = jnp.where(causal, jnp.exp(decay_gap), 0.0) * scores[..., None] * step_block[:, None, :, :]
        weights = weights.astype(jnp.bfloat16).astype(jnp.float32)
        within = jnp.einsum('ktuh,kuhp->kthp', weights, value_wide, precision=highest)
        to_end = jnp.exp(decay_block[:, -1:, :] - decay_block) * step_block
        scaled = (to_end[..., None] * value_wide).astype(jnp.bfloat16).astype(jnp.float32)
        states = jnp.einsum('kuhp,kun->khpn', scaled, input_wide, precision=highest)
        return (within, states)

    def blocked(array):
        return array.reshape((bundle_count, bundle) + array.shape[1:])
    within, states = lax.map(local_block, (blocked(value_rows), blocked(input_rows), blocked(output_rows), blocked(step_rows), blocked(decay_sum)))
    within = within.reshape(block_count, block_len, head_count, head_width)
    states = states.reshape((block_count,) + states.shape[2:])
    totals = decay_sum[:, -1, :]
    running = jnp.cumsum(totals, axis=0)
    starts = running - totals
    before = (jnp.arange(block_count)[:, None] > jnp.arange(block_count)[None, :])[:, :, None]
    mixing = jnp.where(before, jnp.exp(jnp.where(before, starts[:, None, :] - running[None, :, :], 0.0)), 0.0)
    entering = jnp.einsum('kjh,jhpn->khpn', mixing, states, precision=highest)
    carried = jnp.einsum('khpn,ktn->kthp', entering, output_rows.astype(jnp.float32), precision=highest) * jnp.exp(decay_sum)[..., None]
    output = within + carried + skip_gain[:, None] * value_rows.astype(jnp.float32)
    return output.reshape(length, head_count, head_width)

def group_norm(values, norm_gain):
    length = values.shape[0]
    grouped = values.astype(jnp.float32).reshape(length, GROUPS, -1)
    mean_square = lax.optimization_barrier(jnp.mean(jnp.square(grouped), axis=-1, keepdims=True))
    return (grouped * lax.rsqrt(mean_square + 1e-05)).reshape(length, -1) * norm_gain

def reference(tokens, in_weight, step_weight, step_bias, decay_rate, skip_gain, filter_taps, filter_bias, norm_gain):
    inner_width = HEADS * HEAD_DIM
    map_width = GROUPS * STATE
    group_heads = HEADS // GROUPS
    results = []
    for member in range(BATCH):
        token_rows = tokens[member]
        projected = jnp.dot(token_rows, in_weight, preferred_element_type=jnp.float32).astype(jnp.bfloat16)
        step_raw = jnp.dot(token_rows, step_weight, preferred_element_type=jnp.float32).astype(jnp.bfloat16)
        prefix = jnp.zeros((CONV_K - 1, projected.shape[1]), jnp.bfloat16)
        active = jax.nn.silu(filter_rows(prefix, projected, filter_taps, filter_bias)).astype(jnp.bfloat16)
        step_size = jax.nn.softplus(step_raw.astype(jnp.float32) + step_bias)
        inputs = active[:, :inner_width].reshape(SEQLEN, HEADS, HEAD_DIM)
        outputs = []
        for group_index in range(GROUPS):
            heads_here = slice(group_index * group_heads, (group_index + 1) * group_heads)
            first_in = inner_width + group_index * STATE
            first_out = inner_width + map_width + group_index * STATE
            outputs.append(ssd_group(inputs[:, heads_here], active[:, first_in:first_in + STATE], active[:, first_out:first_out + STATE], step_size[:, heads_here], decay_rate[heads_here], skip_gain[heads_here], BLOCK))
        mixed_rows = jnp.concatenate(outputs, axis=1).reshape(SEQLEN, inner_width).astype(jnp.bfloat16)
        results.append(group_norm(mixed_rows, norm_gain).astype(jnp.bfloat16))
    return jnp.stack(results)
```

```python
import functools

import jax
import jax.numpy as jnp
from jax import lax
from jax.experimental import pallas as pl
from jax.experimental.pallas import tpu as pltpu
from jax.sharding import PartitionSpec as P

D = 2048
HEADS = 64
HEAD_DIM = 64
STATE = 128
GROUPS = 4
BLOCK = 256
ROWS = 512
HALO = 16
SHARD = 1280
XBC = 5120
INNER = 4096
LOG2E = 1.4426950408889634
MESH = pl.DeviceIdType.MESH
F32 = jnp.float32
BF16 = jnp.bfloat16

RING_COL = ((0, 4, 1, 5), (2, 6, 3, 7))
SAME_SLOT = (10, 11, 14, 15, 16)
OTHER_SLOT = (12, 13, 17, 18, 19)


def same_slot(column):
    return 2 * SAME_SLOT[column // 2] + column % 2


def other_slot(column):
    return 2 * OTHER_SLOT[column // 2] + column % 2


def project_kernel(
    tok_ref, w_ref, sw_ref, small_ref, taps_ref, fb_ref,
    act_ref, a_ref, bt_ref, lt_ref, w2_ref, e2_ref, misc_ref,
    tok, wbuf, pbuf, abuf, swp,
    loc_sem, tok_sem, act_sem, halo_sem, sib_send, sib_recv,
    x_send, x_recv, ring_send, ring_recv, fwd_send, fwd_recv,
):
    dp = lax.axis_index("dp")
    ctx = lax.axis_index("ctx")
    z = ctx % 4
    y = (ctx // 4) % 4
    xh = ctx // 16
    sibling = dp + 1 - 2 * (dp % 2)
    across = (dp + 2) % 4
    place = (z, y)

    def along(dim, step):
        if dim == 0:
            return xh * 16 + y * 4 + (z + step) % 4
        return xh * 16 + ((y + step) % 4) * 4 + z

    source_a = (across, ctx)
    source_b = (across, (ctx + 16) % 32)
    after = (dp, (ctx + 1) % 32)
    before = (dp, (ctx + 31) % 32)

    tok_copy = pltpu.make_async_copy(tok_ref.at[0], tok.at[HALO:], tok_sem)
    tok_copy.start()

    def loc_copy(j):
        return pltpu.make_async_copy(
            w_ref.at[:, j * 128 : (j + 1) * 128], wbuf.at[j], loc_sem.at[j]
        )

    barrier = pltpu.get_barrier_semaphore()
    for peer in (
        (sibling, ctx), source_a, source_b, after, before,
        (dp, along(0, 1)), (dp, along(0, 3)), (dp, along(1, 1)), (dp, along(1, 3)),
    ):
        pl.semaphore_signal(barrier, inc=1, device_id=peer, device_id_type=MESH)
    for j in range(4):
        loc_copy(j).start()
    pl.semaphore_wait(barrier, 9)

    def remote(src, dst, send, recv, peer):
        return pltpu.make_async_remote_copy(
            src_ref=src, dst_ref=dst, send_sem=send, recv_sem=recv,
            device_id=peer, device_id_type=MESH,
        )

    def x_piece(dim, p):
        column = RING_COL[dim][p]
        rows = pl.ds(pl.multiple_of(place[dim] * 512, 512), 512)
        peer = source_a if p < 2 else source_b
        return remote(
            w_ref.at[rows, column * 128 : (column + 1) * 128],
            wbuf.at[same_slot(column), rows],
            x_send.at[dim * 4 + p], x_recv.at[dim * 4 + p], peer,
        )

    def x_direct(k):
        column = 8 + k
        return remote(
            w_ref.at[:, column * 128 : (column + 1) * 128],
            wbuf.at[same_slot(column)],
            x_send.at[8 + k], x_recv.at[8 + k], (source_a, source_b)[k],
        )

    def ring_rows(dim, kind, p):
        back = (3, 1, 2)[kind]
        return pl.ds(pl.multiple_of(((place[dim] + back) % 4) * 512, 512), 512)

    def ring_out(dim, kind, p):
        column = RING_COL[dim][p]
        if kind == 0:
            rows, peer = pl.ds(pl.multiple_of(place[dim] * 512, 512), 512), along(dim, 1)
        elif kind == 1:
            rows, peer = pl.ds(pl.multiple_of(place[dim] * 512, 512), 512), along(dim, 3)
        elif p < 2:
            rows, peer = ring_rows(dim, 0, p), along(dim, 1)
        else:
            rows, peer = ring_rows(dim, 1, p), along(dim, 3)
        at = wbuf.at[same_slot(column), rows]
        index = dim * 12 + kind * 4 + p
        return remote(at, at, ring_send.at[index], ring_recv.at[index], (dp, peer))

    def ring_in(dim, kind, p):
        column = RING_COL[dim][p]
        at = wbuf.at[same_slot(column), ring_rows(dim, kind, p)]
        index = dim * 12 + kind * 4 + p
        return remote(at, at, ring_send.at[index], ring_recv.at[index], (dp, along(dim, 1)))

    def forward(index):
        if index in (8, 9):
            src, dst = wbuf.at[same_slot(index)], wbuf.at[other_slot(index)]
        else:
            if index < 8:
                dim, p = divmod(index, 4)
                rows = pl.ds(pl.multiple_of(place[dim] * 512, 512), 512)
            else:
                dim, rest = divmod(index - 10, 12)
                kind, p = divmod(rest, 4)
                rows = ring_rows(dim, kind, p)
            column = RING_COL[dim][p]
            src = wbuf.at[same_slot(column), rows]
            dst = wbuf.at[other_slot(column), rows]
        return remote(src, dst, fwd_send.at[index], fwd_recv.at[index], (sibling, ctx))

    def sib_copy(j):
        return remote(
            w_ref.at[:, j * 128 : (j + 1) * 128], wbuf.at[10 + j],
            sib_send.at[j], sib_recv.at[j], (sibling, ctx),
        )

    halo_copy = remote(
        tok_ref.at[0, ROWS - HALO :], tok.at[:HALO], halo_sem.at[0], halo_sem.at[1], after
    )
    halo_copy.start()
    for p, q in ((0, 2), (1, 3)):
        x_piece(0, p).start()
        x_piece(1, q).start()
        x_piece(1, p).start()
        x_piece(0, q).start()
    x_direct(0).start()
    x_direct(1).start()
    for j in range(4, 10):
        loc_copy(j).start()
    for j in range(10):
        sib_copy(j).start()

    swp[...] = jnp.zeros_like(swp)
    swp[:, 0:HEADS] = sw_ref[...]
    tok_copy.wait()
    step_raw = jnp.dot(tok[HALO:], swp[...], preferred_element_type=F32)
    step_raw = step_raw.astype(BF16).astype(F32) + small_ref[0:1]
    step = jnp.maximum(step_raw, 0.0) + jnp.log1p(jnp.exp(-jnp.abs(step_raw)))
    keep = lax.broadcasted_iota(jnp.int32, (ROWS, 128), 1) < HEADS
    step = jnp.where(keep, step, 0.0)
    fall = step * (small_ref[1:2] * (-LOG2E))
    lower = (
        lax.broadcasted_iota(jnp.int32, (BLOCK, BLOCK), 0)
        >= lax.broadcasted_iota(jnp.int32, (BLOCK, BLOCK), 1)
    ).astype(F32)
    level = jnp.log2(step)

    def halves(value):
        high = value.astype(BF16).astype(F32)
        low = (value - high).astype(BF16).astype(F32)
        return (high + pltpu.roll(low, 64, 1)).astype(BF16)

    ends = []
    for k in range(2):
        at = slice(k * BLOCK, (k + 1) * BLOCK)
        a = jnp.dot(
            lower, fall[at], precision=lax.Precision.HIGHEST, preferred_element_type=F32
        )
        end = a[BLOCK - 1 : BLOCK]
        ends.append(end)
        weight = jnp.where(keep[at], jnp.exp2(end - a) * step[at], 0.0)
        w2_ref[at] = halves(weight)
        e2_ref[at] = halves(jnp.where(keep[at], jnp.exp2(a), 0.0))
        for g in range(GROUPS):
            a_ref[g, at] = a if g == 0 else pltpu.roll(a, 128 - 16 * g, 1)
        bt_ref[:, at] = jnp.transpose(level[at] - a)
        lt_ref[:, at] = jnp.transpose(level[at])
    row = lax.broadcasted_iota(jnp.int32, (8, 128), 0)
    lane_ok = lax.broadcasted_iota(jnp.int32, (8, 128), 1) < HEADS
    exponent = jnp.where(row == 0, ends[0], jnp.where(row == 1, ends[1], ends[0] + ends[1]))
    rows_of = jnp.where(row == 3, small_ref[2:3], jnp.exp2(exponent))
    misc_ref[...] = halves(jnp.where(lane_ok, rows_of, 0.0))

    halo_copy.wait_recv()

    @pl.when(ctx == 0)
    def _():
        tok[:HALO] = jnp.zeros((HALO, D), BF16)

    def x_arrive(dim, p):
        x_piece(dim, p).wait_recv()
        ring_out(dim, 0, p).start()
        ring_out(dim, 1, p).start()
        forward(dim * 4 + p).start()

    def near_arrive(dim, kind, p):
        ring_in(dim, kind, p).wait_recv()
        if (kind == 0) == (p < 2):
            ring_out(dim, 2, p).start()
        forward(10 + dim * 12 + kind * 4 + p).start()

    def far_arrive(dim, p):
        ring_in(dim, 2, p).wait_recv()
        forward(10 + dim * 12 + 8 + p).start()

    def direct_arrive(k):
        x_direct(k).wait_recv()
        forward(8 + k).start()

    def other_wait(pieces):
        for dim, p in pieces:
            forward(dim * 4 + p).wait_recv()
            for kind in range(3):
                forward(10 + dim * 12 + kind * 4 + p).wait_recv()

    first = ((0, 0), (1, 2), (1, 0), (0, 2))
    second = ((0, 1), (1, 3), (1, 1), (0, 3))

    def events(i):
        for j in range(5):
            @pl.when(i == j)
            def _(j=j):
                loc_copy(2 * j).wait()
                loc_copy(2 * j + 1).wait()

            @pl.when(i == 5 + j)
            def _(j=j):
                sib_copy(2 * j).wait_recv()
                sib_copy(2 * j + 1).wait_recv()

        @pl.when(i == 2)
        def _():
            x_arrive(*first[0])
            x_arrive(*first[1])

        @pl.when(i == 5)
        def _():
            x_arrive(*first[2])
            x_arrive(*first[3])

        @pl.when(i == 7)
        def _():
            for piece in first[:2]:
                near_arrive(piece[0], 0, piece[1])
                near_arrive(piece[0], 1, piece[1])
            x_arrive(*second[0])
            x_arrive(*second[1])

        @pl.when(i == 9)
        def _():
            for piece in first[2:]:
                near_arrive(piece[0], 0, piece[1])
                near_arrive(piece[0], 1, piece[1])
            x_arrive(*second[2])
            x_arrive(*second[3])

        @pl.when(i == 10)
        def _():
            for piece in first:
                far_arrive(*piece)

        @pl.when(i == 11)
        def _():
            for piece in second[:2]:
                near_arrive(piece[0], 0, piece[1])
                near_arrive(piece[0], 1, piece[1])

        @pl.when(i == 12)
        def _():
            other_wait(((0, 0), (0, 2)))

        @pl.when(i == 13)
        def _():
            other_wait(((1, 0), (1, 2)))
            for piece in second[2:]:
                near_arrive(piece[0], 0, piece[1])
                near_arrive(piece[0], 1, piece[1])

        @pl.when(i == 14)
        def _():
            for piece in second:
                far_arrive(*piece)

        @pl.when(i == 15)
        def _():
            direct_arrive(0)
            direct_arrive(1)

        @pl.when(i == 17)
        def _():
            other_wait(((0, 1), (0, 3)))

        @pl.when(i == 18)
        def _():
            other_wait(((1, 1), (1, 3)))

        @pl.when(i == 19)
        def _():
            forward(8).wait_recv()
            forward(9).wait_recv()

    def column_of(i):
        m = i - 10
        foreign = i // 10
        late = (i - 6) // 8 * foreign
        kind = foreign * (2 + (1 - late) * ((m % 4) // 2) + late * ((i - 14 + 30) // 3 - 10))
        near_kind = (1 - foreign) * (i // 5)
        pair = (1 - foreign) * (i % 5) + foreign * (
            (1 - late) * (m % 2) + late * (2 + (i - 14 + 30) % 3)
        )
        relation = kind + near_kind
        lo = (dp + relation) % 2
        hi = (dp // 2 + relation // 2) % 2
        return (2 * hi + lo) * SHARD + pair * 256

    def act_copy(i):
        columns = pl.ds(pl.multiple_of(column_of(i), 256), 256)
        return pltpu.make_async_copy(abuf.at[i], act_ref.at[:, columns], act_sem)

    @pl.loop(0, 20)
    def _(i):
        events(i)
        weights = jnp.concatenate([wbuf[2 * i], wbuf[2 * i + 1]], axis=1)
        pbuf[...] = (
            jnp.dot(tok[...], weights, preferred_element_type=F32).astype(BF16).astype(F32)
        )
        columns = pl.ds(pl.multiple_of(column_of(i), 256), 256)
        taps = taps_ref[:, columns]
        summed = fb_ref[:, columns] + taps[0:1] * pbuf[HALO - 3 : HALO - 3 + ROWS]
        for k in range(1, 4):
            summed = summed + taps[k : k + 1] * pbuf[HALO - 3 + k : HALO - 3 + k + ROWS]
        abuf[i] = (summed / (1.0 + jnp.exp(-summed))).astype(BF16)
        act_copy(i).start()

    halo_copy.wait_send()
    for dim in range(2):
        for p in range(4):
            x_piece(dim, p).wait_send()
            for kind in range(3):
                ring_out(dim, kind, p).wait_send()
    for k in range(2):
        x_direct(k).wait_send()
    for j in range(10):
        sib_copy(j).wait_send()
    for index in range(34):
        forward(index).wait_send()
    pltpu.make_async_copy(abuf, abuf, act_sem).wait()


def project(tokens, in_weight, step_weight, small, filter_taps, filter_bias):
    vmem = pl.BlockSpec(memory_space=pltpu.VMEM)
    anywhere = pl.BlockSpec(memory_space=pl.ANY)
    dma = pltpu.SemaphoreType.DMA
    return pl.pallas_call(
        project_kernel,
        out_shape=(
            jax.ShapeDtypeStruct((ROWS, XBC), BF16),
            jax.ShapeDtypeStruct((GROUPS, ROWS, 128), F32),
            jax.ShapeDtypeStruct((128, ROWS), F32),
            jax.ShapeDtypeStruct((128, ROWS), F32),
            jax.ShapeDtypeStruct((ROWS, 128), BF16),
            jax.ShapeDtypeStruct((ROWS, 128), BF16),
            jax.ShapeDtypeStruct((8, 128), BF16),
        ),
        in_specs=[anywhere, anywhere, vmem, vmem, vmem, vmem],
        out_specs=(anywhere,) + (vmem,) * 6,
        scratch_shapes=[
            pltpu.VMEM((HALO + ROWS, D), BF16),
            pltpu.VMEM((40, D, 128), BF16),
            pltpu.VMEM((HALO + ROWS, 256), F32),
            pltpu.VMEM((20, ROWS, 256), BF16),
            pltpu.VMEM((D, 128), BF16),
            dma((10,)), dma, dma, dma((2,)), dma((10,)), dma((10,)),
            dma((10,)), dma((10,)), dma((24,)), dma((24,)), dma((34,)), dma((34,)),
        ],
        compiler_params=pltpu.CompilerParams(
            collective_id=0, has_side_effects=True, vmem_limit_bytes=56 * 2**20
        ),
        name="project",
    )(tokens, in_weight, step_weight, small, filter_taps, filter_bias)


def mix_kernel(
    act_ref, a_ref, bt_ref, lt_ref, w2_ref, e2_ref, misc_ref, gain_ref,
    out_ref,
    spread, first, mix, scores, state_out, decay_out, state_in, decay_in, enter_out, enter_in,
    sems,
):
    dp = lax.axis_index("dp")
    me = lax.axis_index("ctx")
    barrier = pltpu.get_barrier_semaphore()

    @pl.loop(1, 32)
    def _(r):
        pl.semaphore_signal(
            barrier, inc=1, device_id=(dp, (me + r) % 32), device_id_type=MESH
        )

    head_row = lax.broadcasted_iota(jnp.int32, (128, 1024), 0) % HEADS
    head_lane = lax.broadcasted_iota(jnp.int32, (128, 1024), 1) // HEAD_DIM
    for g in range(GROUPS):
        spread[g] = (head_row == head_lane + 16 * g).astype(F32).astype(BF16)

    def widen(value, g):
        return jnp.dot(value, spread[g], preferred_element_type=F32)

    def columns(start, size):
        return pl.ds(pl.multiple_of(start, 128), size)

    @pl.loop(0, GROUPS)
    def _(g):
        decays = widen(misc_ref[...], g)
        total = None
        for k in range(2):
            at = slice(k * BLOCK, (k + 1) * BLOCK)
            values = act_ref[at, columns(g * 1024, 1024)].astype(F32)
            scaled = (widen(w2_ref[at], g) * values).astype(BF16)
            maps = act_ref[at, columns(INNER + g * STATE, STATE)]
            state = lax.dot_general(
                maps, scaled, (((0,), (0,)), ((), ())), preferred_element_type=F32
            )
            if k == 0:
                first[g] = state
                total = decays[1:2] * state
            else:
                total = total + state
        for i in range(8):
            lanes = slice(i * 128, (i + 1) * 128)
            state_out[g * 8 + i] = total[:, lanes].astype(BF16)
            decay_out[g * 8 + i] = jnp.broadcast_to(decays[2:3, lanes], (8, 128))

    def send(r, src, dst, pair):
        peer = (me + r) % 32
        return pltpu.make_async_remote_copy(
            src_ref=src.at[peer], dst_ref=dst.at[me],
            send_sem=sems.at[pair], recv_sem=sems.at[pair + 1],
            device_id=(dp, peer), device_id_type=MESH,
        )

    def wait_all(buffer, index):
        part = buffer.at[0:31]
        pltpu.make_async_copy(part, part, sems.at[index]).wait()

    pl.semaphore_wait(barrier, 31)

    @pl.loop(1, 32)
    def _(r):
        send(r, decay_out, decay_in, 2).start()
        send(r, state_out, state_in, 0).start()

    state_in[me] = state_out[me]
    decay_in[me] = decay_out[me]

    lane = lax.broadcasted_iota(jnp.int32, (BLOCK, 128), 1) < HEAD_DIM
    causal = lax.broadcasted_iota(jnp.int32, (128, 128), 0) >= lax.broadcasted_iota(
        jnp.int32, (128, 128), 1
    )

    def within(n):
        g = n // 2
        start = (n % 2) * BLOCK
        rows = pl.ds(pl.multiple_of(start, BLOCK), BLOCK)
        read = act_ref[rows, columns(INNER + GROUPS * STATE + g * STATE, STATE)]
        write = act_ref[rows, columns(INNER + g * STATE, STATE)]
        full = lax.dot_general(
            read, write, (((1,), (1,)), ((), ())), preferred_element_type=F32
        )
        scores[0] = jnp.where(causal, full[:128, :128], 0.0)
        scores[1] = full[128:, :128]
        scores[2] = jnp.where(causal, full[128:, 128:], 0.0)
        skip = widen(misc_ref[...], g)[3:4]
        for i in range(8):
            lanes = columns(g * 1024 + i * 128, 128)
            values = act_ref[rows, lanes]
            made = []
            for h in (2 * i, 2 * i + 1):
                upper = a_ref[g, pl.ds(pl.multiple_of(start, BLOCK), 128), h : h + 1]
                under = a_ref[g, pl.ds(pl.multiple_of(start + 128, 128), 128), h : h + 1]
                b0 = bt_ref[g, h : h + 1, columns(start, 128)]
                b1 = bt_ref[g, h : h + 1, columns(start + 128, 128)]
                l0 = lt_ref[g, h : h + 1, columns(start, 128)]
                l1 = lt_ref[g, h : h + 1, columns(start + 128, 128)]
                w00 = (jnp.exp2(jnp.minimum(upper + b0, l0)) * scores[0]).astype(BF16)
                w10 = (jnp.exp2(under + b0) * scores[1]).astype(BF16)
                w11 = (jnp.exp2(jnp.minimum(under + b1, l1)) * scores[2]).astype(BF16)
                top = jnp.dot(w00, values[:128], preferred_element_type=F32)
                low = jnp.dot(
                    jnp.concatenate([w10, w11], axis=1), values, preferred_element_type=F32
                )
                made.append(jnp.concatenate([top, low], axis=0))
            mixed = jnp.where(lane, made[0], made[1])
            mix[rows, lanes] = mixed + skip[:, i * 128 : (i + 1) * 128] * values.astype(F32)

    pl.loop(0, 4)(within)

    wait_all(decay_in, 3)
    wait_all(state_in, 1)

    def scan(k, carry):
        enter_out[k] = carry.astype(BF16)
        return decay_in[k, 0:1] * carry + state_in[k].astype(F32)

    lax.fori_loop(0, 32, scan, jnp.zeros((STATE, 128), F32))

    @pl.loop(1, 32)
    def _(r):
        send(r, enter_out, enter_in, 4).start()

    enter_in[me] = enter_out[me]

    pl.loop(4, 8)(within)

    wait_all(enter_in, 5)

    @pl.loop(0, GROUPS)
    def _(g):
        decays = widen(misc_ref[...], g)
        enter = jnp.concatenate([enter_in[g * 8 + i] for i in range(8)], axis=1)
        for k in range(2):
            rows = slice(k * BLOCK, (k + 1) * BLOCK)
            if k == 1:
                enter = (decays[0:1] * enter.astype(F32) + first[g]).astype(BF16)
            read = act_ref[rows, columns(INNER + GROUPS * STATE + g * STATE, STATE)]
            carried = jnp.dot(read, enter, preferred_element_type=F32) * widen(e2_ref[rows], g)
            mixed = (mix[rows, columns(g * 1024, 1024)] + carried).astype(BF16).astype(F32)
            mean = jnp.mean(mixed * mixed, axis=1, keepdims=True)
            normed = mixed * lax.rsqrt(mean + 1e-05) * gain_ref[:, columns(g * 1024, 1024)]
            out_ref[rows, columns(g * 1024, 1024)] = normed.astype(BF16)

    wait_all(state_out, 0)
    wait_all(decay_out, 2)
    wait_all(enter_out, 4)


def mixer(act, a, bt, lt, w2, e2, misc, gain):
    vmem = pl.BlockSpec(memory_space=pltpu.VMEM)
    return pl.pallas_call(
        mix_kernel,
        out_shape=jax.ShapeDtypeStruct((ROWS, INNER), BF16),
        in_specs=[vmem] * 8,
        out_specs=vmem,
        scratch_shapes=[
            pltpu.VMEM((GROUPS, 128, 1024), BF16),
            pltpu.VMEM((GROUPS, STATE, 1024), F32),
            pltpu.VMEM((ROWS, INNER), F32),
            pltpu.VMEM((3, 128, 128), F32),
            pltpu.VMEM((32, STATE, 128), BF16),
            pltpu.VMEM((32, 8, 128), F32),
            pltpu.VMEM((32, STATE, 128), BF16),
            pltpu.VMEM((32, 8, 128), F32),
            pltpu.VMEM((32, STATE, 128), BF16),
            pltpu.VMEM((32, STATE, 128), BF16),
            pltpu.SemaphoreType.DMA((6,)),
        ],
        compiler_params=pltpu.CompilerParams(
            collective_id=1, has_side_effects=True, vmem_limit_bytes=56 * 2**20
        ),
        name="mixer",
    )(act, a, bt, lt, w2, e2, misc, gain)


def per_device(
    tokens,
    in_weight,
    step_weight,
    step_bias,
    decay_rate,
    skip_gain,
    filter_taps,
    filter_bias,
    norm_gain,
):
    small = jnp.zeros((8, 128), F32)
    small = small.at[0:3, 0:HEADS].set(jnp.stack([step_bias, decay_rate, skip_gain]))
    act, a, bt, lt, w2, e2, misc = project(
        tokens, in_weight, step_weight, small, filter_taps, filter_bias[None]
    )
    bt = bt.reshape(8, 16, ROWS)
    lt = lt.reshape(8, 16, ROWS)
    return mixer(act, a, bt, lt, w2, e2, misc, norm_gain[None])[None]


def solution(mesh):
    in_specs = (P("dp", "ctx", None), P(None, "dp"), P(), P(), P(), P(), P(), P(), P())
    out_specs = P("dp", "ctx", None)
    return jax.shard_map(
        per_device, mesh=mesh, in_specs=in_specs, out_specs=out_specs, check_vma=False
    )
```

```python
import functools

import jax
import jax.numpy as jnp
from jax import lax
from jax.experimental import pallas as pl
from jax.experimental.pallas import tpu as pltpu
from jax.sharding import PartitionSpec as P

D = 2048
HEADS = 64
HEAD_DIM = 64
STATE = 128
GROUPS = 4
BLOCK = 256
ROWS = 512
HALO = 16
SHARD = 1280
XBC = 5120
INNER = 4096
LOG2E = 1.4426950408889634
MESH = pl.DeviceIdType.MESH
F32 = jnp.float32
BF16 = jnp.bfloat16

RING_COL = ((0, 4, 1, 5), (2, 6, 3, 7))
SAME_SLOT = (10, 11, 14, 15, 16)
OTHER_SLOT = (12, 13, 17, 18, 19)
PEERS = 34


def same_slot(column):
    return 2 * SAME_SLOT[column // 2] + column % 2


def other_slot(column):
    return 2 * OTHER_SLOT[column // 2] + column % 2


def mixer_kernel(
    tok_ref, w_ref, sw_ref, bias_ref, rate_ref, skip_ref, taps_ref, fb_ref,
    out_ref,
    tok, wbuf, pbuf_a, pbuf_b, act, swp, small,
    a_ref, bt_ref, lt_ref, w2_ref, e2_ref, misc_ref,
    spread, first, mix, mixed_out, scores, totals, decays_in,
    state_out, state_in, enter_out, enter_in,
    loc_sem, tok_sem, out_sem, halo_sem, sib_send, sib_recv,
    x_send, x_recv, ring_send, ring_recv, fwd_send, fwd_recv, sems,
):
    dp = lax.axis_index("dp")
    ctx = lax.axis_index("ctx")
    z = ctx % 4
    y = (ctx // 4) % 4
    xh = ctx // 16
    sibling = dp + 1 - 2 * (dp % 2)
    across = (dp + 2) % 4
    place = (z, y)

    def along(dim, step):
        if dim == 0:
            return xh * 16 + y * 4 + (z + step) % 4
        return xh * 16 + ((y + step) % 4) * 4 + z

    source_a = (across, ctx)
    source_b = (across, (ctx + 16) % 32)
    after = (dp, (ctx + 1) % 32)

    def loc_copy(j):
        return pltpu.make_async_copy(
            w_ref.at[:, j * 128 : (j + 1) * 128], wbuf.at[j], loc_sem.at[j]
        )

    barrier = pltpu.get_barrier_semaphore()
    for peer in ((sibling, ctx), source_a, source_b):
        pl.semaphore_signal(barrier, inc=1, device_id=peer, device_id_type=MESH)

    @pl.loop(1, 32)
    def _(r):
        pl.semaphore_signal(
            barrier, inc=1, device_id=(dp, (ctx + r) % 32), device_id_type=MESH
        )

    tok_copy = pltpu.make_async_copy(tok_ref.at[0], tok.at[HALO:], tok_sem)
    tok_copy.start()
    for j in range(4):
        loc_copy(j).start()

    def remote(src, dst, send, recv, peer):
        return pltpu.make_async_remote_copy(
            src_ref=src, dst_ref=dst, send_sem=send, recv_sem=recv,
            device_id=peer, device_id_type=MESH,
        )

    def x_piece(dim, p):
        column = RING_COL[dim][p]
        rows = pl.ds(pl.multiple_of(place[dim] * 512, 512), 512)
        return remote(
            w_ref.at[rows, column * 128 : (column + 1) * 128],
            wbuf.at[same_slot(column), rows],
            x_send.at[dim * 4 + p], x_recv.at[dim * 4 + p],
            source_a if p < 2 else source_b,
        )

    def x_direct(k):
        column = 8 + k
        return remote(
            w_ref.at[:, column * 128 : (column + 1) * 128],
            wbuf.at[same_slot(column)],
            x_send.at[8 + k], x_recv.at[8 + k], (source_a, source_b)[k],
        )

    def ring_rows(dim, kind, p):
        back = (3, 1, 2)[kind]
        return pl.ds(pl.multiple_of(((place[dim] + back) % 4) * 512, 512), 512)

    def ring_out(dim, kind, p):
        column = RING_COL[dim][p]
        if kind == 0:
            rows, peer = pl.ds(pl.multiple_of(place[dim] * 512, 512), 512), along(dim, 1)
        elif kind == 1:
            rows, peer = pl.ds(pl.multiple_of(place[dim] * 512, 512), 512), along(dim, 3)
        elif p < 2:
            rows, peer = ring_rows(dim, 0, p), along(dim, 1)
        else:
            rows, peer = ring_rows(dim, 1, p), along(dim, 3)
        at = wbuf.at[same_slot(column), rows]
        index = dim * 12 + kind * 4 + p
        return remote(at, at, ring_send.at[index], ring_recv.at[index], (dp, peer))

    def ring_in(dim, kind, p):
        column = RING_COL[dim][p]
        at = wbuf.at[same_slot(column), ring_rows(dim, kind, p)]
        index = dim * 12 + kind * 4 + p
        return remote(at, at, ring_send.at[index], ring_recv.at[index], (dp, along(dim, 1)))

    def forward(index):
        if index in (8, 9):
            src, dst = wbuf.at[same_slot(index)], wbuf.at[other_slot(index)]
        else:
            if index < 8:
                dim, p = divmod(index, 4)
                rows = pl.ds(pl.multiple_of(place[dim] * 512, 512), 512)
            else:
                dim, rest = divmod(index - 10, 12)
                kind, p = divmod(rest, 4)
                rows = ring_rows(dim, kind, p)
            column = RING_COL[dim][p]
            src = wbuf.at[same_slot(column), rows]
            dst = wbuf.at[other_slot(column), rows]
        return remote(src, dst, fwd_send.at[index], fwd_recv.at[index], (sibling, ctx))

    def sib_copy(j):
        return remote(
            w_ref.at[:, j * 128 : (j + 1) * 128], wbuf.at[10 + j],
            sib_send.at[j], sib_recv.at[j], (sibling, ctx),
        )

    halo_copy = remote(
        tok_ref.at[0, ROWS - HALO :], tok.at[:HALO], halo_sem.at[0], halo_sem.at[1], after
    )

    pl.semaphore_wait(barrier, PEERS)
    for p, q in ((0, 2), (1, 3)):
        x_piece(0, p).start()
        x_piece(1, q).start()
        x_piece(1, p).start()
        x_piece(0, q).start()
    x_direct(0).start()
    x_direct(1).start()
    halo_copy.start()
    for j in range(4, 10):
        loc_copy(j).start()
    for j in range(10):
        sib_copy(j).start()

    swp[...] = jnp.zeros_like(swp)
    swp[0:HEADS] = sw_ref[...]
    small[...] = jnp.zeros_like(small)
    small[0:1, 0:HEADS] = bias_ref[...]
    small[1:2, 0:HEADS] = rate_ref[...]
    small[2:3, 0:HEADS] = skip_ref[...]
    tok_copy.wait()
    step_raw = lax.dot_general(
        tok[HALO:], swp[...], (((1,), (1,)), ((), ())), preferred_element_type=F32
    )
    step_raw = step_raw.astype(BF16).astype(F32) + small[0:1]
    step = jnp.maximum(step_raw, 0.0) + jnp.log1p(jnp.exp(-jnp.abs(step_raw)))
    keep = lax.broadcasted_iota(jnp.int32, (ROWS, 128), 1) < HEADS
    step = jnp.where(keep, step, 0.0)
    fall = step * (small[1:2] * (-LOG2E))
    lower = (
        lax.broadcasted_iota(jnp.int32, (BLOCK, BLOCK), 0)
        >= lax.broadcasted_iota(jnp.int32, (BLOCK, BLOCK), 1)
    ).astype(F32)
    level = jnp.log2(step)

    def halves(value):
        high = value.astype(BF16).astype(F32)
        low = (value - high).astype(BF16).astype(F32)
        return (high + pltpu.roll(low, 64, 1)).astype(BF16)

    ends = []
    for k in range(2):
        at = slice(k * BLOCK, (k + 1) * BLOCK)
        a = jnp.dot(
            lower, fall[at], precision=lax.Precision.HIGHEST, preferred_element_type=F32
        )
        end = a[BLOCK - 1 : BLOCK]
        ends.append(end)
        weight = jnp.where(keep[at], jnp.exp2(end - a) * step[at], 0.0)
        w2_ref[at] = halves(weight)
        e2_ref[at] = halves(jnp.where(keep[at], jnp.exp2(a), 0.0))
        turned = jnp.transpose(level[at] - a)
        turned_level = jnp.transpose(level[at])
        for g in range(GROUPS):
            a_ref[g, at] = a if g == 0 else pltpu.roll(a, 128 - 16 * g, 1)
            bt_ref[g, :, at] = turned[16 * g : 16 * g + 16]
            lt_ref[g, :, at] = turned_level[16 * g : 16 * g + 16]
    row = lax.broadcasted_iota(jnp.int32, (8, 128), 0)
    lane_ok = lax.broadcasted_iota(jnp.int32, (8, 128), 1) < HEADS
    exponent = jnp.where(row == 0, ends[0], jnp.where(row == 1, ends[1], ends[0] + ends[1]))
    rows_of = jnp.where(row == 3, small[2:3], jnp.exp2(exponent))
    misc_ref[...] = halves(jnp.where(lane_ok, rows_of, 0.0))

    head_row = lax.broadcasted_iota(jnp.int32, (128, 1024), 0) % HEADS
    head_lane = lax.broadcasted_iota(jnp.int32, (128, 1024), 1) // HEAD_DIM
    for g in range(GROUPS):
        spread[g] = (head_row == head_lane + 16 * g).astype(F32).astype(BF16)

    def total_send(r):
        peer = (ctx + r) % 32
        return remote(misc_ref, totals.at[ctx], sems.at[0], sems.at[1], (dp, peer))

    @pl.loop(1, 32)
    def _(r):
        total_send(r).start()

    totals[ctx] = misc_ref[...]

    halo_copy.wait_recv()

    @pl.when(ctx == 0)
    def _():
        tok[:HALO] = jnp.zeros((HALO, D), BF16)

    def x_arrive(dim, p):
        x_piece(dim, p).wait_recv()
        ring_out(dim, 0, p).start()
        ring_out(dim, 1, p).start()
        forward(dim * 4 + p).start()

    def near_arrive(dim, p):
        for kind in range(2):
            ring_in(dim, kind, p).wait_recv()
            if (kind == 0) == (p < 2):
                ring_out(dim, 2, p).start()
            forward(10 + dim * 12 + kind * 4 + p).start()

    def far_arrive(dim, p):
        ring_in(dim, 2, p).wait_recv()
        forward(10 + dim * 12 + 8 + p).start()

    def direct_arrive(k):
        x_direct(k).wait_recv()
        forward(8 + k).start()

    def other_wait(pieces):
        for dim, p in pieces:
            forward(dim * 4 + p).wait_recv()
            for kind in range(3):
                forward(10 + dim * 12 + kind * 4 + p).wait_recv()

    one = ((0, 0), (1, 2))
    two = ((1, 0), (0, 2))
    three = ((0, 1), (1, 3))
    four = ((1, 1), (0, 3))

    def events(ii):
        for n in range(5):
            @pl.when(ii == n)
            def _(n=n):
                for i in (2 * n, 2 * n + 1):
                    for j in (2 * i, 2 * i + 1):
                        if i < 5:
                            loc_copy(j).wait()
                        else:
                            sib_copy(j - 10).wait_recv()
                if n == 1:
                    for piece in one:
                        x_arrive(*piece)
                if n == 3:
                    for piece in two:
                        x_arrive(*piece)

        @pl.when(ii == 5)
        def _():
            for piece in three:
                x_arrive(*piece)
            for piece in one:
                near_arrive(*piece)
            for piece in four:
                x_arrive(*piece)
            for piece in two:
                near_arrive(*piece)
            for piece in one:
                far_arrive(*piece)
            for piece in two:
                far_arrive(*piece)

        @pl.when(ii == 6)
        def _():
            for piece in three:
                near_arrive(*piece)
            other_wait(((0, 0), (0, 2), (1, 0), (1, 2)))

        @pl.when(ii == 7)
        def _():
            for piece in four:
                near_arrive(*piece)
            for piece in three:
                far_arrive(*piece)
            for piece in four:
                far_arrive(*piece)

        @pl.when(ii == 8)
        def _():
            direct_arrive(0)
            direct_arrive(1)
            other_wait(((0, 1), (0, 3)))

        @pl.when(ii == 9)
        def _():
            other_wait(((1, 1), (1, 3)))
            forward(8).wait_recv()
            forward(9).wait_recv()

    def block_of(i):
        m = i - 10
        foreign = i // 10
        late = (i - 6) // 8 * foreign
        kind = foreign * (2 + (1 - late) * ((m % 4) // 2) + late * ((i - 14 + 30) // 3 - 10))
        near_kind = (1 - foreign) * (i // 5)
        pair = (1 - foreign) * (i % 5) + foreign * (
            (1 - late) * (m % 2) + late * (2 + (i - 14 + 30) % 3)
        )
        relation = kind + near_kind
        lo = (dp + relation) % 2
        hi = (dp // 2 + relation // 2) % 2
        return (2 * hi + lo) * 5 + pair

    def product(i, pbuf):
        weights = jnp.concatenate([wbuf[2 * i], wbuf[2 * i + 1]], axis=1)
        pbuf[...] = (
            jnp.dot(tok[...], weights, preferred_element_type=F32).astype(BF16).astype(F32)
        )

    def activate(block, at, pbuf):
        columns = pl.ds(pl.multiple_of(block * 256, 256), 256)
        taps = taps_ref[:, columns]
        summed = fb_ref[:, columns] + taps[0:1] * pbuf[HALO - 3 : HALO - 3 + ROWS]
        for k in range(1, 4):
            summed = summed + taps[k : k + 1] * pbuf[HALO - 3 + k : HALO - 3 + k + ROWS]
        half = 0.5 * summed
        act[at] = (half * jnp.tanh(half) + half).astype(BF16)

    pbuf_b[...] = jnp.zeros_like(pbuf_b)

    @pl.loop(0, 10)
    def _(ii):
        events(ii)
        i = 2 * ii
        started = (ii + 9) // 10
        block = block_of(i - started)
        at = started * block + (1 - started) * 20
        product(i, pbuf_a)
        activate(block, at, pbuf_b)
        product(i + 1, pbuf_b)
        activate(block_of(i), block_of(i), pbuf_a)

    activate(block_of(19), block_of(19), pbuf_b)

    def widen(value, g):
        return jnp.dot(value, spread[g], preferred_element_type=F32)

    def group_of(g, at):
        return jnp.concatenate([act[4 * g + j, at] for j in range(4)], axis=1)

    def map_lanes(g, at, base):
        return act[base + g // 2, at, pl.ds(pl.multiple_of((g % 2) * 128, 128), 128)]

    def state_send(r, half):
        peer = (ctx + r) % 32
        rows = slice(half * 64, half * 64 + 64)
        return remote(
            state_out.at[peer, rows], state_in.at[half, ctx],
            sems.at[2 + half], sems.at[4 + half], (dp, peer),
        )

    def enter_send(r, half):
        peer = (ctx + r) % 32
        rows = slice(half * 64, half * 64 + 64)
        return remote(
            enter_out.at[half, peer], enter_in.at[ctx, rows],
            sems.at[6 + half], sems.at[8 + half], (dp, peer),
        )

    def wait_all(part, index):
        pltpu.make_async_copy(part, part, sems.at[index]).wait()

    @pl.loop(0, GROUPS)
    def _(g):
        decays = widen(misc_ref[...], g)
        total = None
        for k in range(2):
            at = slice(k * BLOCK, (k + 1) * BLOCK)
            values = group_of(g, at).astype(F32)
            scaled = (widen(w2_ref[at], g) * values).astype(BF16)
            maps = map_lanes(g, at, 16)
            state = lax.dot_general(
                maps, scaled, (((0,), (0,)), ((), ())), preferred_element_type=F32
            )
            if k == 0:
                first[g] = state
                total = decays[1:2] * state
            else:
                total = total + state
        for i in range(8):
            state_out[g * 8 + i] = total[:, i * 128 : (i + 1) * 128].astype(BF16)

    for half in range(2):
        @pl.loop(1, 32)
        def _(r):
            state_send(r, half).start()

        state_in[half, ctx] = state_out[ctx, half * 64 : half * 64 + 64]

    lane = lax.broadcasted_iota(jnp.int32, (BLOCK, 128), 1) < HEAD_DIM
    causal = lax.broadcasted_iota(jnp.int32, (128, 128), 0) >= lax.broadcasted_iota(
        jnp.int32, (128, 128), 1
    )

    @pl.loop(0, 8)
    def _(n):
        g = n // 2
        start = (n % 2) * BLOCK
        rows = pl.ds(pl.multiple_of(start, BLOCK), BLOCK)
        early = pl.ds(pl.multiple_of(start, 128), 128)
        later = pl.ds(pl.multiple_of(start + 128, 128), 128)
        full = lax.dot_general(
            map_lanes(g, rows, 18), map_lanes(g, rows, 16),
            (((1,), (1,)), ((), ())), preferred_element_type=F32,
        )
        scores[0] = jnp.where(causal, full[:128, :128], 0.0)
        scores[1] = full[128:, :128]
        scores[2] = jnp.where(causal, full[128:, 128:], 0.0)
        skip = widen(misc_ref[...], g)[3:4]
        for i in range(8):
            lanes = slice((i % 2) * 128, (i % 2) * 128 + 128)
            values = act[4 * g + i // 2, rows, lanes]
            made = []
            for h in (2 * i, 2 * i + 1):
                upper = a_ref[g, early, h : h + 1]
                under = a_ref[g, later, h : h + 1]
                b0 = bt_ref[g, h : h + 1, early]
                b1 = bt_ref[g, h : h + 1, later]
                l0 = lt_ref[g, h : h + 1, early]
                l1 = lt_ref[g, h : h + 1, later]
                w00 = (jnp.exp2(jnp.minimum(upper + b0, l0)) * scores[0]).astype(BF16)
                w10 = (jnp.exp2(under + b0) * scores[1]).astype(BF16)
                w11 = (jnp.exp2(jnp.minimum(under + b1, l1)) * scores[2]).astype(BF16)
                top = jnp.dot(w00, values[:128], preferred_element_type=F32)
                low = jnp.dot(
                    jnp.concatenate([w10, w11], axis=1), values, preferred_element_type=F32
                )
                made.append(jnp.concatenate([top, low], axis=0))
            mixed = jnp.where(lane, made[0], made[1])
            mix[g, rows, i * 128 : (i + 1) * 128] = (
                mixed + skip[:, i * 128 : (i + 1) * 128] * values.astype(F32)
            )

    wait_all(totals.at[0:31], 1)
    mine = lax.broadcasted_iota(jnp.int32, (128, 128), 0) % HEADS == (
        2 * ctx + lax.broadcasted_iota(jnp.int32, (128, 128), 1) // HEAD_DIM
    )
    pick = mine.astype(F32).astype(BF16)
    for k in range(32):
        decays_in[k] = jnp.dot(totals[k], pick, preferred_element_type=F32)

    for half in range(2):
        wait_all(state_in.at[half, 0:31], 4 + half)

        def scan(k, carry):
            enter_out[half, k] = carry.astype(BF16)
            return decays_in[k, 2:3] * carry + state_in[half, k].astype(F32)

        lax.fori_loop(0, 32, scan, jnp.zeros((64, 128), F32))

        @pl.loop(1, 32)
        def _(r):
            enter_send(r, half).start()

        enter_in[ctx, half * 64 : half * 64 + 64] = enter_out[half, ctx]

    for half in range(2):
        wait_all(enter_in.at[0:31, half * 64 : half * 64 + 64], 8 + half)

    def out_copy(g):
        columns = pl.ds(pl.multiple_of(g * 1024, 1024), 1024)
        return pltpu.make_async_copy(mixed_out.at[g], out_ref.at[:, columns], out_sem)

    @pl.loop(0, GROUPS)
    def _(g):
        decays = widen(misc_ref[...], g)
        enter = jnp.concatenate([enter_in[g * 8 + i] for i in range(8)], axis=1)
        for k in range(2):
            rows = slice(k * BLOCK, (k + 1) * BLOCK)
            if k == 1:
                enter = (decays[0:1] * enter.astype(F32) + first[g]).astype(BF16)
            carried = jnp.dot(
                map_lanes(g, rows, 18), enter, preferred_element_type=F32
            ) * widen(e2_ref[rows], g)
            mixed_out[g, rows] = (mix[g, rows] + carried).astype(BF16)
        out_copy(g).start()

    halo_copy.wait_send()
    for dim in range(2):
        for p in range(4):
            x_piece(dim, p).wait_send()
            for kind in range(3):
                ring_out(dim, kind, p).wait_send()
    for k in range(2):
        x_direct(k).wait_send()
    for j in range(10):
        sib_copy(j).wait_send()
    for index in range(34):
        forward(index).wait_send()
    wait_all(totals.at[0:31], 0)
    for half in range(2):
        wait_all(state_in.at[half, 0:31], 2 + half)
        wait_all(state_in.at[half, 0:31], 6 + half)
    pltpu.make_async_copy(mixed_out, mixed_out, out_sem).wait()


def mixer(tokens, in_weight, step_weight, bias, rate, skip, taps, filter_bias):
    vmem = pl.BlockSpec(memory_space=pltpu.VMEM)
    anywhere = pl.BlockSpec(memory_space=pl.ANY)
    dma = pltpu.SemaphoreType.DMA
    return pl.pallas_call(
        mixer_kernel,
        out_shape=jax.ShapeDtypeStruct((ROWS, INNER), BF16),
        in_specs=[anywhere, anywhere] + [vmem] * 6,
        out_specs=anywhere,
        scratch_shapes=[
            pltpu.VMEM((HALO + ROWS, D), BF16),
            pltpu.VMEM((40, D, 128), BF16),
            pltpu.VMEM((HALO + ROWS, 256), F32),
            pltpu.VMEM((HALO + ROWS, 256), F32),
            pltpu.VMEM((21, ROWS, 256), BF16),
            pltpu.VMEM((128, D), BF16),
            pltpu.VMEM((8, 128), F32),
            pltpu.VMEM((GROUPS, ROWS, 128), F32),
            pltpu.VMEM((GROUPS, 16, ROWS), F32),
            pltpu.VMEM((GROUPS, 16, ROWS), F32),
            pltpu.VMEM((ROWS, 128), BF16),
            pltpu.VMEM((ROWS, 128), BF16),
            pltpu.VMEM((8, 128), BF16),
            pltpu.VMEM((GROUPS, 128, 1024), BF16),
            pltpu.VMEM((GROUPS, STATE, 1024), F32),
            pltpu.VMEM((GROUPS, ROWS, 1024), F32),
            pltpu.VMEM((GROUPS, ROWS, 1024), BF16),
            pltpu.VMEM((3, 128, 128), F32),
            pltpu.VMEM((32, 8, 128), BF16),
            pltpu.VMEM((32, 8, 128), F32),
            pltpu.VMEM((32, STATE, 128), BF16),
            pltpu.VMEM((2, 32, 64, 128), BF16),
            pltpu.VMEM((2, 32, 64, 128), BF16),
            pltpu.VMEM((32, STATE, 128), BF16),
            dma((10,)), dma, dma, dma((2,)), dma((10,)), dma((10,)),
            dma((10,)), dma((10,)), dma((24,)), dma((24,)), dma((34,)), dma((34,)), dma((10,)),
        ],
        compiler_params=pltpu.CompilerParams(
            collective_id=0, has_side_effects=True, vmem_limit_bytes=58 * 2**20
        ),
        name="mixer",
    )(tokens, in_weight, step_weight, bias, rate, skip, taps, filter_bias)


def norm_kernel(mixed_ref, gain_ref, out_ref):
    for g in range(GROUPS):
        columns = slice(g * 1024, (g + 1) * 1024)
        mixed = mixed_ref[:, columns].astype(F32)
        mean = jnp.mean(mixed * mixed, axis=1, keepdims=True)
        out_ref[:, columns] = (mixed * lax.rsqrt(mean + 1e-05) * gain_ref[:, columns]).astype(
            BF16
        )


def group_norm(mixed, gain):
    tile = 64
    return pl.pallas_call(
        norm_kernel,
        out_shape=jax.ShapeDtypeStruct((ROWS, INNER), BF16),
        grid=(ROWS // tile,),
        in_specs=[
            pl.BlockSpec((tile, INNER), lambda i: (i, 0)),
            pl.BlockSpec((1, INNER), lambda i: (0, 0)),
        ],
        out_specs=pl.BlockSpec((tile, INNER), lambda i: (i, 0)),
        name="group_norm",
    )(mixed, gain)


def per_device(
    tokens,
    in_weight,
    step_weight,
    step_bias,
    decay_rate,
    skip_gain,
    filter_taps,
    filter_bias,
    norm_gain,
):
    mixed = mixer(
        tokens, in_weight, step_weight.T, step_bias[None], decay_rate[None], skip_gain[None],
        filter_taps, filter_bias[None],
    )
    return group_norm(mixed, norm_gain[None])[None]


def solution(mesh):
    in_specs = (P("dp", "ctx", None), P(None, "dp"), P(), P(), P(), P(), P(), P(), P())
    out_specs = P("dp", "ctx", None)
    return jax.shard_map(
        per_device, mesh=mesh, in_specs=in_specs, out_specs=out_specs, check_vma=False
    )
```

```python
import functools

import jax
import jax.numpy as jnp
from jax import lax
from jax.experimental import pallas as pl
from jax.experimental.pallas import tpu as pltpu
from jax.sharding import PartitionSpec as P

D = 2048
HEADS = 64
HEAD_DIM = 64
STATE = 128
GROUPS = 4
BLOCK = 256
ROWS = 512
HALO = 16
SHARD = 1280
XBC = 5120
INNER = 4096
LOG2E = 1.4426950408889634
MESH = pl.DeviceIdType.MESH
F32 = jnp.float32
BF16 = jnp.bfloat16

RING_COL = ((0, 4, 1, 5), (2, 6, 3, 7))
SAME_SLOT = (10, 11, 14, 15, 16)
OTHER_SLOT = (12, 13, 17, 18, 19)
PEERS = 34


def same_slot(column):
    return 2 * SAME_SLOT[column // 2] + column % 2


def other_slot(column):
    return 2 * OTHER_SLOT[column // 2] + column % 2


def mixer_kernel(
    tok_ref, w_ref, sw_ref, bias_ref, rate_ref, skip_ref, taps_ref, fb_ref,
    out_ref,
    tok, wbuf, pbuf, act, swp, small,
    a_ref, bt_ref, lt_ref, w2_ref, e2_ref, misc_ref,
    spread, first, mix, mixed_out, scores, totals, decays_in,
    state_out, state_in, enter_out, enter_in,
    loc_sem, tok_sem, out_sem, halo_sem, sib_send, sib_recv,
    x_send, x_recv, ring_send, ring_recv, fwd_send, fwd_recv, sems,
):
    dp = lax.axis_index("dp")
    ctx = lax.axis_index("ctx")
    z = ctx % 4
    y = (ctx // 4) % 4
    xh = ctx // 16
    sibling = dp + 1 - 2 * (dp % 2)
    across = (dp + 2) % 4
    place = (z, y)

    def along(dim, step):
        if dim == 0:
            return xh * 16 + y * 4 + (z + step) % 4
        return xh * 16 + ((y + step) % 4) * 4 + z

    source_a = (across, ctx)
    source_b = (across, (ctx + 16) % 32)
    after = (dp, (ctx + 1) % 32)

    def loc_copy(j):
        return pltpu.make_async_copy(
            w_ref.at[:, j * 128 : (j + 1) * 128], wbuf.at[j], loc_sem.at[j]
        )

    barrier = pltpu.get_barrier_semaphore()
    for peer in ((sibling, ctx), source_a, source_b):
        pl.semaphore_signal(barrier, inc=1, device_id=peer, device_id_type=MESH)

    @pl.loop(1, 32)
    def _(r):
        pl.semaphore_signal(
            barrier, inc=1, device_id=(dp, (ctx + r) % 32), device_id_type=MESH
        )

    tok_copy = pltpu.make_async_copy(tok_ref.at[0], tok.at[HALO:], tok_sem)
    tok_copy.start()
    for j in range(4):
        loc_copy(j).start()

    def remote(src, dst, send, recv, peer):
        return pltpu.make_async_remote_copy(
            src_ref=src, dst_ref=dst, send_sem=send, recv_sem=recv,
            device_id=peer, device_id_type=MESH,
        )

    def x_piece(dim, p):
        column = RING_COL[dim][p]
        rows = pl.ds(pl.multiple_of(place[dim] * 512, 512), 512)
        return remote(
            w_ref.at[rows, column * 128 : (column + 1) * 128],
            wbuf.at[same_slot(column), rows],
            x_send.at[dim * 4 + p], x_recv.at[dim * 4 + p],
            source_a if p < 2 else source_b,
        )

    def x_direct(k):
        column = 8 + k
        return remote(
            w_ref.at[:, column * 128 : (column + 1) * 128],
            wbuf.at[same_slot(column)],
            x_send.at[8 + k], x_recv.at[8 + k], (source_a, source_b)[k],
        )

    def ring_rows(dim, kind, p):
        back = (3, 1, 2)[kind]
        return pl.ds(pl.multiple_of(((place[dim] + back) % 4) * 512, 512), 512)

    def ring_out(dim, kind, p):
        column = RING_COL[dim][p]
        rows = pl.ds(pl.multiple_of(place[dim] * 512, 512), 512)
        peer = along(dim, (1, 3, 2)[kind])
        at = wbuf.at[same_slot(column), rows]
        index = dim * 12 + kind * 4 + p
        return remote(at, at, ring_send.at[index], ring_recv.at[index], (dp, peer))

    def ring_in(dim, kind, p):
        column = RING_COL[dim][p]
        at = wbuf.at[same_slot(column), ring_rows(dim, kind, p)]
        index = dim * 12 + kind * 4 + p
        return remote(at, at, ring_send.at[index], ring_recv.at[index], (dp, along(dim, 1)))

    def forward(index):
        if index in (8, 9):
            src, dst = wbuf.at[same_slot(index)], wbuf.at[other_slot(index)]
        else:
            if index < 8:
                dim, p = divmod(index, 4)
                rows = pl.ds(pl.multiple_of(place[dim] * 512, 512), 512)
            else:
                dim, rest = divmod(index - 10, 12)
                kind, p = divmod(rest, 4)
                rows = ring_rows(dim, kind, p)
            column = RING_COL[dim][p]
            src = wbuf.at[same_slot(column), rows]
            dst = wbuf.at[other_slot(column), rows]
        return remote(src, dst, fwd_send.at[index], fwd_recv.at[index], (sibling, ctx))

    def sib_copy(j):
        return remote(
            w_ref.at[:, j * 128 : (j + 1) * 128], wbuf.at[10 + j],
            sib_send.at[j], sib_recv.at[j], (sibling, ctx),
        )

    halo_copy = remote(
        tok_ref.at[0, ROWS - HALO :], tok.at[:HALO], halo_sem.at[0], halo_sem.at[1], after
    )

    with jax.named_scope("barrier"):
        pl.semaphore_wait(barrier, PEERS)
    halo_copy.start()
    for p, q in ((0, 2), (1, 3)):
        x_piece(0, p).start()
        x_piece(1, q).start()
        x_piece(1, p).start()
        x_piece(0, q).start()
    x_direct(0).start()
    x_direct(1).start()
    for j in range(4, 10):
        loc_copy(j).start()
    for j in range(10):
        sib_copy(j).start()

    swp[...] = jnp.zeros_like(swp)
    swp[0:HEADS] = sw_ref[...]
    small[...] = jnp.zeros_like(small)
    small[0:1, 0:HEADS] = bias_ref[...]
    small[1:2, 0:HEADS] = rate_ref[...]
    small[2:3, 0:HEADS] = skip_ref[...]
    with jax.named_scope("tokwait"):
        tok_copy.wait()
    step_raw = lax.dot_general(
        tok[HALO:], swp[...], (((1,), (1,)), ((), ())), preferred_element_type=F32
    )
    step_raw = step_raw.astype(BF16).astype(F32) + small[0:1]
    step = jnp.maximum(step_raw, 0.0) + jnp.log1p(jnp.exp(-jnp.abs(step_raw)))
    keep = lax.broadcasted_iota(jnp.int32, (ROWS, 128), 1) < HEADS
    step = jnp.where(keep, step, 0.0)
    fall = step * (small[1:2] * (-LOG2E))
    lower = (
        lax.broadcasted_iota(jnp.int32, (BLOCK, BLOCK), 0)
        >= lax.broadcasted_iota(jnp.int32, (BLOCK, BLOCK), 1)
    ).astype(F32)
    level = jnp.log2(step)

    def halves(value):
        high = value.astype(BF16).astype(F32)
        low = (value - high).astype(BF16).astype(F32)
        return (high + pltpu.roll(low, 64, 1)).astype(BF16)

    ends = []
    for k in range(2):
        at = slice(k * BLOCK, (k + 1) * BLOCK)
        a = jnp.dot(
            lower, fall[at], precision=lax.Precision.HIGHEST, preferred_element_type=F32
        )
        end = a[BLOCK - 1 : BLOCK]
        ends.append(end)
        weight = jnp.where(keep[at], jnp.exp2(end - a) * step[at], 0.0)
        w2_ref[at] = halves(weight)
        e2_ref[at] = halves(jnp.where(keep[at], jnp.exp2(a), 0.0))
        turned = jnp.transpose(level[at] - a)
        turned_level = jnp.transpose(level[at])
        for g in range(GROUPS):
            a_ref[g, at] = a if g == 0 else pltpu.roll(a, 128 - 16 * g, 1)
            bt_ref[g, :, at] = turned[16 * g : 16 * g + 16]
            lt_ref[g, :, at] = turned_level[16 * g : 16 * g + 16]
    row = lax.broadcasted_iota(jnp.int32, (8, 128), 0)
    lane_ok = lax.broadcasted_iota(jnp.int32, (8, 128), 1) < HEADS
    exponent = jnp.where(row == 0, ends[0], jnp.where(row == 1, ends[1], ends[0] + ends[1]))
    rows_of = jnp.where(row == 3, small[2:3], jnp.exp2(exponent))
    misc_ref[...] = halves(jnp.where(lane_ok, rows_of, 0.0))

    head_row = lax.broadcasted_iota(jnp.int32, (128, 1024), 0) % HEADS
    head_lane = lax.broadcasted_iota(jnp.int32, (128, 1024), 1) // HEAD_DIM
    for g in range(GROUPS):
        spread[g] = (head_row == head_lane + 16 * g).astype(F32).astype(BF16)

    def total_send(r):
        peer = (ctx + r) % 32
        return remote(misc_ref, totals.at[ctx], sems.at[0], sems.at[1], (dp, peer))

    @pl.loop(1, 32)
    def _(r):
        total_send(r).start()

    totals[ctx] = misc_ref[...]

    with jax.named_scope("halowait"):
        halo_copy.wait_recv()

    @pl.when(ctx == 0)
    def _():
        tok[:HALO] = jnp.zeros((HALO, D), BF16)

    def x_arrive(dim, p):
        x_piece(dim, p).wait_recv()
        ring_out(dim, 0, p).start()
        ring_out(dim, 1, p).start()
        ring_out(dim, 2, p).start()
        forward(dim * 4 + p).start()

    def near_arrive(dim, p):
        for kind in range(2):
            ring_in(dim, kind, p).wait_recv()
            forward(10 + dim * 12 + kind * 4 + p).start()

    def far_arrive(dim, p):
        ring_in(dim, 2, p).wait_recv()
        forward(10 + dim * 12 + 8 + p).start()

    def direct_arrive(k):
        x_direct(k).wait_recv()
        forward(8 + k).start()

    def other_wait(pieces):
        for dim, p in pieces:
            forward(dim * 4 + p).wait_recv()
            for kind in range(3):
                forward(10 + dim * 12 + kind * 4 + p).wait_recv()

    one = ((0, 0), (1, 2))
    two = ((1, 0), (0, 2))
    three = ((0, 1), (1, 3))
    four = ((1, 1), (0, 3))

    def events(i):
        for n in range(5):
            @pl.when(i == n)
            def _(n=n):
                loc_copy(2 * n).wait()
                loc_copy(2 * n + 1).wait()

            @pl.when(i == 5 + n)
            def _(n=n):
                sib_copy(2 * n).wait_recv()
                sib_copy(2 * n + 1).wait_recv()

        def at(step, *actions):
            @pl.when(i == step)
            def _():
                for action, pieces in actions:
                    for piece in pieces:
                        action(*piece)

        at(1, (x_arrive, one))
        at(4, (x_arrive, two))
        at(7, (x_arrive, three))
        at(9, (x_arrive, four), (near_arrive, one))
        at(10, (near_arrive, two), (far_arrive, one), (far_arrive, two))
        at(11, (near_arrive, three))

        @pl.when(i == 12)
        def _():
            other_wait(((0, 0), (0, 2)))

        @pl.when(i == 13)
        def _():
            other_wait(((1, 0), (1, 2)))

        at(14, (near_arrive, four), (far_arrive, three), (far_arrive, four))

        @pl.when(i == 15)
        def _():
            direct_arrive(0)
            direct_arrive(1)

        @pl.when(i == 17)
        def _():
            other_wait(((0, 1), (0, 3)))

        @pl.when(i == 18)
        def _():
            other_wait(((1, 1), (1, 3)))

        @pl.when(i == 19)
        def _():
            forward(8).wait_recv()
            forward(9).wait_recv()

    def block_of(i):
        m = i - 10
        foreign = i // 10
        late = (i - 6) // 8 * foreign
        kind = foreign * (2 + (1 - late) * ((m % 4) // 2) + late * ((i - 14 + 30) // 3 - 10))
        near_kind = (1 - foreign) * (i // 5)
        pair = (1 - foreign) * (i % 5) + foreign * (
            (1 - late) * (m % 2) + late * (2 + (i - 14 + 30) % 3)
        )
        relation = kind + near_kind
        lo = (dp + relation) % 2
        hi = (dp // 2 + relation // 2) % 2
        return (2 * hi + lo) * 5 + pair

    @pl.loop(0, 20)
    def _(i):
        with jax.named_scope("events"):
            events(i)
        with jax.named_scope("compute"):
            block = block_of(i)
            weights = jnp.concatenate([wbuf[2 * i], wbuf[2 * i + 1]], axis=1)
            result = jnp.dot(tok[...], weights, preferred_element_type=F32)
            result = result.astype(BF16).astype(F32)
            for side in range(2):
                pbuf[side] = result[:, side * 128 : side * 128 + 128]
            for side in range(2):
                lanes = pl.ds(pl.multiple_of(block * 256 + side * 128, 128), 128)
                taps = taps_ref[:, lanes]
                bias = fb_ref[:, lanes]
                for row in range(0, ROWS, 64):
                    at = HALO - 3 + row
                    summed = bias + taps[0:1] * pbuf[side, at : at + 64]
                    for k in range(1, 4):
                        summed = summed + taps[k : k + 1] * pbuf[side, at + k : at + k + 64]
                    half = 0.5 * summed
                    act[block, row : row + 64, side * 128 : side * 128 + 128] = (
                        half * jnp.tanh(half) + half
                    ).astype(BF16)


    def widen(value, g):
        return jnp.dot(value, spread[g], preferred_element_type=F32)

    def group_of(g, at):
        return jnp.concatenate([act[4 * g + j, at] for j in range(4)], axis=1)

    def map_lanes(g, at, base):
        return act[base + g // 2, at, pl.ds(pl.multiple_of((g % 2) * 128, 128), 128)]

    def state_send(r, half):
        peer = (ctx + r) % 32
        rows = slice(half * 64, half * 64 + 64)
        return remote(
            state_out.at[peer, rows], state_in.at[half, ctx],
            sems.at[2 + half], sems.at[4 + half], (dp, peer),
        )

    def enter_send(r, half):
        peer = (ctx + r) % 32
        rows = slice(half * 64, half * 64 + 64)
        return remote(
            enter_out.at[half, peer], enter_in.at[ctx, rows],
            sems.at[6 + half], sems.at[8 + half], (dp, peer),
        )

    def wait_all(part, index):
        pltpu.make_async_copy(part, part, sems.at[index]).wait()

    @pl.loop(0, GROUPS)
    @jax.named_scope("groups")
    def _(g):
        decays = widen(misc_ref[...], g)
        total = None
        for k in range(2):
            at = slice(k * BLOCK, (k + 1) * BLOCK)
            values = group_of(g, at).astype(F32)
            scaled = (widen(w2_ref[at], g) * values).astype(BF16)
            maps = map_lanes(g, at, 16)
            state = lax.dot_general(
                maps, scaled, (((0,), (0,)), ((), ())), preferred_element_type=F32
            )
            if k == 0:
                first[g] = state
                total = decays[1:2] * state
            else:
                total = total + state
        for i in range(8):
            state_out[g * 8 + i] = total[:, i * 128 : (i + 1) * 128].astype(BF16)

    for half in range(2):
        @pl.loop(1, 32)
        def _(r):
            state_send(r, half).start()

        state_in[half, ctx] = state_out[ctx, half * 64 : half * 64 + 64]

    lane = lax.broadcasted_iota(jnp.int32, (BLOCK, 128), 1) < HEAD_DIM
    causal = lax.broadcasted_iota(jnp.int32, (128, 128), 0) >= lax.broadcasted_iota(
        jnp.int32, (128, 128), 1
    )

    @pl.loop(0, 8)
    @jax.named_scope("within")
    def _(n):
        g = n // 2
        start = (n % 2) * BLOCK
        rows = pl.ds(pl.multiple_of(start, BLOCK), BLOCK)
        early = pl.ds(pl.multiple_of(start, 128), 128)
        later = pl.ds(pl.multiple_of(start + 128, 128), 128)
        full = lax.dot_general(
            map_lanes(g, rows, 18), map_lanes(g, rows, 16),
            (((1,), (1,)), ((), ())), preferred_element_type=F32,
        )
        scores[0] = jnp.where(causal, full[:128, :128], 0.0)
        scores[1] = full[128:, :128]
        scores[2] = jnp.where(causal, full[128:, 128:], 0.0)
        skip = widen(misc_ref[...], g)[3:4]
        for i in range(8):
            lanes = slice((i % 2) * 128, (i % 2) * 128 + 128)
            values = act[4 * g + i // 2, rows, lanes]
            made = []
            for h in (2 * i, 2 * i + 1):
                upper = a_ref[g, early, h : h + 1]
                under = a_ref[g, later, h : h + 1]
                b0 = bt_ref[g, h : h + 1, early]
                b1 = bt_ref[g, h : h + 1, later]
                l0 = lt_ref[g, h : h + 1, early]
                l1 = lt_ref[g, h : h + 1, later]
                w00 = (jnp.exp2(jnp.minimum(upper + b0, l0)) * scores[0]).astype(BF16)
                w10 = (jnp.exp2(under + b0) * scores[1]).astype(BF16)
                w11 = (jnp.exp2(jnp.minimum(under + b1, l1)) * scores[2]).astype(BF16)
                top = jnp.dot(w00, values[:128], preferred_element_type=F32)
                low = jnp.dot(
                    jnp.concatenate([w10, w11], axis=1), values, preferred_element_type=F32
                )
                made.append(jnp.concatenate([top, low], axis=0))
            mixed = jnp.where(lane, made[0], made[1])
            mix[g, rows, i * 128 : (i + 1) * 128] = (
                mixed + skip[:, i * 128 : (i + 1) * 128] * values.astype(F32)
            )

    with jax.named_scope("totals"):
        wait_all(totals.at[0:31], 1)
    mine = lax.broadcasted_iota(jnp.int32, (128, 128), 0) % HEADS == (
        2 * ctx + lax.broadcasted_iota(jnp.int32, (128, 128), 1) // HEAD_DIM
    )
    pick = mine.astype(F32).astype(BF16)
    for k in range(32):
        decays_in[k] = jnp.dot(totals[k], pick, preferred_element_type=F32)

    for half in range(2):
        with jax.named_scope("statewait"):
            wait_all(state_in.at[half, 0:31], 4 + half)

        def scan(k, carry):
            enter_out[half, k] = carry.astype(BF16)
            return decays_in[k, 2:3] * carry + state_in[half, k].astype(F32)

        lax.fori_loop(0, 32, scan, jnp.zeros((64, 128), F32))

        @pl.loop(1, 32)
        def _(r):
            enter_send(r, half).start()

        enter_in[ctx, half * 64 : half * 64 + 64] = enter_out[half, ctx]

    for half in range(2):
        with jax.named_scope("enterwait"):
            wait_all(enter_in.at[0:31, half * 64 : half * 64 + 64], 8 + half)

    def out_copy(g):
        columns = pl.ds(pl.multiple_of(g * 1024, 1024), 1024)
        return pltpu.make_async_copy(mixed_out.at[g], out_ref.at[:, columns], out_sem)

    @pl.loop(0, GROUPS)
    @jax.named_scope("groups")
    def _(g):
        decays = widen(misc_ref[...], g)
        enter = jnp.concatenate([enter_in[g * 8 + i] for i in range(8)], axis=1)
        for k in range(2):
            rows = slice(k * BLOCK, (k + 1) * BLOCK)
            if k == 1:
                enter = (decays[0:1] * enter.astype(F32) + first[g]).astype(BF16)
            carried = jnp.dot(
                map_lanes(g, rows, 18), enter, preferred_element_type=F32
            ) * widen(e2_ref[rows], g)
            mixed_out[g, rows] = (mix[g, rows] + carried).astype(BF16)
        out_copy(g).start()

    with jax.named_scope("drain"):
        halo_copy.wait_send()
        for dim in range(2):
            for p in range(4):
                x_piece(dim, p).wait_send()
                for kind in range(3):
                    ring_out(dim, kind, p).wait_send()
        for k in range(2):
            x_direct(k).wait_send()
        for j in range(10):
            sib_copy(j).wait_send()
        for index in range(34):
            forward(index).wait_send()
        wait_all(totals.at[0:31], 0)
        for half in range(2):
            wait_all(state_in.at[half, 0:31], 2 + half)
            wait_all(state_in.at[half, 0:31], 6 + half)
        pltpu.make_async_copy(mixed_out, mixed_out, out_sem).wait()


def mixer(tokens, in_weight, step_weight, bias, rate, skip, taps, filter_bias):
    vmem = pl.BlockSpec(memory_space=pltpu.VMEM)
    anywhere = pl.BlockSpec(memory_space=pl.ANY)
    dma = pltpu.SemaphoreType.DMA
    return pl.pallas_call(
        mixer_kernel,
        out_shape=jax.ShapeDtypeStruct((ROWS, INNER), BF16),
        in_specs=[anywhere, anywhere] + [vmem] * 6,
        out_specs=anywhere,
        scratch_shapes=[
            pltpu.VMEM((HALO + ROWS, D), BF16),
            pltpu.VMEM((40, D, 128), BF16),
            pltpu.VMEM((2, HALO + ROWS, 128), F32),
            pltpu.VMEM((20, ROWS, 256), BF16),
            pltpu.VMEM((128, D), BF16),
            pltpu.VMEM((8, 128), F32),
            pltpu.VMEM((GROUPS, ROWS, 128), F32),
            pltpu.VMEM((GROUPS, 16, ROWS), F32),
            pltpu.VMEM((GROUPS, 16, ROWS), F32),
            pltpu.VMEM((ROWS, 128), BF16),
            pltpu.VMEM((ROWS, 128), BF16),
            pltpu.VMEM((8, 128), BF16),
            pltpu.VMEM((GROUPS, 128, 1024), BF16),
            pltpu.VMEM((GROUPS, STATE, 1024), F32),
            pltpu.VMEM((GROUPS, ROWS, 1024), F32),
            pltpu.VMEM((GROUPS, ROWS, 1024), BF16),
            pltpu.VMEM((3, 128, 128), F32),
            pltpu.VMEM((32, 8, 128), BF16),
            pltpu.VMEM((32, 8, 128), F32),
            pltpu.VMEM((32, STATE, 128), BF16),
            pltpu.VMEM((2, 32, 64, 128), BF16),
            pltpu.VMEM((2, 32, 64, 128), BF16),
            pltpu.VMEM((32, STATE, 128), BF16),
            dma((10,)), dma, dma, dma((2,)), dma((10,)), dma((10,)),
            dma((10,)), dma((10,)), dma((24,)), dma((24,)), dma((34,)), dma((34,)), dma((10,)),
        ],
        compiler_params=pltpu.CompilerParams(
            collective_id=0, has_side_effects=True, vmem_limit_bytes=58 * 2**20
        ),
        name="mixer",
    )(tokens, in_weight, step_weight, bias, rate, skip, taps, filter_bias)


def norm_kernel(mixed_ref, gain_ref, out_ref):
    for g in range(GROUPS):
        columns = slice(g * 1024, (g + 1) * 1024)
        mixed = mixed_ref[:, columns].astype(F32)
        mean = jnp.mean(mixed * mixed, axis=1, keepdims=True)
        out_ref[:, columns] = (mixed * lax.rsqrt(mean + 1e-05) * gain_ref[:, columns]).astype(
            BF16
        )


def group_norm(mixed, gain):
    tile = 256
    return pl.pallas_call(
        norm_kernel,
        out_shape=jax.ShapeDtypeStruct((ROWS, INNER), BF16),
        grid=(ROWS // tile,),
        in_specs=[
            pl.BlockSpec((tile, INNER), lambda i: (i, 0)),
            pl.BlockSpec((1, INNER), lambda i: (0, 0)),
        ],
        out_specs=pl.BlockSpec((tile, INNER), lambda i: (i, 0)),
        name="group_norm",
    )(mixed, gain)


def per_device(
    tokens,
    in_weight,
    step_weight,
    step_bias,
    decay_rate,
    skip_gain,
    filter_taps,
    filter_bias,
    norm_gain,
):
    mixed = mixer(
        tokens, in_weight, step_weight.T, step_bias[None], decay_rate[None], skip_gain[None],
        filter_taps, filter_bias[None],
    )
    return group_norm(mixed, norm_gain[None])[None]


def solution(mesh):
    in_specs = (P("dp", "ctx", None), P(None, "dp"), P(), P(), P(), P(), P(), P(), P())
    out_specs = P("dp", "ctx", None)
    return jax.shard_map(
        per_device, mesh=mesh, in_specs=in_specs, out_specs=out_specs, check_vma=False
    )
```

```python
import functools

import jax
import jax.numpy as jnp
from jax import lax
from jax.experimental import pallas as pl
from jax.experimental.pallas import tpu as pltpu
from jax.sharding import PartitionSpec as P

D = 2048
HEADS = 64
HEAD_DIM = 64
STATE = 128
GROUPS = 4
BLOCK = 256
ROWS = 512
HALO = 16
SHARD = 1280
XBC = 5120
INNER = 4096
LOG2E = 1.4426950408889634
MESH = pl.DeviceIdType.MESH
F32 = jnp.float32
BF16 = jnp.bfloat16

RING_COL = ((0, 4, 3, 7), (2, 6, 1, 5))
SAME_SLOT = (10, 12, 14, 16, 18)
OTHER_SLOT = (11, 13, 15, 17, 19)
PEERS = 34


def same_slot(column):
    return 2 * SAME_SLOT[column // 2] + column % 2


def other_slot(column):
    return 2 * OTHER_SLOT[column // 2] + column % 2


def mixer_kernel(
    tok_ref, w_ref, sw_ref, bias_ref, rate_ref, skip_ref, taps_ref, fb_ref,
    out_ref,
    tok, wbuf, pbuf, act, swp, small,
    a_ref, bt_ref, lt_ref, w2_ref, e2_ref, misc_ref,
    spread, first, mix, mixed_out, scores, totals, decays_in,
    state_out, state_in, enter_out, enter_in,
    loc_sem, tok_sem, out_sem, halo_sem, sib_send, sib_recv,
    x_send, x_recv, ring_send, ring_recv, fwd_send, fwd_recv, sems,
):
    dp = lax.axis_index("dp")
    ctx = lax.axis_index("ctx")
    z = ctx % 4
    y = (ctx // 4) % 4
    xh = ctx // 16
    sibling = dp + 1 - 2 * (dp % 2)
    across = (dp + 2) % 4
    place = (z, y)

    def along(dim, step):
        if dim == 0:
            return xh * 16 + y * 4 + (z + step) % 4
        return xh * 16 + ((y + step) % 4) * 4 + z

    source_a = (across, ctx)
    source_b = (across, (ctx + 16) % 32)
    after = (dp, (ctx + 1) % 32)

    def loc_copy(j):
        return pltpu.make_async_copy(
            w_ref.at[:, j * 128 : (j + 1) * 128], wbuf.at[j], loc_sem.at[j]
        )

    barrier = pltpu.get_barrier_semaphore()
    for peer in ((sibling, ctx), source_a, source_b):
        pl.semaphore_signal(barrier, inc=1, device_id=peer, device_id_type=MESH)

    @pl.loop(1, 32)
    def _(r):
        pl.semaphore_signal(
            barrier, inc=1, device_id=(dp, (ctx + r) % 32), device_id_type=MESH
        )

    tok_copy = pltpu.make_async_copy(tok_ref.at[0], tok.at[HALO:], tok_sem)
    tok_copy.start()
    for j in range(4):
        loc_copy(j).start()

    def remote(src, dst, send, recv, peer):
        return pltpu.make_async_remote_copy(
            src_ref=src, dst_ref=dst, send_sem=send, recv_sem=recv,
            device_id=peer, device_id_type=MESH,
        )

    def x_piece(dim, p):
        column = RING_COL[dim][p]
        rows = pl.ds(pl.multiple_of(place[dim] * 512, 512), 512)
        return remote(
            w_ref.at[rows, column * 128 : (column + 1) * 128],
            wbuf.at[same_slot(column), rows],
            x_send.at[dim * 4 + p], x_recv.at[dim * 4 + p],
            source_a if p < 2 else source_b,
        )

    def x_direct(k):
        column = 8 + k
        return remote(
            w_ref.at[:, column * 128 : (column + 1) * 128],
            wbuf.at[same_slot(column)],
            x_send.at[8 + k], x_recv.at[8 + k], (source_a, source_b)[k],
        )

    def ring_rows(dim, kind, p):
        back = (3, 1, 2)[kind]
        return pl.ds(pl.multiple_of(((place[dim] + back) % 4) * 512, 512), 512)

    def ring_out(dim, kind, p):
        column = RING_COL[dim][p]
        rows = pl.ds(pl.multiple_of(place[dim] * 512, 512), 512)
        peer = along(dim, (1, 3, 1 if p < 2 else 3)[kind])
        if kind == 2:
            rows = ring_rows(dim, 0 if p < 2 else 1, p)
        at = wbuf.at[same_slot(column), rows]
        index = dim * 12 + kind * 4 + p
        return remote(at, at, ring_send.at[index], ring_recv.at[index], (dp, peer))

    def ring_in(dim, kind, p):
        column = RING_COL[dim][p]
        at = wbuf.at[same_slot(column), ring_rows(dim, kind, p)]
        index = dim * 12 + kind * 4 + p
        return remote(at, at, ring_send.at[index], ring_recv.at[index], (dp, along(dim, 1)))

    def forward(index):
        if index in (8, 9):
            src, dst = wbuf.at[same_slot(index)], wbuf.at[other_slot(index)]
        else:
            if index < 8:
                dim, p = divmod(index, 4)
                rows = pl.ds(pl.multiple_of(place[dim] * 512, 512), 512)
            else:
                dim, rest = divmod(index - 10, 12)
                kind, p = divmod(rest, 4)
                rows = ring_rows(dim, kind, p)
            column = RING_COL[dim][p]
            src = wbuf.at[same_slot(column), rows]
            dst = wbuf.at[other_slot(column), rows]
        return remote(src, dst, fwd_send.at[index], fwd_recv.at[index], (sibling, ctx))

    def sib_copy(j):
        return remote(
            w_ref.at[:, j * 128 : (j + 1) * 128], wbuf.at[10 + j],
            sib_send.at[j], sib_recv.at[j], (sibling, ctx),
        )

    halo_copy = remote(
        tok_ref.at[0, ROWS - HALO :], tok.at[:HALO], halo_sem.at[0], halo_sem.at[1], after
    )

    with jax.named_scope("barrier"):
        pl.semaphore_wait(barrier, PEERS)
    halo_copy.start()
    for p, q in ((0, 2), (1, 3)):
        x_piece(0, p).start()
        x_piece(1, q).start()
        x_piece(1, p).start()
        x_piece(0, q).start()
    x_direct(0).start()
    x_direct(1).start()
    for j in range(4, 10):
        loc_copy(j).start()
    for j in range(10):
        sib_copy(j).start()

    swp[...] = jnp.zeros_like(swp)
    swp[0:HEADS] = sw_ref[...]
    small[...] = jnp.zeros_like(small)
    small[0:1, 0:HEADS] = bias_ref[...]
    small[1:2, 0:HEADS] = rate_ref[...]
    small[2:3, 0:HEADS] = skip_ref[...]
    with jax.named_scope("tokwait"):
        tok_copy.wait()
    step_raw = lax.dot_general(
        tok[HALO:], swp[...], (((1,), (1,)), ((), ())), preferred_element_type=F32
    )
    step_raw = step_raw.astype(BF16).astype(F32) + small[0:1]
    step = jnp.maximum(step_raw, 0.0) + jnp.log1p(jnp.exp(-jnp.abs(step_raw)))
    keep = lax.broadcasted_iota(jnp.int32, (ROWS, 128), 1) < HEADS
    step = jnp.where(keep, step, 0.0)
    fall = step * (small[1:2] * (-LOG2E))
    lower = (
        lax.broadcasted_iota(jnp.int32, (BLOCK, BLOCK), 0)
        >= lax.broadcasted_iota(jnp.int32, (BLOCK, BLOCK), 1)
    ).astype(F32)
    level = jnp.log2(step)

    def halves(value):
        high = value.astype(BF16).astype(F32)
        low = (value - high).astype(BF16).astype(F32)
        return (high + pltpu.roll(low, 64, 1)).astype(BF16)

    ends = []
    for k in range(2):
        at = slice(k * BLOCK, (k + 1) * BLOCK)
        a = jnp.dot(
            lower, fall[at], precision=lax.Precision.HIGHEST, preferred_element_type=F32
        )
        end = a[BLOCK - 1 : BLOCK]
        ends.append(end)
        weight = jnp.where(keep[at], jnp.exp2(end - a) * step[at], 0.0)
        w2_ref[at] = halves(weight)
        e2_ref[at] = halves(jnp.where(keep[at], jnp.exp2(a), 0.0))
        turned = jnp.transpose(level[at] - a)
        turned_level = jnp.transpose(level[at])
        for g in range(GROUPS):
            a_ref[g, at] = a if g == 0 else pltpu.roll(a, 128 - 16 * g, 1)
            bt_ref[g, :, at] = turned[16 * g : 16 * g + 16]
            lt_ref[g, :, at] = turned_level[16 * g : 16 * g + 16]
    row = lax.broadcasted_iota(jnp.int32, (8, 128), 0)
    lane_ok = lax.broadcasted_iota(jnp.int32, (8, 128), 1) < HEADS
    exponent = jnp.where(row == 0, ends[0], jnp.where(row == 1, ends[1], ends[0] + ends[1]))
    rows_of = jnp.where(row == 3, small[2:3], jnp.exp2(exponent))
    misc_ref[...] = halves(jnp.where(lane_ok, rows_of, 0.0))

    head_row = lax.broadcasted_iota(jnp.int32, (128, 1024), 0) % HEADS
    head_lane = lax.broadcasted_iota(jnp.int32, (128, 1024), 1) // HEAD_DIM
    for g in range(GROUPS):
        spread[g] = (head_row == head_lane + 16 * g).astype(F32).astype(BF16)

    def total_send(r):
        peer = (ctx + r) % 32
        return remote(misc_ref, totals.at[ctx], sems.at[0], sems.at[1], (dp, peer))

    @pl.loop(1, 32)
    def _(r):
        total_send(r).start()

    totals[ctx] = misc_ref[...]

    with jax.named_scope("halowait"):
        halo_copy.wait_recv()

    @pl.when(ctx == 0)
    def _():
        tok[:HALO] = jnp.zeros((HALO, D), BF16)

    def x_arrive(dim, p):
        x_piece(dim, p).wait_recv()
        ring_out(dim, 0, p).start()
        ring_out(dim, 1, p).start()
        forward(dim * 4 + p).start()

    def near_arrive(dim, p):
        for kind in range(2):
            ring_in(dim, kind, p).wait_recv()
            if (kind == 0) == (p < 2):
                ring_out(dim, 2, p).start()
            forward(10 + dim * 12 + kind * 4 + p).start()

    def far_arrive(dim, p):
        ring_in(dim, 2, p).wait_recv()
        forward(10 + dim * 12 + 8 + p).start()

    def direct_arrive(k):
        x_direct(k).wait_recv()
        forward(8 + k).start()

    def other_wait(pieces):
        for dim, p in pieces:
            forward(dim * 4 + p).wait_recv()
            for kind in range(3):
                forward(10 + dim * 12 + kind * 4 + p).wait_recv()

    one = ((0, 0), (1, 2))
    two = ((1, 0), (0, 2))
    three = ((0, 1), (1, 3))
    four = ((1, 1), (0, 3))

    def events(i):
        for n in range(5):
            @pl.when(i == n)
            def _(n=n):
                loc_copy(2 * n).wait()
                loc_copy(2 * n + 1).wait()

            @pl.when(i == 5 + n)
            def _(n=n):
                sib_copy(2 * n).wait_recv()
                sib_copy(2 * n + 1).wait_recv()

        def at(step, *actions):
            @pl.when(i == step)
            def _():
                for action, pieces in actions:
                    for piece in pieces:
                        action(*piece)

        def other(pieces):
            other_wait(pieces)

        at(2, (x_arrive, one))
        at(5, (x_arrive, two))
        at(7, (near_arrive, one))
        at(8, (x_arrive, three))
        at(9, (near_arrive, two))
        at(10, (x_arrive, four), (far_arrive, one))
        at(11, (near_arrive, three), (other, ((one,),)))
        at(12, (far_arrive, two))
        at(13, (near_arrive, four), (other, ((two,),)))
        at(14, (far_arrive, three))
        at(15, (other, ((three,),)))
        at(16, (far_arrive, four), (direct_arrive, ((0,), (1,))))
        at(17, (other, ((four,),)))

        @pl.when(i == 19)
        def _():
            forward(8).wait_recv()
            forward(9).wait_recv()

    def block_of(i):
        foreign = i // 10
        relation = (1 - foreign) * (i // 5) + foreign * (2 + i % 2)
        pair = (1 - foreign) * (i % 5) + foreign * (i // 2 - 5)
        lo = (dp + relation) % 2
        hi = (dp // 2 + relation // 2) % 2
        return (2 * hi + lo) * 5 + pair

    @pl.loop(0, 20)
    def _(i):
        with jax.named_scope("events"):
            events(i)
        with jax.named_scope("compute"):
            block = block_of(i)
            weights = jnp.concatenate([wbuf[2 * i], wbuf[2 * i + 1]], axis=1)
            result = jnp.dot(tok[...], weights, preferred_element_type=F32)
            result = result.astype(BF16).astype(F32)
            for side in range(2):
                pbuf[side] = result[:, side * 128 : side * 128 + 128]
            for side in range(2):
                lanes = pl.ds(pl.multiple_of(block * 256 + side * 128, 128), 128)
                taps = taps_ref[:, lanes]
                bias = fb_ref[:, lanes]
                for row in range(0, ROWS, 64):
                    at = HALO - 3 + row
                    summed = bias + taps[0:1] * pbuf[side, at : at + 64]
                    for k in range(1, 4):
                        summed = summed + taps[k : k + 1] * pbuf[side, at + k : at + k + 64]
                    half = 0.5 * summed
                    act[block, row : row + 64, side * 128 : side * 128 + 128] = (
                        half * jnp.tanh(half) + half
                    ).astype(BF16)


    def widen(value, g):
        return jnp.dot(value, spread[g], preferred_element_type=F32)

    def group_of(g, at):
        return jnp.concatenate([act[4 * g + j, at] for j in range(4)], axis=1)

    def map_lanes(g, at, base):
        return act[base + g // 2, at, pl.ds(pl.multiple_of((g % 2) * 128, 128), 128)]

    def state_send(peer, half):
        rows = slice(half * 64, half * 64 + 64)
        return remote(
            state_out.at[peer, rows], state_in.at[half, ctx],
            sems.at[2 + half], sems.at[4 + half], (dp, peer),
        )

    def enter_send(r, half):
        peer = (ctx + r) % 32
        rows = slice(half * 64, half * 64 + 64)
        return remote(
            enter_out.at[half, peer], enter_in.at[ctx, rows],
            sems.at[6 + half], sems.at[8 + half], (dp, peer),
        )

    def wait_all(part, index):
        pltpu.make_async_copy(part, part, sems.at[index]).wait()

    @pl.loop(0, GROUPS)
    @jax.named_scope("groups")
    def _(n):
        g = (n + ctx // 8) % 4
        decays = widen(misc_ref[...], g)
        total = None
        for k in range(2):
            at = slice(k * BLOCK, (k + 1) * BLOCK)
            values = group_of(g, at).astype(F32)
            scaled = (widen(w2_ref[at], g) * values).astype(BF16)
            maps = map_lanes(g, at, 16)
            state = lax.dot_general(
                maps, scaled, (((0,), (0,)), ((), ())), preferred_element_type=F32
            )
            if k == 0:
                first[g] = state
                total = decays[1:2] * state
            else:
                total = total + state
        for i in range(8):
            state_out[g * 8 + i] = total[:, i * 128 : (i + 1) * 128].astype(BF16)

        @pl.loop(0, 8)
        def _(m):
            peer = g * 8 + (m + ctx) % 8

            @pl.when(peer != ctx)
            def _():
                state_send(peer, 0).start()

    @pl.loop(1, 32)
    def _(r):
        state_send((ctx + r) % 32, 1).start()

    for half in range(2):
        state_in[half, ctx] = state_out[ctx, half * 64 : half * 64 + 64]

    lane = lax.broadcasted_iota(jnp.int32, (BLOCK, 128), 1) < HEAD_DIM
    causal = lax.broadcasted_iota(jnp.int32, (128, 128), 0) >= lax.broadcasted_iota(
        jnp.int32, (128, 128), 1
    )

    @jax.named_scope("within")
    def within(n):
        g = n // 2
        start = (n % 2) * BLOCK
        rows = pl.ds(pl.multiple_of(start, BLOCK), BLOCK)
        early = pl.ds(pl.multiple_of(start, 128), 128)
        later = pl.ds(pl.multiple_of(start + 128, 128), 128)
        full = lax.dot_general(
            map_lanes(g, rows, 18), map_lanes(g, rows, 16),
            (((1,), (1,)), ((), ())), preferred_element_type=F32,
        )
        scores[0] = jnp.where(causal, full[:128, :128], 0.0)
        scores[1] = full[128:, :128]
        scores[2] = jnp.where(causal, full[128:, 128:], 0.0)
        skip = widen(misc_ref[...], g)[3:4]
        for i in range(8):
            lanes = slice((i % 2) * 128, (i % 2) * 128 + 128)
            values = act[4 * g + i // 2, rows, lanes]
            made = []
            for h in (2 * i, 2 * i + 1):
                upper = a_ref[g, early, h : h + 1]
                under = a_ref[g, later, h : h + 1]
                b0 = bt_ref[g, h : h + 1, early]
                b1 = bt_ref[g, h : h + 1, later]
                l0 = lt_ref[g, h : h + 1, early]
                l1 = lt_ref[g, h : h + 1, later]
                w00 = (jnp.exp2(jnp.minimum(upper + b0, l0)) * scores[0]).astype(BF16)
                w10 = (jnp.exp2(under + b0) * scores[1]).astype(BF16)
                w11 = (jnp.exp2(jnp.minimum(under + b1, l1)) * scores[2]).astype(BF16)
                top = jnp.dot(w00, values[:128], preferred_element_type=F32)
                low = jnp.dot(
                    jnp.concatenate([w10, w11], axis=1), values, preferred_element_type=F32
                )
                made.append(jnp.concatenate([top, low], axis=0))
            mixed = jnp.where(lane, made[0], made[1])
            mix[g, rows, i * 128 : (i + 1) * 128] = (
                mixed + skip[:, i * 128 : (i + 1) * 128] * values.astype(F32)
            )

    pl.loop(0, 5)(within)

    with jax.named_scope("totals"):
        wait_all(totals.at[0:31], 1)
    mine = lax.broadcasted_iota(jnp.int32, (128, 128), 0) % HEADS == (
        2 * ctx + lax.broadcasted_iota(jnp.int32, (128, 128), 1) // HEAD_DIM
    )
    pick = mine.astype(F32).astype(BF16)
    for k in range(32):
        decays_in[k] = jnp.dot(totals[k], pick, preferred_element_type=F32)

    for half in range(2):
        with jax.named_scope("statewait"):
            wait_all(state_in.at[half, 0:31], 4 + half)

        def scan(k, carry):
            enter_out[half, k] = carry.astype(BF16)
            return decays_in[k, 2:3] * carry + state_in[half, k].astype(F32)

        lax.fori_loop(0, 32, scan, jnp.zeros((64, 128), F32))

        @pl.loop(1, 32)
        def _(r):
            enter_send(r, half).start()

        enter_in[ctx, half * 64 : half * 64 + 64] = enter_out[half, ctx]

        if half == 0:
            pl.loop(5, 8)(within)

    for half in range(2):
        with jax.named_scope("enterwait"):
            wait_all(enter_in.at[0:31, half * 64 : half * 64 + 64], 8 + half)

    def out_copy(g, k):
        columns = pl.ds(pl.multiple_of(g * 1024, 1024), 1024)
        rows = slice(k * BLOCK, (k + 1) * BLOCK)
        return pltpu.make_async_copy(mixed_out.at[g, rows], out_ref.at[rows, columns], out_sem)

    @pl.loop(0, GROUPS)
    @jax.named_scope("groups")
    def _(g):
        decays = widen(misc_ref[...], g)[0:1]
        for k in range(2):
            rows = slice(k * BLOCK, (k + 1) * BLOCK)
            read = map_lanes(g, rows, 18)
            for j in range(4):
                lanes = slice(j * 256, (j + 1) * 256)
                enter = jnp.concatenate(
                    [enter_in[g * 8 + 2 * j], enter_in[g * 8 + 2 * j + 1]], axis=1
                )
                if k == 1:
                    enter = decays[:, lanes] * enter.astype(F32) + first[g, :, lanes]
                    enter = enter.astype(BF16)
                carried = jnp.dot(read, enter, preferred_element_type=F32) * jnp.dot(
                    e2_ref[rows], spread[g, :, lanes], preferred_element_type=F32
                )
                mixed_out[g, rows, lanes] = (mix[g, rows, lanes] + carried).astype(BF16)
            out_copy(g, k).start()

    with jax.named_scope("drain"):
        halo_copy.wait_send()
        for dim in range(2):
            for p in range(4):
                x_piece(dim, p).wait_send()
                for kind in range(3):
                    ring_out(dim, kind, p).wait_send()
        for k in range(2):
            x_direct(k).wait_send()
        for j in range(10):
            sib_copy(j).wait_send()
        for index in range(34):
            forward(index).wait_send()
        wait_all(totals.at[0:31], 0)
        for half in range(2):
            wait_all(state_in.at[half, 0:31], 2 + half)
            wait_all(state_in.at[half, 0:31], 6 + half)
        pltpu.make_async_copy(mixed_out, mixed_out, out_sem).wait()


def mixer(tokens, in_weight, step_weight, bias, rate, skip, taps, filter_bias):
    vmem = pl.BlockSpec(memory_space=pltpu.VMEM)
    anywhere = pl.BlockSpec(memory_space=pl.ANY)
    dma = pltpu.SemaphoreType.DMA
    return pl.pallas_call(
        mixer_kernel,
        out_shape=jax.ShapeDtypeStruct((ROWS, INNER), BF16),
        in_specs=[anywhere, anywhere] + [vmem] * 6,
        out_specs=anywhere,
        scratch_shapes=[
            pltpu.VMEM((HALO + ROWS, D), BF16),
            pltpu.VMEM((40, D, 128), BF16),
            pltpu.VMEM((2, HALO + ROWS, 128), F32),
            pltpu.VMEM((20, ROWS, 256), BF16),
            pltpu.VMEM((128, D), BF16),
            pltpu.VMEM((8, 128), F32),
            pltpu.VMEM((GROUPS, ROWS, 128), F32),
            pltpu.VMEM((GROUPS, 16, ROWS), F32),
            pltpu.VMEM((GROUPS, 16, ROWS), F32),
            pltpu.VMEM((ROWS, 128), BF16),
            pltpu.VMEM((ROWS, 128), BF16),
            pltpu.VMEM((8, 128), BF16),
            pltpu.VMEM((GROUPS, 128, 1024), BF16),
            pltpu.VMEM((GROUPS, STATE, 1024), F32),
            pltpu.VMEM((GROUPS, ROWS, 1024), F32),
            pltpu.VMEM((GROUPS, ROWS, 1024), BF16),
            pltpu.VMEM((3, 128, 128), F32),
            pltpu.VMEM((32, 8, 128), BF16),
            pltpu.VMEM((32, 8, 128), F32),
            pltpu.VMEM((32, STATE, 128), BF16),
            pltpu.VMEM((2, 32, 64, 128), BF16),
            pltpu.VMEM((2, 32, 64, 128), BF16),
            pltpu.VMEM((32, STATE, 128), BF16),
            dma((10,)), dma, dma, dma((2,)), dma((10,)), dma((10,)),
            dma((10,)), dma((10,)), dma((24,)), dma((24,)), dma((34,)), dma((34,)), dma((10,)),
        ],
        compiler_params=pltpu.CompilerParams(
            collective_id=0, has_side_effects=True, vmem_limit_bytes=58 * 2**20
        ),
        name="mixer",
    )(tokens, in_weight, step_weight, bias, rate, skip, taps, filter_bias)


def norm_kernel(mixed_ref, gain_ref, out_ref):
    for g in range(GROUPS):
        columns = slice(g * 1024, (g + 1) * 1024)
        mixed = mixed_ref[:, columns].astype(F32)
        mean = jnp.mean(mixed * mixed, axis=1, keepdims=True)
        out_ref[:, columns] = (mixed * lax.rsqrt(mean + 1e-05) * gain_ref[:, columns]).astype(
            BF16
        )


def group_norm(mixed, gain):
    tile = 256
    return pl.pallas_call(
        norm_kernel,
        out_shape=jax.ShapeDtypeStruct((ROWS, INNER), BF16),
        grid=(ROWS // tile,),
        in_specs=[
            pl.BlockSpec((tile, INNER), lambda i: (i, 0)),
            pl.BlockSpec((1, INNER), lambda i: (0, 0)),
        ],
        out_specs=pl.BlockSpec((tile, INNER), lambda i: (i, 0)),
        name="group_norm",
    )(mixed, gain)


def per_device(
    tokens,
    in_weight,
    step_weight,
    step_bias,
    decay_rate,
    skip_gain,
    filter_taps,
    filter_bias,
    norm_gain,
):
    mixed = mixer(
        tokens, in_weight, step_weight.T, step_bias[None], decay_rate[None], skip_gain[None],
        filter_taps, filter_bias[None],
    )
    return group_norm(mixed, norm_gain[None])[None]


def solution(mesh):
    in_specs = (P("dp", "ctx", None), P(None, "dp"), P(), P(), P(), P(), P(), P(), P())
    out_specs = P("dp", "ctx", None)
    return jax.shard_map(
        per_device, mesh=mesh, in_specs=in_specs, out_specs=out_specs, check_vma=False
    )
```

```python
import functools

import jax
import jax.numpy as jnp
from jax import lax
from jax.experimental import pallas as pl
from jax.experimental.pallas import tpu as pltpu
from jax.sharding import PartitionSpec as P

D = 2048
HEADS = 64
HEAD_DIM = 64
STATE = 128
GROUPS = 4
BLOCK = 256
ROWS = 512
HALO = 16
SHARD = 1280
XBC = 5120
INNER = 4096
LOG2E = 1.4426950408889634
MESH = pl.DeviceIdType.MESH
F32 = jnp.float32
BF16 = jnp.bfloat16

RING_COL = ((0, 4, 3, 7), (2, 6, 1, 5))
SAME_SLOT = (10, 12, 14, 16, 18)
OTHER_SLOT = (11, 13, 15, 17, 19)
PEERS = 34


def same_slot(column):
    return 2 * SAME_SLOT[column // 2] + column % 2


def other_slot(column):
    return 2 * OTHER_SLOT[column // 2] + column % 2


def mixer_kernel(
    tok_ref, w_ref, sw_ref, bias_ref, rate_ref, skip_ref, taps_ref, fb_ref,
    out_ref,
    tok, wbuf, pbuf, act, swp, small,
    a_ref, bt_ref, lt_ref, w2_ref, e2_ref, misc_ref,
    spread, first, mix, scores, totals, decays_in,
    state_out, state_in, enter_out, enter_in,
    near_sem, tok_sem, halo_sem, sib_send,
    x_send, x_recv, ring_send, ring_recv, fwd_send, fwd_recv, sems,
):
    dp = lax.axis_index("dp")
    ctx = lax.axis_index("ctx")
    z = ctx % 4
    y = (ctx // 4) % 4
    xh = ctx // 16
    sibling = dp + 1 - 2 * (dp % 2)
    across = (dp + 2) % 4
    place = (z, y)

    def along(dim, step):
        if dim == 0:
            return xh * 16 + y * 4 + (z + step) % 4
        return xh * 16 + ((y + step) % 4) * 4 + z

    source_a = (across, ctx)
    source_b = (across, (ctx + 16) % 32)
    after = (dp, (ctx + 1) % 32)

    low, high = dp % 2, dp // 2

    def own_columns(column):
        pair = column // 2
        block = (
            (1 - low) * pair
            + low * (1 - high) * ((pair + 3) % 5)
            + low * high * (1, 2, 0, 3, 4)[pair]
        )
        return pl.ds(pl.multiple_of(block * 256 + column % 2 * 128, 128), 128)

    def loc_copy(j):
        return pltpu.make_async_copy(w_ref.at[:, own_columns(j)], wbuf.at[j], near_sem.at[j])

    barrier = pltpu.get_barrier_semaphore()
    for peer in ((sibling, ctx), source_a, source_b):
        pl.semaphore_signal(barrier, inc=1, device_id=peer, device_id_type=MESH)

    @pl.loop(1, 32)
    def _(r):
        pl.semaphore_signal(
            barrier, inc=1, device_id=(dp, (ctx + r) % 32), device_id_type=MESH
        )

    tok_copy = pltpu.make_async_copy(tok_ref.at[0], tok.at[HALO:], tok_sem)
    tok_copy.start()
    for j in range(4):
        loc_copy(j).start()

    def remote(src, dst, send, recv, peer):
        return pltpu.make_async_remote_copy(
            src_ref=src, dst_ref=dst, send_sem=send, recv_sem=recv,
            device_id=peer, device_id_type=MESH,
        )

    def x_piece(dim, p):
        column = RING_COL[dim][p]
        rows = pl.ds(pl.multiple_of(place[dim] * 512, 512), 512)
        return remote(
            w_ref.at[rows, own_columns(column)],
            wbuf.at[same_slot(column), rows],
            x_send.at[dim * 4 + p], x_recv.at[dim * 4 + p],
            source_a if p < 2 else source_b,
        )

    def x_direct(k):
        column = 8 + k
        return remote(
            w_ref.at[:, own_columns(column)],
            wbuf.at[same_slot(column)],
            x_send.at[8 + k], x_recv.at[8 + k], (source_a, source_b)[k],
        )

    def ring_rows(dim, kind, p):
        back = (3, 1, 2)[kind]
        return pl.ds(pl.multiple_of(((place[dim] + back) % 4) * 512, 512), 512)

    def ring_out(dim, kind, p):
        column = RING_COL[dim][p]
        rows = pl.ds(pl.multiple_of(place[dim] * 512, 512), 512)
        peer = along(dim, (1, 3, 1 if p < 2 else 3)[kind])
        if kind == 2:
            rows = ring_rows(dim, 0 if p < 2 else 1, p)
        at = wbuf.at[same_slot(column), rows]
        index = dim * 12 + kind * 4 + p
        return remote(at, at, ring_send.at[index], ring_recv.at[index], (dp, peer))

    def ring_in(dim, kind, p):
        column = RING_COL[dim][p]
        at = wbuf.at[same_slot(column), ring_rows(dim, kind, p)]
        index = dim * 12 + kind * 4 + p
        return remote(at, at, ring_send.at[index], ring_recv.at[index], (dp, along(dim, 1)))

    def forward(index):
        if index in (8, 9):
            src, dst = wbuf.at[same_slot(index)], wbuf.at[other_slot(index)]
        else:
            if index < 8:
                dim, p = divmod(index, 4)
                rows = pl.ds(pl.multiple_of(place[dim] * 512, 512), 512)
            else:
                dim, rest = divmod(index - 10, 12)
                kind, p = divmod(rest, 4)
                rows = ring_rows(dim, kind, p)
            column = RING_COL[dim][p]
            src = wbuf.at[same_slot(column), rows]
            dst = wbuf.at[other_slot(column), rows]
        return remote(src, dst, fwd_send.at[index], fwd_recv.at[index], (sibling, ctx))

    def sib_copy(j):
        return remote(
            w_ref.at[:, own_columns(j)], wbuf.at[10 + j],
            sib_send.at[j], near_sem.at[10 + j], (sibling, ctx),
        )

    halo_copy = remote(
        tok_ref.at[0, ROWS - HALO :], tok.at[:HALO], halo_sem.at[0], halo_sem.at[1], after
    )

    with jax.named_scope("barrier"):
        pl.semaphore_wait(barrier, PEERS)
    halo_copy.start()
    for p, q in ((0, 2), (1, 3)):
        x_piece(0, p).start()
        x_piece(1, q).start()
        x_piece(1, p).start()
        x_piece(0, q).start()
    x_direct(0).start()
    x_direct(1).start()
    for j in range(4, 10):
        loc_copy(j).start()
    for j in range(10):
        sib_copy(j).start()

    swp[...] = jnp.zeros_like(swp)
    swp[0:HEADS] = sw_ref[...]
    small[...] = jnp.zeros_like(small)
    small[0:1, 0:HEADS] = bias_ref[...]
    small[1:2, 0:HEADS] = rate_ref[...]
    small[2:3, 0:HEADS] = skip_ref[...]
    with jax.named_scope("tokwait"):
        tok_copy.wait()
    step_raw = lax.dot_general(
        tok[HALO:], swp[...], (((1,), (1,)), ((), ())), preferred_element_type=F32
    )
    step_raw = step_raw.astype(BF16).astype(F32) + small[0:1]
    step = jnp.maximum(step_raw, 0.0) + jnp.log1p(jnp.exp(-jnp.abs(step_raw)))
    keep = lax.broadcasted_iota(jnp.int32, (ROWS, 128), 1) < HEADS
    step = jnp.where(keep, step, 0.0)
    fall = step * (small[1:2] * (-LOG2E))
    lower = (
        lax.broadcasted_iota(jnp.int32, (BLOCK, BLOCK), 0)
        >= lax.broadcasted_iota(jnp.int32, (BLOCK, BLOCK), 1)
    ).astype(F32)
    level = jnp.log2(step)

    def halves(value):
        high = value.astype(BF16).astype(F32)
        low = (value - high).astype(BF16).astype(F32)
        return (high + pltpu.roll(low, 64, 1)).astype(BF16)

    ends = []
    for k in range(2):
        at = slice(k * BLOCK, (k + 1) * BLOCK)
        a = jnp.dot(
            lower, fall[at], precision=lax.Precision.HIGHEST, preferred_element_type=F32
        )
        end = a[BLOCK - 1 : BLOCK]
        ends.append(end)
        weight = jnp.where(keep[at], jnp.exp2(end - a) * step[at], 0.0)
        w2_ref[at] = halves(weight)
        e2_ref[at] = halves(jnp.where(keep[at], jnp.exp2(a), 0.0))
        turned = jnp.transpose(level[at] - a)
        turned_level = jnp.transpose(level[at])
        for g in range(GROUPS):
            a_ref[g, at] = a if g == 0 else pltpu.roll(a, 128 - 16 * g, 1)
            bt_ref[g, :, at] = turned[16 * g : 16 * g + 16]
            lt_ref[g, :, at] = turned_level[16 * g : 16 * g + 16]
    row = lax.broadcasted_iota(jnp.int32, (8, 128), 0)
    lane_ok = lax.broadcasted_iota(jnp.int32, (8, 128), 1) < HEADS
    exponent = jnp.where(row == 0, ends[0], jnp.where(row == 1, ends[1], ends[0] + ends[1]))
    rows_of = jnp.where(row == 3, small[2:3], jnp.exp2(exponent))
    misc_ref[...] = halves(jnp.where(lane_ok, rows_of, 0.0))

    head_row = lax.broadcasted_iota(jnp.int32, (128, 1024), 0) % HEADS
    head_lane = lax.broadcasted_iota(jnp.int32, (128, 1024), 1) // HEAD_DIM
    for g in range(GROUPS):
        spread[g] = (head_row == head_lane + 16 * g).astype(F32).astype(BF16)

    def total_send(r):
        peer = (ctx + r) % 32
        return remote(misc_ref, totals.at[ctx], sems.at[0], sems.at[1], (dp, peer))

    @pl.loop(1, 32)
    def _(r):
        total_send(r).start()

    totals[ctx] = misc_ref[...]

    with jax.named_scope("halowait"):
        halo_copy.wait_recv()

    @pl.when(ctx == 0)
    def _():
        tok[:HALO] = jnp.zeros((HALO, D), BF16)

    def x_arrive(dim, p):
        x_piece(dim, p).wait_recv()
        ring_out(dim, 0, p).start()
        ring_out(dim, 1, p).start()
        forward(dim * 4 + p).start()

    def near_arrive(dim, p):
        for kind in range(2):
            ring_in(dim, kind, p).wait_recv()
            if (kind == 0) == (p < 2):
                ring_out(dim, 2, p).start()
            forward(10 + dim * 12 + kind * 4 + p).start()

    def far_arrive(dim, p):
        ring_in(dim, 2, p).wait_recv()
        forward(10 + dim * 12 + 8 + p).start()

    def direct_arrive(k):
        x_direct(k).wait_recv()
        forward(8 + k).start()

    def other_wait(pieces):
        for dim, p in pieces:
            forward(dim * 4 + p).wait_recv()
            for kind in range(3):
                forward(10 + dim * 12 + kind * 4 + p).wait_recv()

    one = ((0, 0), (1, 2))
    two = ((1, 0), (0, 2))
    three = ((0, 1), (1, 3))
    four = ((1, 1), (0, 3))

    def at(i, step, *actions):
        @pl.when(i == step)
        def _():
            for action, pieces in actions:
                for piece in pieces:
                    action(*piece)

    def other(pieces):
        other_wait(pieces)

    def near_events(i):
        for j in (2 * i, 2 * i + 1):
            pltpu.make_async_copy(wbuf.at[j], wbuf.at[j], near_sem.at[j]).wait()
        at(i, 2, (x_arrive, one))
        at(i, 5, (x_arrive, two))
        at(i, 7, (near_arrive, one))
        at(i, 8, (x_arrive, three))
        at(i, 9, (near_arrive, two))

    def early_events(i):
        at(i, 10, (x_arrive, four), (far_arrive, one))
        at(i, 11, (near_arrive, three), (other, ((one,),)))
        at(i, 12, (far_arrive, two))
        at(i, 13, (near_arrive, four), (other, ((two,),)))

    def late_events(i):
        at(i, 14, (far_arrive, three))
        at(i, 15, (other, ((three,),)))
        at(i, 16, (far_arrive, four), (direct_arrive, ((0,), (1,))))
        at(i, 17, (other, ((four,),)))

        @pl.when(i == 19)
        def _():
            forward(8).wait_recv()
            forward(9).wait_recv()

    def block_of(i):
        foreign = i // 10
        relation = (1 - foreign) * (i // 5) + foreign * (2 + i % 2)
        pair = (1 - foreign) * (i % 5) + foreign * (i // 2 - 5)
        slow = (low + relation) % 2
        shigh = (high + relation // 2) % 2
        late = pair // 3
        block = (
            (1 - slow) * pair
            + slow * (1 - shigh) * ((pair + 3) % 5)
            + slow * shigh * (late * pair + (1 - late) * ((pair + 1) % 3))
        )
        return (2 * shigh + slow) * 5 + block

    def project(events, i):
        with jax.named_scope("events"):
            events(i)
        with jax.named_scope("compute"):
            block = block_of(i)
            weights = jnp.concatenate([wbuf[2 * i], wbuf[2 * i + 1]], axis=1)
            result = jnp.dot(tok[...], weights, preferred_element_type=F32)
            result = result.astype(BF16).astype(F32)
            for side in range(2):
                pbuf[side] = result[:, side * 128 : side * 128 + 128]
            for side in range(2):
                lanes = pl.ds(pl.multiple_of(block * 256 + side * 128, 128), 128)
                taps = taps_ref[:, lanes]
                bias = fb_ref[:, lanes]
                for row in range(0, ROWS, 64):
                    at = HALO - 3 + row
                    summed = bias + taps[0:1] * pbuf[side, at : at + 64]
                    for k in range(1, 4):
                        summed = summed + taps[k : k + 1] * pbuf[side, at + k : at + k + 64]
                    half = 0.5 * summed
                    act[block, row : row + 64, side * 128 : side * 128 + 128] = (
                        half * jnp.tanh(half) + half
                    ).astype(BF16)


    def widen(value, g):
        return jnp.dot(value, spread[g], preferred_element_type=F32)

    def group_of(g, at):
        return jnp.concatenate([act[4 * g + j, at] for j in range(4)], axis=1)

    def map_lanes(g, at, base):
        return act[base + g // 2, at, pl.ds(pl.multiple_of((g % 2) * 128, 128), 128)]

    def group_at(stage, m):
        return (1 - high) * (2 * stage + m) + high * (m if stage else 3 - m)

    def state_send(peer, stage):
        return remote(
            state_out.at[stage, peer], state_in.at[stage, ctx],
            sems.at[2 + stage], sems.at[4 + stage], (dp, peer),
        )

    def enter_send(r, stage):
        peer = (ctx + r) % 32
        rows = pl.ds(pl.multiple_of((ctx % 2) * 64, 64), 64)
        return remote(
            enter_out.at[stage, peer], enter_in.at[stage * 16 + ctx // 2, rows],
            sems.at[6 + stage], sems.at[8 + stage], (dp, peer),
        )

    def wait_all(part, index):
        pltpu.make_async_copy(part, part, sems.at[index]).wait()

    def states(stage):
        @pl.loop(0, 2)
        @jax.named_scope("states")
        def _(n):
            m = (n + xh) % 2
            g = group_at(stage, m)
            decays = widen(misc_ref[...], g)
            total = None
            for k in range(2):
                at = slice(k * BLOCK, (k + 1) * BLOCK)
                values = group_of(g, at).astype(F32)
                scaled = (widen(w2_ref[at], g) * values).astype(BF16)
                maps = map_lanes(g, at, 16)
                state = lax.dot_general(
                    maps, scaled, (((0,), (0,)), ((), ())), preferred_element_type=F32
                )
                if k == 0:
                    first[g] = state
                    total = decays[1:2] * state
                else:
                    total = total + state
            for i in range(8):
                for half in range(2):
                    state_out[stage, 16 * m + 2 * i + half] = total[
                        half * 64 : half * 64 + 64, i * 128 : (i + 1) * 128
                    ].astype(BF16)

            @pl.loop(0, 16)
            def _(j):
                peer = 16 * m + (j + ctx) % 16

                @pl.when(peer != ctx)
                def _():
                    state_send(peer, stage).start()

        state_in[stage, ctx] = state_out[stage, ctx]

    pl.loop(0, 10)(functools.partial(project, near_events))
    pl.loop(10, 14)(functools.partial(project, early_events))
    states(0)
    pl.loop(14, 20)(functools.partial(project, late_events))
    states(1)

    lane = lax.broadcasted_iota(jnp.int32, (BLOCK, 128), 1) < HEAD_DIM
    causal = lax.broadcasted_iota(jnp.int32, (128, 128), 0) >= lax.broadcasted_iota(
        jnp.int32, (128, 128), 1
    )

    @jax.named_scope("within")
    def within(n):
        g = n // 2
        start = (n % 2) * BLOCK
        rows = pl.ds(pl.multiple_of(start, BLOCK), BLOCK)
        early = pl.ds(pl.multiple_of(start, 128), 128)
        later = pl.ds(pl.multiple_of(start + 128, 128), 128)
        full = lax.dot_general(
            map_lanes(g, rows, 18), map_lanes(g, rows, 16),
            (((1,), (1,)), ((), ())), preferred_element_type=F32,
        )
        scores[0] = jnp.where(causal, full[:128, :128], 0.0)
        scores[1] = full[128:, :128]
        scores[2] = jnp.where(causal, full[128:, 128:], 0.0)
        skip = widen(misc_ref[...], g)[3:4]
        for i in range(8):
            lanes = slice((i % 2) * 128, (i % 2) * 128 + 128)
            values = act[4 * g + i // 2, rows, lanes]
            made = []
            for h in (2 * i, 2 * i + 1):
                upper = a_ref[g, early, h : h + 1]
                under = a_ref[g, later, h : h + 1]
                b0 = bt_ref[g, h : h + 1, early]
                b1 = bt_ref[g, h : h + 1, later]
                l0 = lt_ref[g, h : h + 1, early]
                l1 = lt_ref[g, h : h + 1, later]
                w00 = (jnp.exp2(jnp.minimum(upper + b0, l0)) * scores[0]).astype(BF16)
                w10 = (jnp.exp2(under + b0) * scores[1]).astype(BF16)
                w11 = (jnp.exp2(jnp.minimum(under + b1, l1)) * scores[2]).astype(BF16)
                top = jnp.dot(w00, values[:128], preferred_element_type=F32)
                low = jnp.dot(
                    jnp.concatenate([w10, w11], axis=1), values, preferred_element_type=F32
                )
                made.append(jnp.concatenate([top, low], axis=0))
            mixed = jnp.where(lane, made[0], made[1])
            mix[g, rows, i * 128 : (i + 1) * 128] = (
                mixed + skip[:, i * 128 : (i + 1) * 128] * values.astype(F32)
            )

    def turn(stage):
        group = group_at(stage, ctx // 16)
        head = 16 * group + 2 * (ctx // 2 % 8)
        mine = lax.broadcasted_iota(jnp.int32, (128, 128), 0) % HEADS == (
            head + lax.broadcasted_iota(jnp.int32, (128, 128), 1) // HEAD_DIM
        )
        pick = mine.astype(F32).astype(BF16)
        for k in range(32):
            decays_in[k] = jnp.dot(totals[k], pick, preferred_element_type=F32)
        with jax.named_scope("statewait"):
            wait_all(state_in.at[stage, 0:31], 4 + stage)

        def scan(k, carry):
            enter_out[stage, k] = carry.astype(BF16)
            return decays_in[k, 2:3] * carry + state_in[stage, k].astype(F32)

        lax.fori_loop(0, 32, scan, jnp.zeros((64, 128), F32))

        @pl.loop(1, 32)
        def _(r):
            enter_send(r, stage).start()

        rows = pl.ds(pl.multiple_of((ctx % 2) * 64, 64), 64)
        enter_in[stage * 16 + ctx // 2, rows] = enter_out[stage, ctx]

    wait_all(totals.at[0:31], 1)
    turn(0)
    pl.loop(0, 6)(within)
    turn(1)
    pl.loop(6, 8)(within)

    for stage in range(2):
        with jax.named_scope("enterwait"):
            wait_all(enter_in.at[0:31, 0:64], 8 + stage)

        @pl.loop(0, 2)
        @jax.named_scope("groups")
        def _(m):
            g = group_at(stage, m)
            decays = widen(misc_ref[...], g)[0:1]
            for k in range(2):
                rows = slice(k * BLOCK, (k + 1) * BLOCK)
                read = map_lanes(g, rows, 18)
                for j in range(4):
                    lanes = slice(j * 256, (j + 1) * 256)
                    pair = stage * 16 + 8 * m + 2 * j
                    enter = jnp.concatenate([enter_in[pair], enter_in[pair + 1]], axis=1)
                    if k == 1:
                        enter = decays[:, lanes] * enter.astype(F32) + first[g, :, lanes]
                        enter = enter.astype(BF16)
                    carried = jnp.dot(read, enter, preferred_element_type=F32) * jnp.dot(
                        e2_ref[rows], spread[g, :, lanes], preferred_element_type=F32
                    )
                    columns = pl.ds(pl.multiple_of(g * 1024 + j * 256, 256), 256)
                    out_ref[rows, columns] = (mix[g, rows, lanes] + carried).astype(BF16)

    with jax.named_scope("drain"):
        halo_copy.wait_send()
        for dim in range(2):
            for p in range(4):
                x_piece(dim, p).wait_send()
                for kind in range(3):
                    ring_out(dim, kind, p).wait_send()
        for k in range(2):
            x_direct(k).wait_send()
        for j in range(10):
            sib_copy(j).wait_send()
        for index in range(34):
            forward(index).wait_send()
        wait_all(totals.at[0:31], 0)
        for half in range(2):
            wait_all(state_in.at[half, 0:31], 2 + half)
            wait_all(state_in.at[half, 0:31], 6 + half)


def mixer(tokens, in_weight, step_weight, bias, rate, skip, taps, filter_bias):
    vmem = pl.BlockSpec(memory_space=pltpu.VMEM)
    anywhere = pl.BlockSpec(memory_space=pl.ANY)
    dma = pltpu.SemaphoreType.DMA
    return pl.pallas_call(
        mixer_kernel,
        out_shape=pltpu.VMEM((ROWS, INNER), BF16),
        in_specs=[anywhere, anywhere] + [vmem] * 6,
        out_specs=vmem,
        scratch_shapes=[
            pltpu.VMEM((HALO + ROWS, D), BF16),
            pltpu.VMEM((40, D, 128), BF16),
            pltpu.VMEM((2, HALO + ROWS, 128), F32),
            pltpu.VMEM((20, ROWS, 256), BF16),
            pltpu.VMEM((128, D), BF16),
            pltpu.VMEM((8, 128), F32),
            pltpu.VMEM((GROUPS, ROWS, 128), F32),
            pltpu.VMEM((GROUPS, 16, ROWS), F32),
            pltpu.VMEM((GROUPS, 16, ROWS), F32),
            pltpu.VMEM((ROWS, 128), BF16),
            pltpu.VMEM((ROWS, 128), BF16),
            pltpu.VMEM((8, 128), BF16),
            pltpu.VMEM((GROUPS, 128, 1024), BF16),
            pltpu.VMEM((GROUPS, STATE, 1024), F32),
            pltpu.VMEM((GROUPS, ROWS, 1024), F32),
            pltpu.VMEM((3, 128, 128), F32),
            pltpu.VMEM((32, 8, 128), BF16),
            pltpu.VMEM((32, 8, 128), F32),
            pltpu.VMEM((2, 32, 64, 128), BF16),
            pltpu.VMEM((2, 32, 64, 128), BF16),
            pltpu.VMEM((2, 32, 64, 128), BF16),
            pltpu.VMEM((32, STATE, 128), BF16),
            dma((20,)), dma, dma((2,)), dma((10,)),
            dma((10,)), dma((10,)), dma((24,)), dma((24,)), dma((34,)), dma((34,)), dma((10,)),
        ],
        compiler_params=pltpu.CompilerParams(
            collective_id=0, has_side_effects=True, vmem_limit_bytes=54 * 2**20
        ),
        name="mixer",
    )(tokens, in_weight, step_weight, bias, rate, skip, taps, filter_bias)


def norm_kernel(mixed_ref, gain_ref, out_ref, rows_out, sem):
    tile = 64

    def copy(n):
        rows = slice(n * tile, (n + 1) * tile)
        return pltpu.make_async_copy(rows_out.at[rows], out_ref.at[rows], sem.at[n])

    for n in range(ROWS // tile):
        rows = slice(n * tile, (n + 1) * tile)
        for g in range(GROUPS):
            columns = slice(g * 1024, (g + 1) * 1024)
            mixed = mixed_ref[rows, columns].astype(F32)
            mean = jnp.mean(mixed * mixed, axis=1, keepdims=True)
            normed = mixed * lax.rsqrt(mean + 1e-05) * gain_ref[:, columns]
            rows_out[rows, columns] = normed.astype(BF16)
        copy(n).start()
    for n in range(ROWS // tile):
        copy(n).wait()


def group_norm(mixed, gain):
    vmem = pl.BlockSpec(memory_space=pltpu.VMEM)
    return pl.pallas_call(
        norm_kernel,
        out_shape=jax.ShapeDtypeStruct((ROWS, INNER), BF16),
        in_specs=[vmem, vmem],
        out_specs=pl.BlockSpec(memory_space=pl.ANY),
        scratch_shapes=[pltpu.VMEM((ROWS, INNER), BF16), pltpu.SemaphoreType.DMA((8,))],
        compiler_params=pltpu.CompilerParams(vmem_limit_bytes=24 * 2**20),
        name="group_norm",
    )(mixed, gain)


def per_device(
    tokens,
    in_weight,
    step_weight,
    step_bias,
    decay_rate,
    skip_gain,
    filter_taps,
    filter_bias,
    norm_gain,
):
    mixed = mixer(
        tokens, in_weight, step_weight.T, step_bias[None], decay_rate[None], skip_gain[None],
        filter_taps, filter_bias[None],
    )
    return group_norm(mixed, norm_gain[None])[None]


def solution(mesh):
    in_specs = (P("dp", "ctx", None), P(None, "dp"), P(), P(), P(), P(), P(), P(), P())
    out_specs = P("dp", "ctx", None)
    return jax.shard_map(
        per_device, mesh=mesh, in_specs=in_specs, out_specs=out_specs, check_vma=False
    )
```

```python
import functools

import jax
import jax.numpy as jnp
from jax import lax
from jax.experimental import pallas as pl
from jax.experimental.pallas import tpu as pltpu
from jax.sharding import PartitionSpec as P

D = 2048
HEADS = 64
HEAD_DIM = 64
STATE = 128
GROUPS = 4
BLOCK = 256
ROWS = 512
HALO = 16
SHARD = 1280
XBC = 5120
INNER = 4096
LOG2E = 1.4426950408889634
MESH = pl.DeviceIdType.MESH
F32 = jnp.float32
BF16 = jnp.bfloat16

RING_COL = ((0, 4, 3, 7), (2, 6, 1, 5))
SAME_SLOT = (10, 12, 14, 16, 18)
OTHER_SLOT = (11, 13, 15, 17, 19)
PEERS = 34


def same_slot(column):
    return 2 * SAME_SLOT[column // 2] + column % 2


def other_slot(column):
    return 2 * OTHER_SLOT[column // 2] + column % 2


def mixer_kernel(
    tok_ref, w_ref, sw_ref, bias_ref, rate_ref, skip_ref, taps_ref, fb_ref,
    out_ref,
    tok, wbuf, pbuf, act, swp, small,
    a_ref, bt_ref, lt_ref, w2_ref, e2_ref, misc_ref,
    spread, first, mix, scores, totals, decays_in,
    out_0, out_1, out_2, in_0, in_1, in_2, back_0, back_1, back_2, enter_in,
    near_sem, tok_sem, halo_sem, sib_send,
    x_send, x_recv, ring_send, ring_recv, fwd_send, fwd_recv, sems,
):
    dp = lax.axis_index("dp")
    ctx = lax.axis_index("ctx")
    z = ctx % 4
    y = (ctx // 4) % 4
    xh = ctx // 16
    sibling = dp + 1 - 2 * (dp % 2)
    across = (dp + 2) % 4
    place = (z, y)

    def along(dim, step):
        if dim == 0:
            return xh * 16 + y * 4 + (z + step) % 4
        return xh * 16 + ((y + step) % 4) * 4 + z

    source_a = (across, ctx)
    source_b = (across, (ctx + 16) % 32)
    after = (dp, (ctx + 1) % 32)

    low, high = dp % 2, dp // 2

    def own_columns(column):
        pair = column // 2
        block = (
            (1 - low) * pair
            + low * (1 - high) * ((pair + 3) % 5)
            + low * high * (1, 2, 0, 3, 4)[pair]
        )
        return pl.ds(pl.multiple_of(block * 256 + column % 2 * 128, 128), 128)

    def loc_copy(j):
        return pltpu.make_async_copy(w_ref.at[:, own_columns(j)], wbuf.at[j], near_sem.at[j])

    barrier = pltpu.get_barrier_semaphore()
    for peer in ((sibling, ctx), source_a, source_b):
        pl.semaphore_signal(barrier, inc=1, device_id=peer, device_id_type=MESH)

    @pl.loop(1, 32)
    def _(r):
        pl.semaphore_signal(
            barrier, inc=1, device_id=(dp, (ctx + r) % 32), device_id_type=MESH
        )

    tok_copy = pltpu.make_async_copy(tok_ref.at[0], tok.at[HALO:], tok_sem)
    tok_copy.start()
    for j in range(4):
        loc_copy(j).start()

    def remote(src, dst, send, recv, peer):
        return pltpu.make_async_remote_copy(
            src_ref=src, dst_ref=dst, send_sem=send, recv_sem=recv,
            device_id=peer, device_id_type=MESH,
        )

    def x_piece(dim, p):
        column = RING_COL[dim][p]
        rows = pl.ds(pl.multiple_of(place[dim] * 512, 512), 512)
        return remote(
            w_ref.at[rows, own_columns(column)],
            wbuf.at[same_slot(column), rows],
            x_send.at[dim * 4 + p], x_recv.at[dim * 4 + p],
            source_a if p < 2 else source_b,
        )

    def x_direct(k):
        column = 8 + k
        return remote(
            w_ref.at[:, own_columns(column)],
            wbuf.at[same_slot(column)],
            x_send.at[8 + k], x_recv.at[8 + k], (source_a, source_b)[k],
        )

    def ring_rows(dim, kind, p):
        back = (3, 1, 2)[kind]
        return pl.ds(pl.multiple_of(((place[dim] + back) % 4) * 512, 512), 512)

    def ring_out(dim, kind, p):
        column = RING_COL[dim][p]
        rows = pl.ds(pl.multiple_of(place[dim] * 512, 512), 512)
        peer = along(dim, (1, 3, 1 if p < 2 else 3)[kind])
        if kind == 2:
            rows = ring_rows(dim, 0 if p < 2 else 1, p)
        at = wbuf.at[same_slot(column), rows]
        index = dim * 12 + kind * 4 + p
        return remote(at, at, ring_send.at[index], ring_recv.at[index], (dp, peer))

    def ring_in(dim, kind, p):
        column = RING_COL[dim][p]
        at = wbuf.at[same_slot(column), ring_rows(dim, kind, p)]
        index = dim * 12 + kind * 4 + p
        return remote(at, at, ring_send.at[index], ring_recv.at[index], (dp, along(dim, 1)))

    def forward(index):
        if index in (8, 9):
            src, dst = wbuf.at[same_slot(index)], wbuf.at[other_slot(index)]
        else:
            if index < 8:
                dim, p = divmod(index, 4)
                rows = pl.ds(pl.multiple_of(place[dim] * 512, 512), 512)
            else:
                dim, rest = divmod(index - 10, 12)
                kind, p = divmod(rest, 4)
                rows = ring_rows(dim, kind, p)
            column = RING_COL[dim][p]
            src = wbuf.at[same_slot(column), rows]
            dst = wbuf.at[other_slot(column), rows]
        return remote(src, dst, fwd_send.at[index], fwd_recv.at[index], (sibling, ctx))

    def sib_copy(j):
        return remote(
            w_ref.at[:, own_columns(j)], wbuf.at[10 + j],
            sib_send.at[j], near_sem.at[10 + j], (sibling, ctx),
        )

    halo_copy = remote(
        tok_ref.at[0, ROWS - HALO :], tok.at[:HALO], halo_sem.at[0], halo_sem.at[1], after
    )

    with jax.named_scope("barrier"):
        pl.semaphore_wait(barrier, PEERS)
    halo_copy.start()
    for p, q in ((0, 2), (1, 3)):
        x_piece(0, p).start()
        x_piece(1, q).start()
        x_piece(1, p).start()
        x_piece(0, q).start()
    x_direct(0).start()
    x_direct(1).start()
    for j in range(4, 10):
        loc_copy(j).start()
    for j in range(10):
        sib_copy(j).start()

    swp[...] = jnp.zeros_like(swp)
    swp[0:HEADS] = sw_ref[...]
    small[...] = jnp.zeros_like(small)
    small[0:1, 0:HEADS] = bias_ref[...]
    small[1:2, 0:HEADS] = rate_ref[...]
    small[2:3, 0:HEADS] = skip_ref[...]
    with jax.named_scope("tokwait"):
        tok_copy.wait()
    step_raw = lax.dot_general(
        tok[HALO:], swp[...], (((1,), (1,)), ((), ())), preferred_element_type=F32
    )
    step_raw = step_raw.astype(BF16).astype(F32) + small[0:1]
    step = jnp.maximum(step_raw, 0.0) + jnp.log1p(jnp.exp(-jnp.abs(step_raw)))
    keep = lax.broadcasted_iota(jnp.int32, (ROWS, 128), 1) < HEADS
    step = jnp.where(keep, step, 0.0)
    fall = step * (small[1:2] * (-LOG2E))
    lower = (
        lax.broadcasted_iota(jnp.int32, (BLOCK, BLOCK), 0)
        >= lax.broadcasted_iota(jnp.int32, (BLOCK, BLOCK), 1)
    ).astype(F32)
    level = jnp.log2(step)

    def halves(value):
        high = value.astype(BF16).astype(F32)
        low = (value - high).astype(BF16).astype(F32)
        return (high + pltpu.roll(low, 64, 1)).astype(BF16)

    ends = []
    for k in range(2):
        at = slice(k * BLOCK, (k + 1) * BLOCK)
        a = jnp.dot(
            lower, fall[at], precision=lax.Precision.HIGHEST, preferred_element_type=F32
        )
        end = a[BLOCK - 1 : BLOCK]
        ends.append(end)
        weight = jnp.where(keep[at], jnp.exp2(end - a) * step[at], 0.0)
        w2_ref[at] = halves(weight)
        e2_ref[at] = halves(jnp.where(keep[at], jnp.exp2(a), 0.0))
        turned = jnp.transpose(level[at] - a)
        turned_level = jnp.transpose(level[at])
        for g in range(GROUPS):
            a_ref[g, at] = a if g == 0 else pltpu.roll(a, 128 - 16 * g, 1)
            bt_ref[g, :, at] = turned[16 * g : 16 * g + 16]
            lt_ref[g, :, at] = turned_level[16 * g : 16 * g + 16]
    row = lax.broadcasted_iota(jnp.int32, (8, 128), 0)
    lane_ok = lax.broadcasted_iota(jnp.int32, (8, 128), 1) < HEADS
    exponent = jnp.where(row == 0, ends[0], jnp.where(row == 1, ends[1], ends[0] + ends[1]))
    rows_of = jnp.where(row == 3, small[2:3], jnp.exp2(exponent))
    misc_ref[...] = halves(jnp.where(lane_ok, rows_of, 0.0))

    head_row = lax.broadcasted_iota(jnp.int32, (128, 1024), 0) % HEADS
    head_lane = lax.broadcasted_iota(jnp.int32, (128, 1024), 1) // HEAD_DIM
    for g in range(GROUPS):
        spread[g] = (head_row == head_lane + 16 * g).astype(F32).astype(BF16)

    def total_send(r):
        peer = (ctx + r) % 32
        return remote(misc_ref, totals.at[ctx], sems.at[0], sems.at[1], (dp, peer))

    @pl.loop(1, 32)
    def _(r):
        total_send(r).start()

    totals[ctx] = misc_ref[...]

    with jax.named_scope("halowait"):
        halo_copy.wait_recv()

    @pl.when(ctx == 0)
    def _():
        tok[:HALO] = jnp.zeros((HALO, D), BF16)

    def x_arrive(dim, p):
        x_piece(dim, p).wait_recv()
        ring_out(dim, 0, p).start()
        ring_out(dim, 1, p).start()
        forward(dim * 4 + p).start()

    def near_arrive(dim, p):
        for kind in range(2):
            ring_in(dim, kind, p).wait_recv()
            if (kind == 0) == (p < 2):
                ring_out(dim, 2, p).start()
            forward(10 + dim * 12 + kind * 4 + p).start()

    def far_arrive(dim, p):
        ring_in(dim, 2, p).wait_recv()
        forward(10 + dim * 12 + 8 + p).start()

    def direct_arrive(k):
        x_direct(k).wait_recv()
        forward(8 + k).start()

    def other_wait(pieces):
        for dim, p in pieces:
            forward(dim * 4 + p).wait_recv()
            for kind in range(3):
                forward(10 + dim * 12 + kind * 4 + p).wait_recv()

    one = ((0, 0), (1, 2))
    two = ((1, 0), (0, 2))
    three = ((0, 1), (1, 3))
    four = ((1, 1), (0, 3))

    def at(i, step, *actions):
        @pl.when(i == step)
        def _():
            for action, pieces in actions:
                for piece in pieces:
                    action(*piece)

    def other(pieces):
        other_wait(pieces)

    def near_events(i):
        for j in (2 * i, 2 * i + 1):
            pltpu.make_async_copy(wbuf.at[j], wbuf.at[j], near_sem.at[j]).wait()
        at(i, 2, (x_arrive, one))
        at(i, 5, (x_arrive, two))
        at(i, 7, (near_arrive, one))
        at(i, 8, (x_arrive, three))
        at(i, 9, (near_arrive, two))

    def early_events(i):
        at(i, 10, (x_arrive, four), (far_arrive, one))
        at(i, 11, (other, ((one,),)))
        at(i, 12, (far_arrive, two), (near_arrive, three))
        at(i, 13, (near_arrive, four), (other, ((two,),)))

    def late_events(i):
        at(i, 14, (far_arrive, three))
        at(i, 15, (other, ((three,),)))
        at(i, 16, (far_arrive, four), (direct_arrive, ((0,), (1,))))
        at(i, 17, (other, ((four,),)))

    def last_events(i):
        @pl.when(i == 19)
        def _():
            forward(8).wait_recv()
            forward(9).wait_recv()

    def block_of(i):
        foreign = i // 10
        relation = (1 - foreign) * (i // 5) + foreign * (2 + i % 2)
        pair = (1 - foreign) * (i % 5) + foreign * (i // 2 - 5)
        slow = (low + relation) % 2
        shigh = (high + relation // 2) % 2
        late = pair // 3
        block = (
            (1 - slow) * pair
            + slow * (1 - shigh) * ((pair + 3) % 5)
            + slow * shigh * (late * pair + (1 - late) * ((pair + 1) % 3))
        )
        return (2 * shigh + slow) * 5 + block

    def project(events, i):
        with jax.named_scope("events"):
            events(i)
        with jax.named_scope("compute"):
            block = block_of(i)
            weights = jnp.concatenate([wbuf[2 * i], wbuf[2 * i + 1]], axis=1)
            result = jnp.dot(tok[...], weights, preferred_element_type=F32)
            result = result.astype(BF16).astype(F32)
            for side in range(2):
                pbuf[side] = result[:, side * 128 : side * 128 + 128]
            for side in range(2):
                lanes = pl.ds(pl.multiple_of(block * 256 + side * 128, 128), 128)
                taps = taps_ref[:, lanes]
                bias = fb_ref[:, lanes]
                for row in range(0, ROWS, 64):
                    at = HALO - 3 + row
                    summed = bias + taps[0:1] * pbuf[side, at : at + 64]
                    for k in range(1, 4):
                        summed = summed + taps[k : k + 1] * pbuf[side, at + k : at + k + 64]
                    half = 0.5 * summed
                    act[block, row : row + 64, side * 128 : side * 128 + 128] = (
                        half * jnp.tanh(half) + half
                    ).astype(BF16)


    def widen(value, g):
        return jnp.dot(value, spread[g], preferred_element_type=F32)

    def group_of(g, at):
        return jnp.concatenate([act[4 * g + j, at] for j in range(4)], axis=1)

    def map_lanes(g, at, base):
        return act[base + g // 2, at, pl.ds(pl.multiple_of((g % 2) * 128, 128), 128)]

    state_out, state_in, enter_out = (out_0, out_1, out_2), (in_0, in_1, in_2), (back_0, back_1, back_2)
    parts, begin = (2, 4, 4), (0, 16, 24)

    def group_at(stage, m):
        if stage == 0:
            return (1 - high) * m + high * (3 - m)
        return (1 - high) * (1 + stage) + high * (stage - 1)

    def state_send(peer, stage):
        return remote(
            state_out[stage].at[peer], state_in[stage].at[ctx],
            sems.at[2 + stage], sems.at[5 + stage], (dp, peer),
        )

    def my_place(stage):
        size = STATE // parts[stage]
        rows = pl.ds(pl.multiple_of(ctx % parts[stage] * size, size), size)
        return begin[stage] + ctx // parts[stage], rows

    def enter_send(r, stage):
        peer = (ctx + r) % 32
        pair, rows = my_place(stage)
        return remote(
            enter_out[stage].at[peer], enter_in.at[pair, rows],
            sems.at[8 + stage], sems.at[11 + stage], (dp, peer),
        )

    def wait_all(part, index):
        pltpu.make_async_copy(part, part, sems.at[index]).wait()

    def states(stage):
        groups = 1 if stage else 2
        owners = 32 // groups
        size = STATE // parts[stage]

        @pl.loop(0, groups)
        @jax.named_scope("states")
        def _(n):
            m = (n + xh) % groups
            g = group_at(stage, m)
            decays = widen(misc_ref[...], g)
            total = None
            for k in range(2):
                at = slice(k * BLOCK, (k + 1) * BLOCK)
                values = group_of(g, at).astype(F32)
                scaled = (widen(w2_ref[at], g) * values).astype(BF16)
                maps = map_lanes(g, at, 16)
                state = lax.dot_general(
                    maps, scaled, (((0,), (0,)), ((), ())), preferred_element_type=F32
                )
                if k == 0:
                    first[g] = state
                    total = decays[1:2] * state
                else:
                    total = total + state
            for i in range(8):
                for part in range(parts[stage]):
                    state_out[stage][owners * m + parts[stage] * i + part] = total[
                        part * size : part * size + size, i * 128 : (i + 1) * 128
                    ].astype(BF16)

            @pl.loop(0, owners)
            def _(j):
                peer = owners * m + (j + ctx) % owners

                @pl.when(peer != ctx)
                def _():
                    state_send(peer, stage).start()

        state_in[stage][ctx] = state_out[stage][ctx]

    pl.loop(0, 10)(functools.partial(project, near_events))
    pl.loop(10, 14)(functools.partial(project, early_events))
    states(0)
    pl.loop(14, 18)(functools.partial(project, late_events))
    states(1)
    pl.loop(18, 20)(functools.partial(project, last_events))
    states(2)

    lane = lax.broadcasted_iota(jnp.int32, (BLOCK, 128), 1) < HEAD_DIM
    causal = lax.broadcasted_iota(jnp.int32, (128, 128), 0) >= lax.broadcasted_iota(
        jnp.int32, (128, 128), 1
    )

    @jax.named_scope("within")
    def within(n):
        g = n // 2
        start = (n % 2) * BLOCK
        rows = pl.ds(pl.multiple_of(start, BLOCK), BLOCK)
        early = pl.ds(pl.multiple_of(start, 128), 128)
        later = pl.ds(pl.multiple_of(start + 128, 128), 128)
        full = lax.dot_general(
            map_lanes(g, rows, 18), map_lanes(g, rows, 16),
            (((1,), (1,)), ((), ())), preferred_element_type=F32,
        )
        scores[0] = jnp.where(causal, full[:128, :128], 0.0)
        scores[1] = full[128:, :128]
        scores[2] = jnp.where(causal, full[128:, 128:], 0.0)
        skip = widen(misc_ref[...], g)[3:4]
        for i in range(8):
            lanes = slice((i % 2) * 128, (i % 2) * 128 + 128)
            values = act[4 * g + i // 2, rows, lanes]
            made = []
            for h in (2 * i, 2 * i + 1):
                upper = a_ref[g, early, h : h + 1]
                under = a_ref[g, later, h : h + 1]
                b0 = bt_ref[g, h : h + 1, early]
                b1 = bt_ref[g, h : h + 1, later]
                l0 = lt_ref[g, h : h + 1, early]
                l1 = lt_ref[g, h : h + 1, later]
                w00 = (jnp.exp2(jnp.minimum(upper + b0, l0)) * scores[0]).astype(BF16)
                w10 = (jnp.exp2(under + b0) * scores[1]).astype(BF16)
                w11 = (jnp.exp2(jnp.minimum(under + b1, l1)) * scores[2]).astype(BF16)
                top = jnp.dot(w00, values[:128], preferred_element_type=F32)
                low = jnp.dot(
                    jnp.concatenate([w10, w11], axis=1), values, preferred_element_type=F32
                )
                made.append(jnp.concatenate([top, low], axis=0))
            mixed = jnp.where(lane, made[0], made[1])
            mix[g, rows, i * 128 : (i + 1) * 128] = (
                mixed + skip[:, i * 128 : (i + 1) * 128] * values.astype(F32)
            )

    def turn(stage):
        pair, rows = my_place(stage)
        pair = pair - begin[stage]
        head = 16 * group_at(stage, pair // 8) + 2 * (pair % 8)
        mine = lax.broadcasted_iota(jnp.int32, (128, 128), 0) % HEADS == (
            head + lax.broadcasted_iota(jnp.int32, (128, 128), 1) // HEAD_DIM
        )
        pick = mine.astype(F32).astype(BF16)
        for k in range(32):
            decays_in[k] = jnp.dot(totals[k], pick, preferred_element_type=F32)
        with jax.named_scope("statewait"):
            wait_all(state_in[stage].at[0:31], 5 + stage)

        def scan(k, carry):
            enter_out[stage][k] = carry.astype(BF16)
            return decays_in[k, 2:3] * carry + state_in[stage][k].astype(F32)

        lax.fori_loop(0, 32, scan, jnp.zeros((STATE // parts[stage], 128), F32))

        @pl.loop(1, 32)
        def _(r):
            enter_send(r, stage).start()

        enter_in[begin[stage] + pair, rows] = enter_out[stage][ctx]

    wait_all(totals.at[0:31], 1)
    turn(0)
    pl.loop(0, 2)(within)
    turn(1)
    pl.loop(2, 5)(within)
    turn(2)
    pl.loop(5, 8)(within)

    for stage in range(3):
        with jax.named_scope("enterwait"):
            wait_all(enter_in.at[0:31, 0 : STATE // parts[stage]], 11 + stage)

        @pl.loop(0, 1 if stage else 2)
        @jax.named_scope("groups")
        def _(m):
            g = group_at(stage, m)
            decays = widen(misc_ref[...], g)[0:1]
            for k in range(2):
                rows = slice(k * BLOCK, (k + 1) * BLOCK)
                read = map_lanes(g, rows, 18)
                for j in range(4):
                    lanes = slice(j * 256, (j + 1) * 256)
                    pair = begin[stage] + 8 * m + 2 * j
                    enter = jnp.concatenate([enter_in[pair], enter_in[pair + 1]], axis=1)
                    if k == 1:
                        enter = decays[:, lanes] * enter.astype(F32) + first[g, :, lanes]
                        enter = enter.astype(BF16)
                    carried = jnp.dot(read, enter, preferred_element_type=F32) * jnp.dot(
                        e2_ref[rows], spread[g, :, lanes], preferred_element_type=F32
                    )
                    columns = pl.ds(pl.multiple_of(g * 1024 + j * 256, 256), 256)
                    out_ref[rows, columns] = (mix[g, rows, lanes] + carried).astype(BF16)

    with jax.named_scope("drain"):
        halo_copy.wait_send()
        for dim in range(2):
            for p in range(4):
                x_piece(dim, p).wait_send()
                for kind in range(3):
                    ring_out(dim, kind, p).wait_send()
        for k in range(2):
            x_direct(k).wait_send()
        for j in range(10):
            sib_copy(j).wait_send()
        for index in range(34):
            forward(index).wait_send()
        wait_all(totals.at[0:31], 0)
        for stage in range(3):
            wait_all(state_in[stage].at[0:31], 2 + stage)
            wait_all(state_in[stage].at[0:31], 8 + stage)


def mixer(tokens, in_weight, step_weight, bias, rate, skip, taps, filter_bias):
    vmem = pl.BlockSpec(memory_space=pltpu.VMEM)
    anywhere = pl.BlockSpec(memory_space=pl.ANY)
    dma = pltpu.SemaphoreType.DMA
    return pl.pallas_call(
        mixer_kernel,
        out_shape=pltpu.VMEM((ROWS, INNER), BF16),
        in_specs=[anywhere, anywhere] + [vmem] * 6,
        out_specs=vmem,
        scratch_shapes=[
            pltpu.VMEM((HALO + ROWS, D), BF16),
            pltpu.VMEM((40, D, 128), BF16),
            pltpu.VMEM((2, HALO + ROWS, 128), F32),
            pltpu.VMEM((20, ROWS, 256), BF16),
            pltpu.VMEM((128, D), BF16),
            pltpu.VMEM((8, 128), F32),
            pltpu.VMEM((GROUPS, ROWS, 128), F32),
            pltpu.VMEM((GROUPS, 16, ROWS), F32),
            pltpu.VMEM((GROUPS, 16, ROWS), F32),
            pltpu.VMEM((ROWS, 128), BF16),
            pltpu.VMEM((ROWS, 128), BF16),
            pltpu.VMEM((8, 128), BF16),
            pltpu.VMEM((GROUPS, 128, 1024), BF16),
            pltpu.VMEM((GROUPS, STATE, 1024), F32),
            pltpu.VMEM((GROUPS, ROWS, 1024), F32),
            pltpu.VMEM((3, 128, 128), F32),
            pltpu.VMEM((32, 8, 128), BF16),
            pltpu.VMEM((32, 8, 128), F32),
            *[pltpu.VMEM((32, rows, 128), BF16) for rows in (64, 32, 32) * 3],
            pltpu.VMEM((32, STATE, 128), BF16),
            dma((20,)), dma, dma((2,)), dma((10,)),
            dma((10,)), dma((10,)), dma((24,)), dma((24,)), dma((34,)), dma((34,)), dma((14,)),
        ],
        compiler_params=pltpu.CompilerParams(
            collective_id=0, has_side_effects=True, vmem_limit_bytes=54 * 2**20
        ),
        name="mixer",
    )(tokens, in_weight, step_weight, bias, rate, skip, taps, filter_bias)


def norm_kernel(mixed_ref, gain_ref, out_ref, rows_out, sem):
    tile = 64

    def copy(n):
        rows = slice(n * tile, (n + 1) * tile)
        return pltpu.make_async_copy(rows_out.at[rows], out_ref.at[rows], sem.at[n])

    for n in range(ROWS // tile):
        rows = slice(n * tile, (n + 1) * tile)
        for g in range(GROUPS):
            columns = slice(g * 1024, (g + 1) * 1024)
            mixed = mixed_ref[rows, columns].astype(F32)
            mean = jnp.mean(mixed * mixed, axis=1, keepdims=True)
            normed = mixed * lax.rsqrt(mean + 1e-05) * gain_ref[:, columns]
            rows_out[rows, columns] = normed.astype(BF16)
        copy(n).start()
    for n in range(ROWS // tile):
        copy(n).wait()


def group_norm(mixed, gain):
    vmem = pl.BlockSpec(memory_space=pltpu.VMEM)
    return pl.pallas_call(
        norm_kernel,
        out_shape=jax.ShapeDtypeStruct((ROWS, INNER), BF16),
        in_specs=[vmem, vmem],
        out_specs=pl.BlockSpec(memory_space=pl.ANY),
        scratch_shapes=[pltpu.VMEM((ROWS, INNER), BF16), pltpu.SemaphoreType.DMA((8,))],
        compiler_params=pltpu.CompilerParams(vmem_limit_bytes=24 * 2**20),
        name="group_norm",
    )(mixed, gain)


def per_device(
    tokens,
    in_weight,
    step_weight,
    step_bias,
    decay_rate,
    skip_gain,
    filter_taps,
    filter_bias,
    norm_gain,
):
    mixed = mixer(
        tokens, in_weight, step_weight.T, step_bias[None], decay_rate[None], skip_gain[None],
        filter_taps, filter_bias[None],
    )
    return group_norm(mixed, norm_gain[None])[None]


def solution(mesh):
    in_specs = (P("dp", "ctx", None), P(None, "dp"), P(), P(), P(), P(), P(), P(), P())
    out_specs = P("dp", "ctx", None)
    return jax.shard_map(
        per_device, mesh=mesh, in_specs=in_specs, out_specs=out_specs, check_vma=False
    )
```

```python
import functools

import jax
import jax.numpy as jnp
from jax import lax
from jax.experimental import pallas as pl
from jax.experimental.pallas import tpu as pltpu
from jax.sharding import PartitionSpec as P

D = 2048
HEADS = 64
HEAD_DIM = 64
STATE = 128
GROUPS = 4
BLOCK = 256
ROWS = 512
HALO = 16
SHARD = 1280
XBC = 5120
INNER = 4096
LOG2E = 1.4426950408889634
MESH = pl.DeviceIdType.MESH
F32 = jnp.float32
BF16 = jnp.bfloat16

RING_COL = ((0, 4, 3, 9), (2, 8, 1, 5))
DIRECT_COL = 6
SAME_SLOT = (10, 12, 14, 16, 18)
OTHER_SLOT = (11, 13, 15, 17, 19)
PEERS = 34


def same_slot(column):
    return 2 * SAME_SLOT[column // 2] + column % 2


def other_slot(column):
    return 2 * OTHER_SLOT[column // 2] + column % 2


def mixer_kernel(
    tok_ref, w_ref, sw_hbm, bias_hbm, rate_hbm, skip_hbm, taps_hbm, fb_hbm,
    out_ref,
    taps_ref, fb_ref, bias_ref, rate_ref, skip_ref,
    tok, wbuf, pbuf, act, swp, small,
    a_ref, bt_ref, lt_ref, w2_ref, e2_ref, misc_ref,
    spread, first, mix, scores, totals, decays_in,
    out_0, out_1, out_2, in_0, in_1, in_2, back_0, back_1, back_2, enter_in,
    near_sem, tok_sem, small_sem, halo_sem, sib_send,
    x_send, x_recv, ring_send, ring_recv, fwd_send, fwd_recv, sems,
):
    dp = lax.axis_index("dp")
    ctx = lax.axis_index("ctx")
    z = ctx % 4
    y = (ctx // 4) % 4
    xh = ctx // 16
    sibling = dp + 1 - 2 * (dp % 2)
    across = (dp + 2) % 4
    place = (z, y)

    def along(dim, step):
        if dim == 0:
            return xh * 16 + y * 4 + (z + step) % 4
        return xh * 16 + ((y + step) % 4) * 4 + z

    source_a = (across, ctx)
    source_b = (across, (ctx + 16) % 32)
    after = (dp, (ctx + 1) % 32)

    low, high = dp % 2, dp // 2

    def own_columns(column):
        pair = column // 2
        block = (
            (1 - low) * pair
            + low * (1 - high) * ((pair + 3) % 5)
            + low * high * (1, 2, 0, 3, 4)[pair]
        )
        return pl.ds(pl.multiple_of(block * 256 + column % 2 * 128, 128), 128)

    def loc_copy(j):
        return pltpu.make_async_copy(w_ref.at[:, own_columns(j)], wbuf.at[j], near_sem.at[j])

    loc_copy(0).start()
    loc_copy(1).start()
    barrier = pltpu.get_barrier_semaphore()
    for peer in ((sibling, ctx), source_a, source_b):
        pl.semaphore_signal(barrier, inc=1, device_id=peer, device_id_type=MESH)

    @pl.loop(1, 32)
    def _(r):
        pl.semaphore_signal(
            barrier, inc=1, device_id=(dp, (ctx + r) % 32), device_id_type=MESH
        )

    tok_copy = pltpu.make_async_copy(tok_ref.at[0], tok.at[HALO:], tok_sem)
    tok_copy.start()
    small_copies = [
        pltpu.make_async_copy(src, dst, small_sem.at[n])
        for n, (src, dst) in enumerate((
            (sw_hbm, swp.at[0:HEADS]), (bias_hbm, bias_ref), (rate_hbm, rate_ref),
            (skip_hbm, skip_ref), (taps_hbm, taps_ref), (fb_hbm, fb_ref),
        ))
    ]
    for copy in small_copies:
        copy.start()
    for j in range(2, 4):
        loc_copy(j).start()

    def remote(src, dst, send, recv, peer):
        return pltpu.make_async_remote_copy(
            src_ref=src, dst_ref=dst, send_sem=send, recv_sem=recv,
            device_id=peer, device_id_type=MESH,
        )

    def x_piece(dim, p):
        column = RING_COL[dim][p]
        rows = pl.ds(pl.multiple_of(place[dim] * 512, 512), 512)
        own = w_ref.at[rows, own_columns(column)] if column > 1 else wbuf.at[column, rows]
        return remote(
            own,
            wbuf.at[same_slot(column), rows],
            x_send.at[dim * 4 + p], x_recv.at[dim * 4 + p],
            source_a if p < 2 else source_b,
        )

    def x_direct(k):
        column = DIRECT_COL + k
        return remote(
            w_ref.at[:, own_columns(column)],
            wbuf.at[same_slot(column)],
            x_send.at[8 + k], x_recv.at[8 + k], (source_a, source_b)[k],
        )

    def ring_rows(dim, kind, p):
        back = (3, 1, 2)[kind]
        return pl.ds(pl.multiple_of(((place[dim] + back) % 4) * 512, 512), 512)

    def ring_out(dim, kind, p):
        column = RING_COL[dim][p]
        rows = pl.ds(pl.multiple_of(place[dim] * 512, 512), 512)
        peer = along(dim, (1, 3, 1 if p < 2 else 3)[kind])
        if kind == 2:
            rows = ring_rows(dim, 0 if p < 2 else 1, p)
        at = wbuf.at[same_slot(column), rows]
        index = dim * 12 + kind * 4 + p
        return remote(at, at, ring_send.at[index], ring_recv.at[index], (dp, peer))

    def ring_in(dim, kind, p):
        column = RING_COL[dim][p]
        at = wbuf.at[same_slot(column), ring_rows(dim, kind, p)]
        index = dim * 12 + kind * 4 + p
        return remote(at, at, ring_send.at[index], ring_recv.at[index], (dp, along(dim, 1)))

    def forward(index):
        if index in (8, 9):
            column = DIRECT_COL + index - 8
            src, dst = wbuf.at[same_slot(column)], wbuf.at[other_slot(column)]
        else:
            if index < 8:
                dim, p = divmod(index, 4)
                rows = pl.ds(pl.multiple_of(place[dim] * 512, 512), 512)
            else:
                dim, rest = divmod(index - 10, 12)
                kind, p = divmod(rest, 4)
                rows = ring_rows(dim, kind, p)
            column = RING_COL[dim][p]
            src = wbuf.at[same_slot(column), rows]
            dst = wbuf.at[other_slot(column), rows]
        return remote(src, dst, fwd_send.at[index], fwd_recv.at[index], (sibling, ctx))

    def sib_copy(j):
        return remote(
            w_ref.at[:, own_columns(j)], wbuf.at[10 + j],
            sib_send.at[j], near_sem.at[10 + j], (sibling, ctx),
        )

    halo_copy = remote(
        tok_ref.at[0, ROWS - HALO :], tok.at[:HALO], halo_sem.at[0], halo_sem.at[1], after
    )

    with jax.named_scope("barrier"):
        pl.semaphore_wait(barrier, PEERS)
    halo_copy.start()
    loc_copy(0).wait()
    loc_copy(1).wait()
    for p, q in ((0, 2), (1, 3)):
        x_piece(0, p).start()
        x_piece(1, q).start()
        x_piece(1, p).start()
        x_piece(0, q).start()
    x_direct(0).start()
    x_direct(1).start()
    for j in range(4, 10):
        loc_copy(j).start()
    for j in range(10):
        sib_copy(j).start()

    swp[HEADS:] = jnp.zeros((128 - HEADS, D), BF16)
    for copy in small_copies:
        copy.wait()
    small[...] = jnp.zeros_like(small)
    small[0:1, 0:HEADS] = bias_ref[...]
    small[1:2, 0:HEADS] = rate_ref[...]
    small[2:3, 0:HEADS] = skip_ref[...]
    with jax.named_scope("tokwait"):
        tok_copy.wait()
    step_raw = lax.dot_general(
        tok[HALO:], swp[...], (((1,), (1,)), ((), ())), preferred_element_type=F32
    )
    step_raw = step_raw.astype(BF16).astype(F32) + small[0:1]
    step = jnp.maximum(step_raw, 0.0) + jnp.log1p(jnp.exp(-jnp.abs(step_raw)))
    keep = lax.broadcasted_iota(jnp.int32, (ROWS, 128), 1) < HEADS
    step = jnp.where(keep, step, 0.0)
    fall = step * (small[1:2] * (-LOG2E))
    lower = (
        lax.broadcasted_iota(jnp.int32, (BLOCK, BLOCK), 0)
        >= lax.broadcasted_iota(jnp.int32, (BLOCK, BLOCK), 1)
    ).astype(F32)
    level = jnp.log2(step)

    def halves(value):
        high = value.astype(BF16).astype(F32)
        low = (value - high).astype(BF16).astype(F32)
        return (high + pltpu.roll(low, 64, 1)).astype(BF16)

    ends = []
    for k in range(2):
        at = slice(k * BLOCK, (k + 1) * BLOCK)
        a = jnp.dot(
            lower, fall[at], precision=lax.Precision.HIGHEST, preferred_element_type=F32
        )
        end = a[BLOCK - 1 : BLOCK]
        ends.append(end)
        weight = jnp.where(keep[at], jnp.exp2(end - a) * step[at], 0.0)
        w2_ref[at] = halves(weight)
        e2_ref[at] = halves(jnp.where(keep[at], jnp.exp2(a), 0.0))
        turned = jnp.transpose(level[at] - a)
        turned_level = jnp.transpose(level[at])
        for g in range(GROUPS):
            a_ref[g, at] = a if g == 0 else pltpu.roll(a, 128 - 16 * g, 1)
            bt_ref[g, :, at] = turned[16 * g : 16 * g + 16]
            lt_ref[g, :, at] = turned_level[16 * g : 16 * g + 16]
    row = lax.broadcasted_iota(jnp.int32, (8, 128), 0)
    lane_ok = lax.broadcasted_iota(jnp.int32, (8, 128), 1) < HEADS
    exponent = jnp.where(row == 0, ends[0], jnp.where(row == 1, ends[1], ends[0] + ends[1]))
    rows_of = jnp.where(row == 3, small[2:3], jnp.exp2(exponent))
    misc_ref[...] = halves(jnp.where(lane_ok, rows_of, 0.0))

    head_row = lax.broadcasted_iota(jnp.int32, (128, 1024), 0) % HEADS
    head_lane = lax.broadcasted_iota(jnp.int32, (128, 1024), 1) // HEAD_DIM
    for g in range(GROUPS):
        spread[g] = (head_row == head_lane + 16 * g).astype(F32).astype(BF16)

    def total_send(r):
        peer = (ctx + r) % 32
        return remote(misc_ref, totals.at[ctx], sems.at[0], sems.at[1], (dp, peer))

    @pl.loop(1, 32)
    def _(r):
        total_send(r).start()

    totals[ctx] = misc_ref[...]

    with jax.named_scope("halowait"):
        halo_copy.wait_recv()

    @pl.when(ctx == 0)
    def _():
        tok[:HALO] = jnp.zeros((HALO, D), BF16)

    def x_arrive(dim, p):
        x_piece(dim, p).wait_recv()
        ring_out(dim, 0, p).start()
        ring_out(dim, 1, p).start()
        forward(dim * 4 + p).start()

    def near_arrive(dim, p):
        for kind in range(2):
            ring_in(dim, kind, p).wait_recv()
            if (kind == 0) == (p < 2):
                ring_out(dim, 2, p).start()
            forward(10 + dim * 12 + kind * 4 + p).start()

    def far_arrive(dim, p):
        ring_in(dim, 2, p).wait_recv()
        forward(10 + dim * 12 + 8 + p).start()

    def direct_arrive(k):
        x_direct(k).wait_recv()
        forward(8 + k).start()

    def other_wait(pieces):
        for dim, p in pieces:
            forward(dim * 4 + p).wait_recv()
            for kind in range(3):
                forward(10 + dim * 12 + kind * 4 + p).wait_recv()

    one = ((0, 0), (1, 2))
    two = ((1, 0), (0, 2))
    three = ((0, 1), (1, 3))
    four = ((1, 1), (0, 3))

    def at(i, step, *actions):
        @pl.when(i == step)
        def _():
            for action, pieces in actions:
                for piece in pieces:
                    action(*piece)

    def other(pieces):
        other_wait(pieces)

    def other_direct(index):
        forward(index).wait_recv()

    def near_events(i):
        @pl.when(i > 0)
        def _():
            for j in (2 * i, 2 * i + 1):
                pltpu.make_async_copy(wbuf.at[j], wbuf.at[j], near_sem.at[j]).wait()

        at(i, 2, (x_arrive, one))
        at(i, 5, (x_arrive, two))
        at(i, 7, (near_arrive, one))
        at(i, 8, (x_arrive, three))
        at(i, 9, (near_arrive, two))

    def early_events(i):
        at(i, 10, (x_arrive, four), (far_arrive, one))
        at(i, 11, (other, ((one,),)))
        at(i, 12, (far_arrive, two), (near_arrive, three))
        at(i, 13, (near_arrive, four), (other, ((two,),)))

    def late_events(i):
        at(i, 14, (far_arrive, three))
        at(i, 15, (direct_arrive, ((0,), (1,))), (other, ((three,),)))
        at(i, 17, (other_direct, ((8,), (9,))))

    def last_events(i):
        at(i, 18, (far_arrive, four))
        at(i, 19, (other, ((four,),)))

    def block_of(i):
        foreign = i // 10
        relation = (1 - foreign) * (i // 5) + foreign * (2 + i % 2)
        pair = (1 - foreign) * (i % 5) + foreign * (i // 2 - 5)
        slow = (low + relation) % 2
        shigh = (high + relation // 2) % 2
        late = pair // 3
        block = (
            (1 - slow) * pair
            + slow * (1 - shigh) * ((pair + 3) % 5)
            + slow * shigh * (late * pair + (1 - late) * ((pair + 1) % 3))
        )
        return (2 * shigh + slow) * 5 + block

    def project(events, i):
        with jax.named_scope("events"):
            events(i)
        with jax.named_scope("compute"):
            block = block_of(i)
            weights = jnp.concatenate([wbuf[2 * i], wbuf[2 * i + 1]], axis=1)
            result = jnp.dot(tok[...], weights, preferred_element_type=F32)
            result = result.astype(BF16).astype(F32)
            for side in range(2):
                pbuf[side] = result[:, side * 128 : side * 128 + 128]
            for side in range(2):
                lanes = pl.ds(pl.multiple_of(block * 256 + side * 128, 128), 128)
                taps = taps_ref[:, lanes]
                bias = fb_ref[:, lanes]
                for row in range(0, ROWS, 64):
                    at = HALO - 3 + row
                    summed = bias + taps[0:1] * pbuf[side, at : at + 64]
                    for k in range(1, 4):
                        summed = summed + taps[k : k + 1] * pbuf[side, at + k : at + k + 64]
                    half = 0.5 * summed
                    act[block, row : row + 64, side * 128 : side * 128 + 128] = (
                        half * jnp.tanh(half) + half
                    ).astype(BF16)


    def widen(value, g):
        return jnp.dot(value, spread[g], preferred_element_type=F32)

    def group_of(g, at):
        return jnp.concatenate([act[4 * g + j, at] for j in range(4)], axis=1)

    def map_lanes(g, at, base):
        return act[base + g // 2, at, pl.ds(pl.multiple_of((g % 2) * 128, 128), 128)]

    state_out, state_in, enter_out = (out_0, out_1, out_2), (in_0, in_1, in_2), (back_0, back_1, back_2)
    parts, begin = (2, 4, 4), (0, 16, 24)

    def group_at(stage, m):
        if stage == 0:
            return (1 - high) * m + high * (3 - m)
        return (1 - high) * (1 + stage) + high * (stage - 1)

    def state_send(peer, stage):
        return remote(
            state_out[stage].at[peer], state_in[stage].at[ctx],
            sems.at[2 + stage], sems.at[5 + stage], (dp, peer),
        )

    def my_place(stage):
        size = STATE // parts[stage]
        rows = pl.ds(pl.multiple_of(ctx % parts[stage] * size, size), size)
        return begin[stage] + ctx // parts[stage], rows

    def enter_send(r, stage):
        peer = (ctx + r) % 32
        pair, rows = my_place(stage)
        return remote(
            enter_out[stage].at[peer], enter_in.at[pair, rows],
            sems.at[8 + stage], sems.at[11 + stage], (dp, peer),
        )

    def wait_all(part, index):
        pltpu.make_async_copy(part, part, sems.at[index]).wait()

    def states(stage):
        groups = 1 if stage else 2
        owners = 32 // groups
        size = STATE // parts[stage]

        @pl.loop(0, groups)
        @jax.named_scope("states")
        def _(n):
            m = (n + xh) % groups
            g = group_at(stage, m)
            decays = widen(misc_ref[...], g)
            total = None
            for k in range(2):
                at = slice(k * BLOCK, (k + 1) * BLOCK)
                values = group_of(g, at).astype(F32)
                scaled = (widen(w2_ref[at], g) * values).astype(BF16)
                maps = map_lanes(g, at, 16)
                state = lax.dot_general(
                    maps, scaled, (((0,), (0,)), ((), ())), preferred_element_type=F32
                )
                if k == 0:
                    first[g] = state
                    total = decays[1:2] * state
                else:
                    total = total + state
            for i in range(8):
                for part in range(parts[stage]):
                    state_out[stage][owners * m + parts[stage] * i + part] = total[
                        part * size : part * size + size, i * 128 : (i + 1) * 128
                    ].astype(BF16)

            @pl.loop(0, owners)
            def _(j):
                peer = owners * m + (j + ctx) % owners

                @pl.when(peer != ctx)
                def _():
                    state_send(peer, stage).start()

        state_in[stage][ctx] = state_out[stage][ctx]

    pl.loop(0, 10)(functools.partial(project, near_events))
    pl.loop(10, 14)(functools.partial(project, early_events))
    states(0)
    pl.loop(14, 18)(functools.partial(project, late_events))
    states(1)
    pl.loop(18, 20)(functools.partial(project, last_events))
    states(2)

    lane = lax.broadcasted_iota(jnp.int32, (BLOCK, 128), 1) < HEAD_DIM
    causal = lax.broadcasted_iota(jnp.int32, (128, 128), 0) >= lax.broadcasted_iota(
        jnp.int32, (128, 128), 1
    )

    @jax.named_scope("within")
    def within(n):
        g = n // 2
        start = (n % 2) * BLOCK
        rows = pl.ds(pl.multiple_of(start, BLOCK), BLOCK)
        early = pl.ds(pl.multiple_of(start, 128), 128)
        later = pl.ds(pl.multiple_of(start + 128, 128), 128)
        full = lax.dot_general(
            map_lanes(g, rows, 18), map_lanes(g, rows, 16),
            (((1,), (1,)), ((), ())), preferred_element_type=F32,
        )
        scores[0] = jnp.where(causal, full[:128, :128], 0.0)
        scores[1] = full[128:, :128]
        scores[2] = jnp.where(causal, full[128:, 128:], 0.0)
        skip = widen(misc_ref[...], g)[3:4]
        for i in range(8):
            lanes = slice((i % 2) * 128, (i % 2) * 128 + 128)
            values = act[4 * g + i // 2, rows, lanes]
            made = []
            for h in (2 * i, 2 * i + 1):
                upper = a_ref[g, early, h : h + 1]
                under = a_ref[g, later, h : h + 1]
                b0 = bt_ref[g, h : h + 1, early]
                b1 = bt_ref[g, h : h + 1, later]
                l0 = lt_ref[g, h : h + 1, early]
                l1 = lt_ref[g, h : h + 1, later]
                w00 = (jnp.exp2(jnp.minimum(upper + b0, l0)) * scores[0]).astype(BF16)
                w10 = (jnp.exp2(under + b0) * scores[1]).astype(BF16)
                w11 = (jnp.exp2(jnp.minimum(under + b1, l1)) * scores[2]).astype(BF16)
                top = jnp.dot(w00, values[:128], preferred_element_type=F32)
                low = jnp.dot(
                    jnp.concatenate([w10, w11], axis=1), values, preferred_element_type=F32
                )
                made.append(jnp.concatenate([top, low], axis=0))
            mixed = jnp.where(lane, made[0], made[1])
            mix[g, rows, i * 128 : (i + 1) * 128] = (
                mixed + skip[:, i * 128 : (i + 1) * 128] * values.astype(F32)
            )

    def turn(stage):
        pair, rows = my_place(stage)
        pair = pair - begin[stage]
        head = 16 * group_at(stage, pair // 8) + 2 * (pair % 8)
        mine = lax.broadcasted_iota(jnp.int32, (128, 128), 0) % HEADS == (
            head + lax.broadcasted_iota(jnp.int32, (128, 128), 1) // HEAD_DIM
        )
        pick = mine.astype(F32).astype(BF16)
        for k in range(32):
            decays_in[k] = jnp.dot(totals[k], pick, preferred_element_type=F32)
        with jax.named_scope("statewait"):
            wait_all(state_in[stage].at[0:31], 5 + stage)

        def scan(k, carry):
            enter_out[stage][k] = carry.astype(BF16)
            return decays_in[k, 2:3] * carry + state_in[stage][k].astype(F32)

        lax.fori_loop(0, 32, scan, jnp.zeros((STATE // parts[stage], 128), F32))

        @pl.loop(1, 32)
        def _(r):
            enter_send(r, stage).start()

        enter_in[begin[stage] + pair, rows] = enter_out[stage][ctx]

    wait_all(totals.at[0:31], 1)
    turn(0)
    pl.loop(0, 4)(within)
    turn(1)
    pl.loop(4, 5)(within)
    turn(2)
    pl.loop(5, 8)(within)

    for stage in range(3):
        with jax.named_scope("enterwait"):
            wait_all(enter_in.at[0:31, 0 : STATE // parts[stage]], 11 + stage)

        @pl.loop(0, 1 if stage else 2)
        @jax.named_scope("groups")
        def _(m):
            g = group_at(stage, m)
            decays = widen(misc_ref[...], g)[0:1]
            for k in range(2):
                rows = slice(k * BLOCK, (k + 1) * BLOCK)
                read = map_lanes(g, rows, 18)
                for j in range(4):
                    lanes = slice(j * 256, (j + 1) * 256)
                    pair = begin[stage] + 8 * m + 2 * j
                    enter = jnp.concatenate([enter_in[pair], enter_in[pair + 1]], axis=1)
                    if k == 1:
                        enter = decays[:, lanes] * enter.astype(F32) + first[g, :, lanes]
                        enter = enter.astype(BF16)
                    carried = jnp.dot(read, enter, preferred_element_type=F32) * jnp.dot(
                        e2_ref[rows], spread[g, :, lanes], preferred_element_type=F32
                    )
                    columns = pl.ds(pl.multiple_of(g * 1024 + j * 256, 256), 256)
                    out_ref[rows, columns] = (mix[g, rows, lanes] + carried).astype(BF16)

    with jax.named_scope("drain"):
        halo_copy.wait_send()
        for dim in range(2):
            for p in range(4):
                x_piece(dim, p).wait_send()
                for kind in range(3):
                    ring_out(dim, kind, p).wait_send()
        for k in range(2):
            x_direct(k).wait_send()
        for j in range(10):
            sib_copy(j).wait_send()
        for index in range(34):
            forward(index).wait_send()
        wait_all(totals.at[0:31], 0)
        for stage in range(3):
            wait_all(state_in[stage].at[0:31], 2 + stage)
            wait_all(state_in[stage].at[0:31], 8 + stage)


def mixer(tokens, in_weight, step_weight, bias, rate, skip, taps, filter_bias):
    vmem = pl.BlockSpec(memory_space=pltpu.VMEM)
    anywhere = pl.BlockSpec(memory_space=pl.ANY)
    dma = pltpu.SemaphoreType.DMA
    return pl.pallas_call(
        mixer_kernel,
        out_shape=pltpu.VMEM((ROWS, INNER), BF16),
        in_specs=[anywhere] * 8,
        out_specs=vmem,
        scratch_shapes=[
            pltpu.VMEM((4, XBC), F32),
            pltpu.VMEM((1, XBC), F32),
            *[pltpu.VMEM((1, HEADS), F32) for _ in range(3)],
            pltpu.VMEM((HALO + ROWS, D), BF16),
            pltpu.VMEM((40, D, 128), BF16),
            pltpu.VMEM((2, HALO + ROWS, 128), F32),
            pltpu.VMEM((20, ROWS, 256), BF16),
            pltpu.VMEM((128, D), BF16),
            pltpu.VMEM((8, 128), F32),
            pltpu.VMEM((GROUPS, ROWS, 128), F32),
            pltpu.VMEM((GROUPS, 16, ROWS), F32),
            pltpu.VMEM((GROUPS, 16, ROWS), F32),
            pltpu.VMEM((ROWS, 128), BF16),
            pltpu.VMEM((ROWS, 128), BF16),
            pltpu.VMEM((8, 128), BF16),
            pltpu.VMEM((GROUPS, 128, 1024), BF16),
            pltpu.VMEM((GROUPS, STATE, 1024), F32),
            pltpu.VMEM((GROUPS, ROWS, 1024), F32),
            pltpu.VMEM((3, 128, 128), F32),
            pltpu.VMEM((32, 8, 128), BF16),
            pltpu.VMEM((32, 8, 128), F32),
            *[pltpu.VMEM((32, rows, 128), BF16) for rows in (64, 32, 32) * 3],
            pltpu.VMEM((32, STATE, 128), BF16),
            dma((20,)), dma, dma((6,)), dma((2,)), dma((10,)),
            dma((10,)), dma((10,)), dma((24,)), dma((24,)), dma((34,)), dma((34,)), dma((14,)),
        ],
        compiler_params=pltpu.CompilerParams(
            collective_id=0, has_side_effects=True, vmem_limit_bytes=54 * 2**20
        ),
        name="mixer",
    )(tokens, in_weight, step_weight, bias, rate, skip, taps, filter_bias)


def norm_kernel(mixed_ref, gain_ref, out_ref, rows_out, sem):
    tile = 64

    def copy(n):
        rows = slice(n * tile, (n + 1) * tile)
        return pltpu.make_async_copy(rows_out.at[rows], out_ref.at[rows], sem.at[n])

    for n in range(ROWS // tile):
        rows = slice(n * tile, (n + 1) * tile)
        for g in range(GROUPS):
            columns = slice(g * 1024, (g + 1) * 1024)
            mixed = mixed_ref[rows, columns].astype(F32)
            mean = jnp.mean(mixed * mixed, axis=1, keepdims=True)
            normed = mixed * lax.rsqrt(mean + 1e-05) * gain_ref[:, columns]
            rows_out[rows, columns] = normed.astype(BF16)
        copy(n).start()
    for n in range(ROWS // tile):
        copy(n).wait()


def group_norm(mixed, gain):
    vmem = pl.BlockSpec(memory_space=pltpu.VMEM)
    return pl.pallas_call(
        norm_kernel,
        out_shape=jax.ShapeDtypeStruct((ROWS, INNER), BF16),
        in_specs=[vmem, vmem],
        out_specs=pl.BlockSpec(memory_space=pl.ANY),
        scratch_shapes=[pltpu.VMEM((ROWS, INNER), BF16), pltpu.SemaphoreType.DMA((8,))],
        compiler_params=pltpu.CompilerParams(vmem_limit_bytes=24 * 2**20),
        name="group_norm",
    )(mixed, gain)


def per_device(
    tokens,
    in_weight,
    step_weight,
    step_bias,
    decay_rate,
    skip_gain,
    filter_taps,
    filter_bias,
    norm_gain,
):
    mixed = mixer(
        tokens, in_weight, step_weight.T, step_bias[None], decay_rate[None], skip_gain[None],
        filter_taps, filter_bias[None],
    )
    return group_norm(mixed, norm_gain[None])[None]


def solution(mesh):
    in_specs = (P("dp", "ctx", None), P(None, "dp"), P(), P(), P(), P(), P(), P(), P())
    out_specs = P("dp", "ctx", None)
    return jax.shard_map(
        per_device, mesh=mesh, in_specs=in_specs, out_specs=out_specs, check_vma=False
    )
```

```python
import functools

import jax
import jax.numpy as jnp
from jax import lax
from jax.experimental import pallas as pl
from jax.experimental.pallas import tpu as pltpu
from jax.sharding import PartitionSpec as P

D = 2048
HEADS = 64
HEAD_DIM = 64
STATE = 128
GROUPS = 4
BLOCK = 256
ROWS = 512
HALO = 16
SHARD = 1280
XBC = 5120
INNER = 4096
LOG2E = 1.4426950408889634
MESH = pl.DeviceIdType.MESH
F32 = jnp.float32
BF16 = jnp.bfloat16

RING_COL = ((0, 4, 3, 9), (2, 8, 1, 5))
DIRECT_COL = 6
SAME_SLOT = (10, 12, 14, 16, 18)
OTHER_SLOT = (11, 13, 15, 17, 19)
PEERS = 34


def same_slot(column):
    return 2 * SAME_SLOT[column // 2] + column % 2


def other_slot(column):
    return 2 * OTHER_SLOT[column // 2] + column % 2


def mixer_kernel(
    tok_ref, w_ref, sw_hbm, bias_hbm, rate_hbm, skip_hbm, taps_hbm, fb_hbm,
    out_ref,
    taps_ref, fb_ref, bias_ref, rate_ref, skip_ref,
    tok, wbuf, pbuf, act, swp, small,
    a_ref, bt_ref, lt_ref, w2_ref, e2_ref, misc_ref,
    spread, first, mix, scores, totals, decays_in,
    out_0, out_1, out_2, in_0, in_1, in_2, back_0, back_1, back_2, enter_in,
    near_sem, tok_sem, small_sem, halo_sem, sib_send,
    x_send, x_recv, ring_send, ring_recv, fwd_send, fwd_recv, sems,
):
    dp = lax.axis_index("dp")
    ctx = lax.axis_index("ctx")
    z = ctx % 4
    y = (ctx // 4) % 4
    xh = ctx // 16
    sibling = dp + 1 - 2 * (dp % 2)
    across = (dp + 2) % 4
    place = (z, y)

    def along(dim, step):
        if dim == 0:
            return xh * 16 + y * 4 + (z + step) % 4
        return xh * 16 + ((y + step) % 4) * 4 + z

    source_a = (across, ctx)
    source_b = (across, (ctx + 16) % 32)
    after = (dp, (ctx + 1) % 32)

    low, high = dp % 2, dp // 2

    def own_columns(column):
        pair = column // 2
        block = (
            (1 - low) * pair
            + low * (1 - high) * ((pair + 3) % 5)
            + low * high * (1, 2, 0, 3, 4)[pair]
        )
        return pl.ds(pl.multiple_of(block * 256 + column % 2 * 128, 128), 128)

    def loc_copy(j):
        return pltpu.make_async_copy(w_ref.at[:, own_columns(j)], wbuf.at[j], near_sem.at[j])

    loc_copy(0).start()
    loc_copy(1).start()
    barrier = pltpu.get_barrier_semaphore()
    for peer in ((sibling, ctx), source_a, source_b):
        pl.semaphore_signal(barrier, inc=1, device_id=peer, device_id_type=MESH)

    @pl.loop(1, 32)
    def _(r):
        pl.semaphore_signal(
            barrier, inc=1, device_id=(dp, (ctx + r) % 32), device_id_type=MESH
        )

    tok_copy = pltpu.make_async_copy(tok_ref.at[0], tok.at[HALO:], tok_sem)
    tok_copy.start()
    small_copies = [
        pltpu.make_async_copy(src, dst, small_sem.at[n])
        for n, (src, dst) in enumerate((
            (sw_hbm, swp.at[0:HEADS]), (bias_hbm, bias_ref), (rate_hbm, rate_ref),
            (skip_hbm, skip_ref), (taps_hbm, taps_ref), (fb_hbm, fb_ref),
        ))
    ]
    for copy in small_copies:
        copy.start()
    for j in range(2, 4):
        loc_copy(j).start()

    def remote(src, dst, send, recv, peer):
        return pltpu.make_async_remote_copy(
            src_ref=src, dst_ref=dst, send_sem=send, recv_sem=recv,
            device_id=peer, device_id_type=MESH,
        )

    def x_piece(dim, p):
        column = RING_COL[dim][p]
        rows = pl.ds(pl.multiple_of(place[dim] * 512, 512), 512)
        own = w_ref.at[rows, own_columns(column)] if column > 1 else wbuf.at[column, rows]
        return remote(
            own,
            wbuf.at[same_slot(column), rows],
            x_send.at[dim * 4 + p], x_recv.at[dim * 4 + p],
            source_a if p < 2 else source_b,
        )

    def x_direct(k):
        column = DIRECT_COL + k
        return remote(
            w_ref.at[:, own_columns(column)],
            wbuf.at[same_slot(column)],
            x_send.at[8 + k], x_recv.at[8 + k], (source_a, source_b)[k],
        )

    def ring_rows(dim, kind, p):
        back = (3, 1, 2)[kind]
        return pl.ds(pl.multiple_of(((place[dim] + back) % 4) * 512, 512), 512)

    def ring_out(dim, kind, p):
        column = RING_COL[dim][p]
        rows = pl.ds(pl.multiple_of(place[dim] * 512, 512), 512)
        peer = along(dim, (1, 3, 1 if p < 2 else 3)[kind])
        if kind == 2:
            rows = ring_rows(dim, 0 if p < 2 else 1, p)
        at = wbuf.at[same_slot(column), rows]
        index = dim * 12 + kind * 4 + p
        return remote(at, at, ring_send.at[index], ring_recv.at[index], (dp, peer))

    def ring_in(dim, kind, p):
        column = RING_COL[dim][p]
        at = wbuf.at[same_slot(column), ring_rows(dim, kind, p)]
        index = dim * 12 + kind * 4 + p
        return remote(at, at, ring_send.at[index], ring_recv.at[index], (dp, along(dim, 1)))

    def forward(index):
        if index in (8, 9):
            column = DIRECT_COL + index - 8
            src, dst = wbuf.at[same_slot(column)], wbuf.at[other_slot(column)]
        else:
            if index < 8:
                dim, p = divmod(index, 4)
                rows = pl.ds(pl.multiple_of(place[dim] * 512, 512), 512)
            else:
                dim, rest = divmod(index - 10, 12)
                kind, p = divmod(rest, 4)
                rows = ring_rows(dim, kind, p)
            column = RING_COL[dim][p]
            src = wbuf.at[same_slot(column), rows]
            dst = wbuf.at[other_slot(column), rows]
        return remote(src, dst, fwd_send.at[index], fwd_recv.at[index], (sibling, ctx))

    def sib_copy(j):
        return remote(
            w_ref.at[:, own_columns(j)], wbuf.at[10 + j],
            sib_send.at[j], near_sem.at[10 + j], (sibling, ctx),
        )

    halo_copy = remote(
        tok_ref.at[0, ROWS - HALO :], tok.at[:HALO], halo_sem.at[0], halo_sem.at[1], after
    )

    with jax.named_scope("barrier"):
        pl.semaphore_wait(barrier, PEERS)
    halo_copy.start()
    loc_copy(0).wait()
    loc_copy(1).wait()
    for p, q in ((0, 2), (1, 3)):
        x_piece(0, p).start()
        x_piece(1, q).start()
        x_piece(1, p).start()
        x_piece(0, q).start()
    x_direct(0).start()
    x_direct(1).start()
    for j in range(4, 10):
        loc_copy(j).start()
    for j in range(10):
        sib_copy(j).start()

    swp[HEADS:] = jnp.zeros((128 - HEADS, D), BF16)
    for copy in small_copies:
        copy.wait()
    small[...] = jnp.zeros_like(small)
    small[0:1, 0:HEADS] = bias_ref[...]
    small[1:2, 0:HEADS] = rate_ref[...]
    small[2:3, 0:HEADS] = skip_ref[...]
    with jax.named_scope("tokwait"):
        tok_copy.wait()
    step_raw = lax.dot_general(
        tok[HALO:], swp[...], (((1,), (1,)), ((), ())), preferred_element_type=F32
    )
    step_raw = step_raw.astype(BF16).astype(F32) + small[0:1]
    step = jnp.maximum(step_raw, 0.0) + jnp.log1p(jnp.exp(-jnp.abs(step_raw)))
    keep = lax.broadcasted_iota(jnp.int32, (ROWS, 128), 1) < HEADS
    step = jnp.where(keep, step, 0.0)
    fall = step * (small[1:2] * (-LOG2E))
    lower = (
        lax.broadcasted_iota(jnp.int32, (BLOCK, BLOCK), 0)
        >= lax.broadcasted_iota(jnp.int32, (BLOCK, BLOCK), 1)
    ).astype(F32)
    level = jnp.log2(step)

    def halves(value):
        high = value.astype(BF16).astype(F32)
        low = (value - high).astype(BF16).astype(F32)
        return (high + pltpu.roll(low, 64, 1)).astype(BF16)

    ends = []
    for k in range(2):
        at = slice(k * BLOCK, (k + 1) * BLOCK)
        a = jnp.dot(
            lower, fall[at], precision=lax.Precision.HIGHEST, preferred_element_type=F32
        )
        end = a[BLOCK - 1 : BLOCK]
        ends.append(end)
        weight = jnp.where(keep[at], jnp.exp2(end - a) * step[at], 0.0)
        w2_ref[at] = halves(weight)
        e2_ref[at] = halves(jnp.where(keep[at], jnp.exp2(a), 0.0))
        turned = jnp.transpose(level[at] - a)
        turned_level = jnp.transpose(level[at])
        for g in range(GROUPS):
            a_ref[g, at] = a if g == 0 else pltpu.roll(a, 128 - 16 * g, 1)
            bt_ref[g, :, at] = turned[16 * g : 16 * g + 16]
            lt_ref[g, :, at] = turned_level[16 * g : 16 * g + 16]
    row = lax.broadcasted_iota(jnp.int32, (8, 128), 0)
    lane_ok = lax.broadcasted_iota(jnp.int32, (8, 128), 1) < HEADS
    exponent = jnp.where(row == 0, ends[0], jnp.where(row == 1, ends[1], ends[0] + ends[1]))
    rows_of = jnp.where(row == 3, small[2:3], jnp.exp2(exponent))
    misc_ref[...] = halves(jnp.where(lane_ok, rows_of, 0.0))

    head_row = lax.broadcasted_iota(jnp.int32, (128, 1024), 0) % HEADS
    head_lane = lax.broadcasted_iota(jnp.int32, (128, 1024), 1) // HEAD_DIM
    for g in range(GROUPS):
        spread[g] = (head_row == head_lane + 16 * g).astype(F32).astype(BF16)

    def total_send(r):
        peer = (ctx + r) % 32
        return remote(misc_ref, totals.at[ctx], sems.at[0], sems.at[1], (dp, peer))

    @pl.loop(1, 32)
    def _(r):
        total_send(r).start()

    totals[ctx] = misc_ref[...]

    with jax.named_scope("halowait"):
        halo_copy.wait_recv()

    @pl.when(ctx == 0)
    def _():
        tok[:HALO] = jnp.zeros((HALO, D), BF16)

    def x_arrive(dim, p):
        x_piece(dim, p).wait_recv()
        ring_out(dim, 0, p).start()
        ring_out(dim, 1, p).start()
        forward(dim * 4 + p).start()

    def near_arrive(dim, p):
        for kind in range(2):
            ring_in(dim, kind, p).wait_recv()
            if (kind == 0) == (p < 2):
                ring_out(dim, 2, p).start()
            forward(10 + dim * 12 + kind * 4 + p).start()

    def far_arrive(dim, p):
        ring_in(dim, 2, p).wait_recv()
        forward(10 + dim * 12 + 8 + p).start()

    def direct_arrive(k):
        x_direct(k).wait_recv()
        forward(8 + k).start()

    def other_wait(pieces):
        for dim, p in pieces:
            forward(dim * 4 + p).wait_recv()
            for kind in range(3):
                forward(10 + dim * 12 + kind * 4 + p).wait_recv()

    one = ((0, 0), (1, 2))
    two = ((1, 0), (0, 2))
    three = ((0, 1), (1, 3))
    four = ((1, 1), (0, 3))

    def at(i, step, *actions):
        @pl.when(i == step)
        def _():
            for action, pieces in actions:
                for piece in pieces:
                    action(*piece)

    def other(pieces):
        other_wait(pieces)

    def other_direct(index):
        forward(index).wait_recv()

    def near_events(i):
        @pl.when(i > 0)
        def _():
            for j in (2 * i, 2 * i + 1):
                pltpu.make_async_copy(wbuf.at[j], wbuf.at[j], near_sem.at[j]).wait()

        at(i, 2, (x_arrive, one))
        at(i, 5, (x_arrive, two))
        at(i, 7, (near_arrive, one))
        at(i, 8, (x_arrive, three))
        at(i, 9, (near_arrive, two))

    def early_events(i):
        at(i, 10, (x_arrive, four), (far_arrive, one))
        at(i, 11, (other, ((one,),)))
        at(i, 12, (near_arrive, three), (far_arrive, two))
        at(i, 13, (near_arrive, four), (other, ((two,),)))

    def late_events(i):
        at(i, 14, (far_arrive, three))
        at(i, 15, (direct_arrive, ((0,), (1,))), (other, ((three,),)))
        at(i, 17, (other_direct, ((8,), (9,))))

    def last_events(i):
        at(i, 18, (far_arrive, four))
        at(i, 19, (other, ((four,),)))

    def block_of(i):
        foreign = i // 10
        relation = (1 - foreign) * (i // 5) + foreign * (2 + i % 2)
        pair = (1 - foreign) * (i % 5) + foreign * (i // 2 - 5)
        slow = (low + relation) % 2
        shigh = (high + relation // 2) % 2
        late = pair // 3
        block = (
            (1 - slow) * pair
            + slow * (1 - shigh) * ((pair + 3) % 5)
            + slow * shigh * (late * pair + (1 - late) * ((pair + 1) % 3))
        )
        return (2 * shigh + slow) * 5 + block

    def project(events, i):
        with jax.named_scope("events"):
            events(i)
        with jax.named_scope("compute"):
            block = block_of(i)
            weights = jnp.concatenate([wbuf[2 * i], wbuf[2 * i + 1]], axis=1)
            result = jnp.dot(tok[...], weights, preferred_element_type=F32)
            result = result.astype(BF16).astype(F32)
            for side in range(2):
                pbuf[side] = result[:, side * 128 : side * 128 + 128]
            for side in range(2):
                lanes = pl.ds(pl.multiple_of(block * 256 + side * 128, 128), 128)
                taps = taps_ref[:, lanes]
                bias = fb_ref[:, lanes]
                for row in range(0, ROWS, 64):
                    at = HALO - 3 + row
                    summed = bias + taps[0:1] * pbuf[side, at : at + 64]
                    for k in range(1, 4):
                        summed = summed + taps[k : k + 1] * pbuf[side, at + k : at + k + 64]
                    half = 0.5 * summed
                    act[block, row : row + 64, side * 128 : side * 128 + 128] = (
                        half * jnp.tanh(half) + half
                    ).astype(BF16)


    def widen(value, g):
        return jnp.dot(value, spread[g], preferred_element_type=F32)

    def group_of(g, at):
        return jnp.concatenate([act[4 * g + j, at] for j in range(4)], axis=1)

    def map_lanes(g, at, base):
        return act[base + g // 2, at, pl.ds(pl.multiple_of((g % 2) * 128, 128), 128)]

    state_out, state_in, enter_out = (out_0, out_1, out_2), (in_0, in_1, in_2), (back_0, back_1, back_2)
    parts, begin = (2, 4, 4), (0, 16, 24)

    def group_at(stage, m):
        if stage == 0:
            return (1 - high) * m + high * (3 - m)
        return (1 - high) * (1 + stage) + high * (stage - 1)

    def state_send(peer, stage):
        return remote(
            state_out[stage].at[peer], state_in[stage].at[ctx],
            sems.at[2 + stage], sems.at[5 + stage], (dp, peer),
        )

    def my_place(stage):
        size = STATE // parts[stage]
        rows = pl.ds(pl.multiple_of(ctx % parts[stage] * size, size), size)
        return begin[stage] + ctx // parts[stage], rows

    def enter_send(r, stage):
        peer = (ctx + r) % 32
        pair, rows = my_place(stage)
        return remote(
            enter_out[stage].at[peer], enter_in.at[pair, rows],
            sems.at[8 + stage], sems.at[11 + stage], (dp, peer),
        )

    def wait_all(part, index):
        pltpu.make_async_copy(part, part, sems.at[index]).wait()

    def fan_out(copy_to):
        @pl.loop(0, 6)
        def _(n):
            for q in range(5):
                copy_to(5 * n + q + 1).start()

        copy_to(31).start()

    def states(stage):
        groups = 1 if stage else 2
        owners = 32 // groups
        size = STATE // parts[stage]

        @pl.loop(0, groups)
        @jax.named_scope("states")
        def _(n):
            m = (n + xh) % groups
            g = group_at(stage, m)
            decays = widen(misc_ref[...], g)
            total = None
            for k in range(2):
                at = slice(k * BLOCK, (k + 1) * BLOCK)
                values = group_of(g, at).astype(F32)
                scaled = (widen(w2_ref[at], g) * values).astype(BF16)
                maps = map_lanes(g, at, 16)
                state = lax.dot_general(
                    maps, scaled, (((0,), (0,)), ((), ())), preferred_element_type=F32
                )
                if k == 0:
                    first[g] = state
                    total = decays[1:2] * state
                else:
                    total = total + state
            for i in range(8):
                for part in range(parts[stage]):
                    state_out[stage][owners * m + parts[stage] * i + part] = total[
                        part * size : part * size + size, i * 128 : (i + 1) * 128
                    ].astype(BF16)

            if stage:
                fan_out(lambda r: state_send((ctx + r) % 32, stage))
            else:
                @pl.loop(0, owners)
                def _(j):
                    peer = owners * m + (j + ctx) % owners

                    @pl.when(peer != ctx)
                    def _():
                        state_send(peer, stage).start()

        state_in[stage][ctx] = state_out[stage][ctx]

    pl.loop(0, 10)(functools.partial(project, near_events))
    pl.loop(10, 14)(functools.partial(project, early_events))
    states(0)
    pl.loop(14, 18)(functools.partial(project, late_events))
    states(1)
    pl.loop(18, 20)(functools.partial(project, last_events))
    states(2)

    lane = lax.broadcasted_iota(jnp.int32, (BLOCK, 128), 1) < HEAD_DIM
    causal = lax.broadcasted_iota(jnp.int32, (128, 128), 0) >= lax.broadcasted_iota(
        jnp.int32, (128, 128), 1
    )

    @jax.named_scope("within")
    def within(n):
        g = n // 2
        start = (n % 2) * BLOCK
        rows = pl.ds(pl.multiple_of(start, BLOCK), BLOCK)
        early = pl.ds(pl.multiple_of(start, 128), 128)
        later = pl.ds(pl.multiple_of(start + 128, 128), 128)
        full = lax.dot_general(
            map_lanes(g, rows, 18), map_lanes(g, rows, 16),
            (((1,), (1,)), ((), ())), preferred_element_type=F32,
        )
        scores[0] = jnp.where(causal, full[:128, :128], 0.0)
        scores[1] = full[128:, :128]
        scores[2] = jnp.where(causal, full[128:, 128:], 0.0)
        skip = widen(misc_ref[...], g)[3:4]
        for i in range(8):
            lanes = slice((i % 2) * 128, (i % 2) * 128 + 128)
            values = act[4 * g + i // 2, rows, lanes]
            made = []
            for h in (2 * i, 2 * i + 1):
                upper = a_ref[g, early, h : h + 1]
                under = a_ref[g, later, h : h + 1]
                b0 = bt_ref[g, h : h + 1, early]
                b1 = bt_ref[g, h : h + 1, later]
                l0 = lt_ref[g, h : h + 1, early]
                l1 = lt_ref[g, h : h + 1, later]
                w00 = (jnp.exp2(jnp.minimum(upper + b0, l0)) * scores[0]).astype(BF16)
                w10 = (jnp.exp2(under + b0) * scores[1]).astype(BF16)
                w11 = (jnp.exp2(jnp.minimum(under + b1, l1)) * scores[2]).astype(BF16)
                top = jnp.dot(w00, values[:128], preferred_element_type=F32)
                low = jnp.dot(
                    jnp.concatenate([w10, w11], axis=1), values, preferred_element_type=F32
                )
                made.append(jnp.concatenate([top, low], axis=0))
            mixed = jnp.where(lane, made[0], made[1])
            mix[g, rows, i * 128 : (i + 1) * 128] = (
                mixed + skip[:, i * 128 : (i + 1) * 128] * values.astype(F32)
            )

    def turn(stage):
        pair, rows = my_place(stage)
        pair = pair - begin[stage]
        head = 16 * group_at(stage, pair // 8) + 2 * (pair % 8)
        mine = lax.broadcasted_iota(jnp.int32, (128, 128), 0) % HEADS == (
            head + lax.broadcasted_iota(jnp.int32, (128, 128), 1) // HEAD_DIM
        )
        pick = mine.astype(F32).astype(BF16)
        for k in range(32):
            decays_in[k] = jnp.dot(totals[k], pick, preferred_element_type=F32)
        with jax.named_scope("statewait"):
            wait_all(state_in[stage].at[0:31], 5 + stage)

        def scan(n, carry):
            for k in range(4):
                enter_out[stage][4 * n + k] = carry.astype(BF16)
                here = state_in[stage][4 * n + k].astype(F32)
                carry = decays_in[4 * n + k, 2:3] * carry + here
            return carry

        lax.fori_loop(0, 8, scan, jnp.zeros((STATE // parts[stage], 128), F32))
        fan_out(lambda r: enter_send(r, stage))

        enter_in[begin[stage] + pair, rows] = enter_out[stage][ctx]

    wait_all(totals.at[0:31], 1)
    pl.loop(0, 1)(within)
    turn(0)
    pl.loop(1, 4)(within)
    turn(1)
    pl.loop(4, 5)(within)
    turn(2)
    pl.loop(5, 8)(within)

    for stage in range(3):
        with jax.named_scope("enterwait"):
            wait_all(enter_in.at[0:31, 0 : STATE // parts[stage]], 11 + stage)

        @pl.loop(0, 1 if stage else 2)
        @jax.named_scope("groups")
        def _(m):
            g = group_at(stage, m)
            decays = widen(misc_ref[...], g)[0:1]
            for k in range(2):
                rows = slice(k * BLOCK, (k + 1) * BLOCK)
                read = map_lanes(g, rows, 18)
                for j in range(4):
                    lanes = slice(j * 256, (j + 1) * 256)
                    pair = begin[stage] + 8 * m + 2 * j
                    enter = jnp.concatenate([enter_in[pair], enter_in[pair + 1]], axis=1)
                    if k == 1:
                        enter = decays[:, lanes] * enter.astype(F32) + first[g, :, lanes]
                        enter = enter.astype(BF16)
                    carried = jnp.dot(read, enter, preferred_element_type=F32) * jnp.dot(
                        e2_ref[rows], spread[g, :, lanes], preferred_element_type=F32
                    )
                    columns = pl.ds(pl.multiple_of(g * 1024 + j * 256, 256), 256)
                    out_ref[rows, columns] = (mix[g, rows, lanes] + carried).astype(BF16)

    with jax.named_scope("drain"):
        halo_copy.wait_send()
        for dim in range(2):
            for p in range(4):
                x_piece(dim, p).wait_send()
                for kind in range(3):
                    ring_out(dim, kind, p).wait_send()
        for k in range(2):
            x_direct(k).wait_send()
        for j in range(10):
            sib_copy(j).wait_send()
        for index in range(34):
            forward(index).wait_send()
        wait_all(totals.at[0:31], 0)
        for stage in range(3):
            wait_all(state_in[stage].at[0:31], 2 + stage)
            wait_all(state_in[stage].at[0:31], 8 + stage)


def mixer(tokens, in_weight, step_weight, bias, rate, skip, taps, filter_bias):
    vmem = pl.BlockSpec(memory_space=pltpu.VMEM)
    anywhere = pl.BlockSpec(memory_space=pl.ANY)
    dma = pltpu.SemaphoreType.DMA
    return pl.pallas_call(
        mixer_kernel,
        out_shape=pltpu.VMEM((ROWS, INNER), BF16),
        in_specs=[anywhere] * 8,
        out_specs=vmem,
        scratch_shapes=[
            pltpu.VMEM((4, XBC), F32),
            pltpu.VMEM((1, XBC), F32),
            *[pltpu.VMEM((1, HEADS), F32) for _ in range(3)],
            pltpu.VMEM((HALO + ROWS, D), BF16),
            pltpu.VMEM((40, D, 128), BF16),
            pltpu.VMEM((2, HALO + ROWS, 128), F32),
            pltpu.VMEM((20, ROWS, 256), BF16),
            pltpu.VMEM((128, D), BF16),
            pltpu.VMEM((8, 128), F32),
            pltpu.VMEM((GROUPS, ROWS, 128), F32),
            pltpu.VMEM((GROUPS, 16, ROWS), F32),
            pltpu.VMEM((GROUPS, 16, ROWS), F32),
            pltpu.VMEM((ROWS, 128), BF16),
            pltpu.VMEM((ROWS, 128), BF16),
            pltpu.VMEM((8, 128), BF16),
            pltpu.VMEM((GROUPS, 128, 1024), BF16),
            pltpu.VMEM((GROUPS, STATE, 1024), F32),
            pltpu.VMEM((GROUPS, ROWS, 1024), F32),
            pltpu.VMEM((3, 128, 128), F32),
            pltpu.VMEM((32, 8, 128), BF16),
            pltpu.VMEM((32, 8, 128), F32),
            *[pltpu.VMEM((32, rows, 128), BF16) for rows in (64, 32, 32) * 3],
            pltpu.VMEM((32, STATE, 128), BF16),
            dma((20,)), dma, dma((6,)), dma((2,)), dma((10,)),
            dma((10,)), dma((10,)), dma((24,)), dma((24,)), dma((34,)), dma((34,)), dma((14,)),
        ],
        compiler_params=pltpu.CompilerParams(
            collective_id=0, has_side_effects=True, vmem_limit_bytes=54 * 2**20
        ),
        name="mixer",
    )(tokens, in_weight, step_weight, bias, rate, skip, taps, filter_bias)


def norm_kernel(mixed_ref, gain_ref, out_ref, rows_out, sem):
    tile = 64

    def copy(n):
        rows = slice(n * tile, (n + 1) * tile)
        return pltpu.make_async_copy(rows_out.at[rows], out_ref.at[rows], sem.at[n])

    for n in range(ROWS // tile):
        rows = slice(n * tile, (n + 1) * tile)
        for g in range(GROUPS):
            columns = slice(g * 1024, (g + 1) * 1024)
            mixed = mixed_ref[rows, columns].astype(F32)
            mean = jnp.mean(mixed * mixed, axis=1, keepdims=True)
            normed = mixed * lax.rsqrt(mean + 1e-05) * gain_ref[:, columns]
            rows_out[rows, columns] = normed.astype(BF16)
        copy(n).start()
    for n in range(ROWS // tile):
        copy(n).wait()


def group_norm(mixed, gain):
    vmem = pl.BlockSpec(memory_space=pltpu.VMEM)
    return pl.pallas_call(
        norm_kernel,
        out_shape=jax.ShapeDtypeStruct((ROWS, INNER), BF16),
        in_specs=[vmem, vmem],
        out_specs=pl.BlockSpec(memory_space=pl.ANY),
        scratch_shapes=[pltpu.VMEM((ROWS, INNER), BF16), pltpu.SemaphoreType.DMA((8,))],
        compiler_params=pltpu.CompilerParams(vmem_limit_bytes=24 * 2**20),
        name="group_norm",
    )(mixed, gain)


def per_device(
    tokens,
    in_weight,
    step_weight,
    step_bias,
    decay_rate,
    skip_gain,
    filter_taps,
    filter_bias,
    norm_gain,
):
    mixed = mixer(
        tokens, in_weight, step_weight.T, step_bias[None], decay_rate[None], skip_gain[None],
        filter_taps, filter_bias[None],
    )
    return group_norm(mixed, norm_gain[None])[None]


def solution(mesh):
    in_specs = (P("dp", "ctx", None), P(None, "dp"), P(), P(), P(), P(), P(), P(), P())
    out_specs = P("dp", "ctx", None)
    return jax.shard_map(
        per_device, mesh=mesh, in_specs=in_specs, out_specs=out_specs, check_vma=False
    )
```

```python
import functools

import jax
import jax.numpy as jnp
from jax import lax
from jax.experimental import pallas as pl
from jax.experimental.pallas import tpu as pltpu
from jax.sharding import PartitionSpec as P

D = 2048
HEADS = 64
HEAD_DIM = 64
STATE = 128
GROUPS = 4
BLOCK = 256
ROWS = 512
HALO = 16
SHARD = 1280
XBC = 5120
INNER = 4096
LOG2E = 1.4426950408889634
MESH = pl.DeviceIdType.MESH
F32 = jnp.float32
BF16 = jnp.bfloat16

RING_COL = ((0, 4, 3, 9), (2, 8, 1, 5))
DIRECT_COL = 6
SAME_SLOT = (10, 12, 14, 16, 18)
OTHER_SLOT = (11, 13, 15, 17, 19)
PEERS = 34


def same_slot(column):
    return 2 * SAME_SLOT[column // 2] + column % 2


def other_slot(column):
    return 2 * OTHER_SLOT[column // 2] + column % 2


def mixer_kernel(
    tok_ref, w_ref, sw_hbm, bias_hbm, rate_hbm, skip_hbm, taps_hbm, fb_hbm,
    out_ref,
    taps_ref, fb_ref, bias_ref, rate_ref, skip_ref,
    tok, wbuf, pbuf, act, swp, small,
    a_ref, bt_ref, lt_ref, w2_ref, e2_ref, misc_ref,
    spread, first, mix, scores, totals, decays_in,
    out_0, out_1, out_2, in_0, in_1, in_2, back_0, back_1, back_2, enter_in,
    near_sem, tok_sem, small_sem, halo_sem, sib_send,
    x_send, x_recv, ring_send, ring_recv, fwd_send, fwd_recv, sems,
):
    dp = lax.axis_index("dp")
    ctx = lax.axis_index("ctx")
    z = ctx % 4
    y = (ctx // 4) % 4
    xh = ctx // 16
    sibling = dp + 1 - 2 * (dp % 2)
    across = (dp + 2) % 4
    place = (z, y)

    def along(dim, step):
        if dim == 0:
            return xh * 16 + y * 4 + (z + step) % 4
        return xh * 16 + ((y + step) % 4) * 4 + z

    source_a = (across, ctx)
    source_b = (across, (ctx + 16) % 32)
    after = (dp, (ctx + 1) % 32)

    low, high = dp % 2, dp // 2

    def own_columns(column):
        pair = column // 2
        block = (
            (1 - low) * pair
            + low * (1 - high) * ((pair + 3) % 5)
            + low * high * (1, 2, 0, 3, 4)[pair]
        )
        return pl.ds(pl.multiple_of(block * 256 + column % 2 * 128, 128), 128)

    def loc_copy(j):
        return pltpu.make_async_copy(w_ref.at[:, own_columns(j)], wbuf.at[j], near_sem.at[j])

    loc_copy(0).start()
    loc_copy(1).start()
    barrier = pltpu.get_barrier_semaphore()
    for peer in ((sibling, ctx), source_a, source_b):
        pl.semaphore_signal(barrier, inc=1, device_id=peer, device_id_type=MESH)

    @pl.loop(1, 32)
    def _(r):
        pl.semaphore_signal(
            barrier, inc=1, device_id=(dp, (ctx + r) % 32), device_id_type=MESH
        )

    tok_copy = pltpu.make_async_copy(tok_ref.at[0], tok.at[HALO:], tok_sem)
    tok_copy.start()
    small_copies = [
        pltpu.make_async_copy(src, dst, small_sem.at[n])
        for n, (src, dst) in enumerate((
            (sw_hbm, swp.at[0:HEADS]), (bias_hbm, bias_ref), (rate_hbm, rate_ref),
            (skip_hbm, skip_ref), (taps_hbm, taps_ref), (fb_hbm, fb_ref),
        ))
    ]
    for copy in small_copies:
        copy.start()
    for j in range(2, 4):
        loc_copy(j).start()

    def remote(src, dst, send, recv, peer):
        return pltpu.make_async_remote_copy(
            src_ref=src, dst_ref=dst, send_sem=send, recv_sem=recv,
            device_id=peer, device_id_type=MESH,
        )

    def x_piece(dim, p):
        column = RING_COL[dim][p]
        rows = pl.ds(pl.multiple_of(place[dim] * 512, 512), 512)
        own = w_ref.at[rows, own_columns(column)] if column > 1 else wbuf.at[column, rows]
        return remote(
            own,
            wbuf.at[same_slot(column), rows],
            x_send.at[dim * 4 + p], x_recv.at[dim * 4 + p],
            source_a if p < 2 else source_b,
        )

    def x_direct(k):
        column = DIRECT_COL + k
        return remote(
            w_ref.at[:, own_columns(column)],
            wbuf.at[same_slot(column)],
            x_send.at[8 + k], x_recv.at[8 + k], (source_a, source_b)[k],
        )

    def ring_rows(dim, kind, p):
        back = (3, 1, 2)[kind]
        return pl.ds(pl.multiple_of(((place[dim] + back) % 4) * 512, 512), 512)

    def ring_out(dim, kind, p):
        column = RING_COL[dim][p]
        rows = pl.ds(pl.multiple_of(place[dim] * 512, 512), 512)
        peer = along(dim, (1, 3, 1 if p < 2 else 3)[kind])
        if kind == 2:
            rows = ring_rows(dim, 0 if p < 2 else 1, p)
        at = wbuf.at[same_slot(column), rows]
        index = dim * 12 + kind * 4 + p
        return remote(at, at, ring_send.at[index], ring_recv.at[index], (dp, peer))

    def ring_in(dim, kind, p):
        column = RING_COL[dim][p]
        at = wbuf.at[same_slot(column), ring_rows(dim, kind, p)]
        index = dim * 12 + kind * 4 + p
        return remote(at, at, ring_send.at[index], ring_recv.at[index], (dp, along(dim, 1)))

    def forward(index):
        if index in (8, 9):
            column = DIRECT_COL + index - 8
            src, dst = wbuf.at[same_slot(column)], wbuf.at[other_slot(column)]
        else:
            if index < 8:
                dim, p = divmod(index, 4)
                rows = pl.ds(pl.multiple_of(place[dim] * 512, 512), 512)
            else:
                dim, rest = divmod(index - 10, 12)
                kind, p = divmod(rest, 4)
                rows = ring_rows(dim, kind, p)
            column = RING_COL[dim][p]
            src = wbuf.at[same_slot(column), rows]
            dst = wbuf.at[other_slot(column), rows]
        return remote(src, dst, fwd_send.at[index], fwd_recv.at[index], (sibling, ctx))

    def sib_copy(j):
        return remote(
            w_ref.at[:, own_columns(j)], wbuf.at[10 + j],
            sib_send.at[j], near_sem.at[10 + j], (sibling, ctx),
        )

    halo_copy = remote(
        tok_ref.at[0, ROWS - HALO :], tok.at[:HALO], halo_sem.at[0], halo_sem.at[1], after
    )

    with jax.named_scope("barrier"):
        pl.semaphore_wait(barrier, PEERS)
    halo_copy.start()
    loc_copy(0).wait()
    loc_copy(1).wait()
    for p, q in ((0, 2), (1, 3)):
        x_piece(0, p).start()
        x_piece(1, q).start()
        x_piece(1, p).start()
        x_piece(0, q).start()
    x_direct(0).start()
    x_direct(1).start()
    for j in range(4, 10):
        loc_copy(j).start()
    for j in range(10):
        sib_copy(j).start()

    swp[HEADS:] = jnp.zeros((128 - HEADS, D), BF16)
    for copy in small_copies:
        copy.wait()
    small[...] = jnp.zeros_like(small)
    small[0:1, 0:HEADS] = bias_ref[...]
    small[1:2, 0:HEADS] = rate_ref[...]
    small[2:3, 0:HEADS] = skip_ref[...]
    with jax.named_scope("tokwait"):
        tok_copy.wait()
    step_raw = lax.dot_general(
        tok[HALO:], swp[...], (((1,), (1,)), ((), ())), preferred_element_type=F32
    )
    step_raw = step_raw.astype(BF16).astype(F32) + small[0:1]
    step = jnp.maximum(step_raw, 0.0) + jnp.log1p(jnp.exp(-jnp.abs(step_raw)))
    keep = lax.broadcasted_iota(jnp.int32, (ROWS, 128), 1) < HEADS
    step = jnp.where(keep, step, 0.0)
    fall = step * (small[1:2] * (-LOG2E))
    lower = (
        lax.broadcasted_iota(jnp.int32, (BLOCK, BLOCK), 0)
        >= lax.broadcasted_iota(jnp.int32, (BLOCK, BLOCK), 1)
    ).astype(F32)
    level = jnp.log2(step)

    def halves(value):
        high = value.astype(BF16).astype(F32)
        low = (value - high).astype(BF16).astype(F32)
        return (high + pltpu.roll(low, 64, 1)).astype(BF16)

    ends = []
    for k in range(2):
        at = slice(k * BLOCK, (k + 1) * BLOCK)
        a = jnp.dot(
            lower, fall[at], precision=lax.Precision.HIGHEST, preferred_element_type=F32
        )
        end = a[BLOCK - 1 : BLOCK]
        ends.append(end)
        weight = jnp.where(keep[at], jnp.exp2(end - a) * step[at], 0.0)
        w2_ref[at] = halves(weight)
        e2_ref[at] = halves(jnp.where(keep[at], jnp.exp2(a), 0.0))
        turned = jnp.transpose(level[at] - a)
        turned_level = jnp.transpose(level[at])
        for g in range(GROUPS):
            a_ref[g, at] = a if g == 0 else pltpu.roll(a, 128 - 16 * g, 1)
            bt_ref[g, :, at] = turned[16 * g : 16 * g + 16]
            lt_ref[g, :, at] = turned_level[16 * g : 16 * g + 16]
    row = lax.broadcasted_iota(jnp.int32, (8, 128), 0)
    lane_ok = lax.broadcasted_iota(jnp.int32, (8, 128), 1) < HEADS
    exponent = jnp.where(row == 0, ends[0], jnp.where(row == 1, ends[1], ends[0] + ends[1]))
    rows_of = jnp.where(row == 3, small[2:3], jnp.exp2(exponent))
    misc_ref[...] = halves(jnp.where(lane_ok, rows_of, 0.0))

    head_row = lax.broadcasted_iota(jnp.int32, (128, 1024), 0) % HEADS
    head_lane = lax.broadcasted_iota(jnp.int32, (128, 1024), 1) // HEAD_DIM
    for g in range(GROUPS):
        spread[g] = (head_row == head_lane + 16 * g).astype(F32).astype(BF16)

    def total_send(r):
        peer = (ctx + r) % 32
        return remote(misc_ref, totals.at[ctx], sems.at[0], sems.at[1], (dp, peer))

    @pl.loop(1, 32)
    def _(r):
        total_send(r).start()

    totals[ctx] = misc_ref[...]

    with jax.named_scope("halowait"):
        halo_copy.wait_recv()

    @pl.when(ctx == 0)
    def _():
        tok[:HALO] = jnp.zeros((HALO, D), BF16)

    def x_arrive(dim, p):
        x_piece(dim, p).wait_recv()
        ring_out(dim, 0, p).start()
        ring_out(dim, 1, p).start()
        forward(dim * 4 + p).start()

    def near_arrive(dim, p):
        for kind in range(2):
            ring_in(dim, kind, p).wait_recv()
            if (kind == 0) == (p < 2):
                ring_out(dim, 2, p).start()
            forward(10 + dim * 12 + kind * 4 + p).start()

    def far_arrive(dim, p):
        ring_in(dim, 2, p).wait_recv()
        forward(10 + dim * 12 + 8 + p).start()

    def direct_arrive(k):
        x_direct(k).wait_recv()
        forward(8 + k).start()

    def other_wait(pieces):
        for dim, p in pieces:
            forward(dim * 4 + p).wait_recv()
            for kind in range(3):
                forward(10 + dim * 12 + kind * 4 + p).wait_recv()

    one = ((0, 0), (1, 2))
    two = ((1, 0), (0, 2))
    three = ((0, 1), (1, 3))
    four = ((1, 1), (0, 3))

    def at(i, step, *actions):
        @pl.when(i == step)
        def _():
            for action, pieces in actions:
                for piece in pieces:
                    action(*piece)

    def other(pieces):
        other_wait(pieces)

    def other_direct(index):
        forward(index).wait_recv()

    def near_events(i):
        @pl.when(i > 0)
        def _():
            for j in (2 * i, 2 * i + 1):
                pltpu.make_async_copy(wbuf.at[j], wbuf.at[j], near_sem.at[j]).wait()

        at(i, 2, (x_arrive, one))
        at(i, 5, (x_arrive, two))
        at(i, 7, (near_arrive, one))
        at(i, 8, (x_arrive, three))
        at(i, 9, (near_arrive, two))

    def early_events(i):
        at(i, 10, (x_arrive, four), (far_arrive, one))
        at(i, 11, (other, ((one,),)))
        at(i, 12, (near_arrive, three), (far_arrive, two))
        at(i, 13, (near_arrive, four), (other, ((two,),)))

    def late_events(i):
        at(i, 14, (far_arrive, three))
        at(i, 15, (direct_arrive, ((0,), (1,))), (other, ((three,),)))
        at(i, 17, (other_direct, ((8,), (9,))))

    def last_events(i):
        at(i, 18, (far_arrive, four))
        at(i, 19, (other, ((four,),)))

    def block_of(i):
        foreign = i // 10
        relation = (1 - foreign) * (i // 5) + foreign * (2 + i % 2)
        pair = (1 - foreign) * (i % 5) + foreign * (i // 2 - 5)
        slow = (low + relation) % 2
        shigh = (high + relation // 2) % 2
        late = pair // 3
        block = (
            (1 - slow) * pair
            + slow * (1 - shigh) * ((pair + 3) % 5)
            + slow * shigh * (late * pair + (1 - late) * ((pair + 1) % 3))
        )
        return (2 * shigh + slow) * 5 + block

    def project(events, i):
        with jax.named_scope("events"):
            events(i)
        with jax.named_scope("compute"):
            block = block_of(i)
            weights = jnp.concatenate([wbuf[2 * i], wbuf[2 * i + 1]], axis=1)
            result = jnp.dot(tok[...], weights, preferred_element_type=F32)
            result = result.astype(BF16).astype(F32)
            for side in range(2):
                pbuf[side] = result[:, side * 128 : side * 128 + 128]
            for side in range(2):
                lanes = pl.ds(pl.multiple_of(block * 256 + side * 128, 128), 128)
                taps = taps_ref[:, lanes]
                bias = fb_ref[:, lanes]
                for row in range(0, ROWS, 64):
                    at = HALO - 3 + row
                    summed = bias + taps[0:1] * pbuf[side, at : at + 64]
                    for k in range(1, 4):
                        summed = summed + taps[k : k + 1] * pbuf[side, at + k : at + k + 64]
                    half = 0.5 * summed
                    act[block, row : row + 64, side * 128 : side * 128 + 128] = (
                        half * jnp.tanh(half) + half
                    ).astype(BF16)


    def widen(value, g):
        return jnp.dot(value, spread[g], preferred_element_type=F32)

    def group_of(g, at):
        return jnp.concatenate([act[4 * g + j, at] for j in range(4)], axis=1)

    def map_lanes(g, at, base):
        return act[base + g // 2, at, pl.ds(pl.multiple_of((g % 2) * 128, 128), 128)]

    state_out, state_in, enter_out = (out_0, out_1, out_2), (in_0, in_1, in_2), (back_0, back_1, back_2)
    parts, begin = (2, 4, 4), (0, 16, 24)

    def group_at(stage, m):
        if stage == 0:
            return (1 - high) * m + high * (3 - m)
        return (1 - high) * (1 + stage) + high * (stage - 1)

    def state_send(peer, stage):
        return remote(
            state_out[stage].at[peer], state_in[stage].at[ctx],
            sems.at[2 + stage], sems.at[5 + stage], (dp, peer),
        )

    def my_place(stage):
        size = STATE // parts[stage]
        rows = pl.ds(pl.multiple_of(ctx % parts[stage] * size, size), size)
        return begin[stage] + ctx // parts[stage], rows

    def enter_send(r, stage):
        peer = (ctx + r) % 32
        pair, rows = my_place(stage)
        return remote(
            enter_out[stage].at[peer], enter_in.at[pair, rows],
            sems.at[8 + stage], sems.at[11 + stage], (dp, peer),
        )

    def wait_all(part, index):
        pltpu.make_async_copy(part, part, sems.at[index]).wait()

    def fan_out(copy_to):
        @pl.loop(0, 6)
        def _(n):
            for q in range(5):
                copy_to(5 * n + q + 1).start()

        copy_to(31).start()

    def states(stage):
        groups = 1 if stage else 2
        owners = 32 // groups
        size = STATE // parts[stage]

        @pl.loop(0, groups)
        @jax.named_scope("states")
        def _(n):
            m = (n + xh) % groups
            g = group_at(stage, m)
            decays = widen(misc_ref[...], g)
            total = None
            for k in range(2):
                at = slice(k * BLOCK, (k + 1) * BLOCK)
                values = group_of(g, at).astype(F32)
                scaled = (widen(w2_ref[at], g) * values).astype(BF16)
                maps = map_lanes(g, at, 16)
                state = lax.dot_general(
                    maps, scaled, (((0,), (0,)), ((), ())), preferred_element_type=F32
                )
                if k == 0:
                    first[g] = state
                    total = decays[1:2] * state
                else:
                    total = total + state
            for i in range(8):
                for part in range(parts[stage]):
                    state_out[stage][owners * m + parts[stage] * i + part] = total[
                        part * size : part * size + size, i * 128 : (i + 1) * 128
                    ].astype(BF16)

            if stage:
                fan_out(lambda r: state_send((ctx + r) % 32, stage))
            else:
                @pl.when(n == 0)
                def _():
                    @pl.loop(0, 3)
                    def _(b):
                        for q in range(5):
                            state_send(16 * m + (ctx + 5 * b + q + 1) % 16, stage).start()

                @pl.when(n == 1)
                def _():
                    @pl.loop(0, 4)
                    def _(b):
                        for q in range(4):
                            state_send(16 * m + (ctx + 4 * b + q) % 16, stage).start()

        state_in[stage][ctx] = state_out[stage][ctx]

    pl.loop(0, 10)(functools.partial(project, near_events))
    pl.loop(10, 14)(functools.partial(project, early_events))
    states(0)
    pl.loop(14, 18)(functools.partial(project, late_events))
    states(1)
    pl.loop(18, 20)(functools.partial(project, last_events))
    states(2)

    lane = lax.broadcasted_iota(jnp.int32, (BLOCK, 128), 1) < HEAD_DIM
    causal = lax.broadcasted_iota(jnp.int32, (128, 128), 0) >= lax.broadcasted_iota(
        jnp.int32, (128, 128), 1
    )

    @jax.named_scope("within")
    def within(n):
        g = n // 2
        start = (n % 2) * BLOCK
        rows = pl.ds(pl.multiple_of(start, BLOCK), BLOCK)
        early = pl.ds(pl.multiple_of(start, 128), 128)
        later = pl.ds(pl.multiple_of(start + 128, 128), 128)
        full = lax.dot_general(
            map_lanes(g, rows, 18), map_lanes(g, rows, 16),
            (((1,), (1,)), ((), ())), preferred_element_type=F32,
        )
        scores[0] = jnp.where(causal, full[:128, :128], 0.0)
        scores[1] = full[128:, :128]
        scores[2] = jnp.where(causal, full[128:, 128:], 0.0)
        skip = widen(misc_ref[...], g)[3:4]
        for i in range(8):
            lanes = slice((i % 2) * 128, (i % 2) * 128 + 128)
            values = act[4 * g + i // 2, rows, lanes]
            made = []
            for h in (2 * i, 2 * i + 1):
                upper = a_ref[g, early, h : h + 1]
                under = a_ref[g, later, h : h + 1]
                b0 = bt_ref[g, h : h + 1, early]
                b1 = bt_ref[g, h : h + 1, later]
                l0 = lt_ref[g, h : h + 1, early]
                l1 = lt_ref[g, h : h + 1, later]
                w00 = (jnp.exp2(jnp.minimum(upper + b0, l0)) * scores[0]).astype(BF16)
                w10 = (jnp.exp2(under + b0) * scores[1]).astype(BF16)
                w11 = (jnp.exp2(jnp.minimum(under + b1, l1)) * scores[2]).astype(BF16)
                top = jnp.dot(w00, values[:128], preferred_element_type=F32)
                low = jnp.dot(
                    jnp.concatenate([w10, w11], axis=1), values, preferred_element_type=F32
                )
                made.append(jnp.concatenate([top, low], axis=0))
            mixed = jnp.where(lane, made[0], made[1])
            mix[g, rows, i * 128 : (i + 1) * 128] = (
                mixed + skip[:, i * 128 : (i + 1) * 128] * values.astype(F32)
            )

    def turn(stage):
        pair, rows = my_place(stage)
        pair = pair - begin[stage]
        head = 16 * group_at(stage, pair // 8) + 2 * (pair % 8)
        mine = lax.broadcasted_iota(jnp.int32, (128, 128), 0) % HEADS == (
            head + lax.broadcasted_iota(jnp.int32, (128, 128), 1) // HEAD_DIM
        )
        pick = mine.astype(F32).astype(BF16)
        for k in range(32):
            decays_in[k] = jnp.dot(totals[k], pick, preferred_element_type=F32)
        with jax.named_scope("statewait"):
            wait_all(state_in[stage].at[0:31], 5 + stage)

        def scan(n, carry):
            for k in range(4):
                enter_out[stage][4 * n + k] = carry.astype(BF16)
                here = state_in[stage][4 * n + k].astype(F32)
                carry = decays_in[4 * n + k, 2:3] * carry + here
            return carry

        lax.fori_loop(0, 8, scan, jnp.zeros((STATE // parts[stage], 128), F32))
        fan_out(lambda r: enter_send(r, stage))

        enter_in[begin[stage] + pair, rows] = enter_out[stage][ctx]

    wait_all(totals.at[0:31], 1)
    pl.loop(0, 1)(within)
    turn(0)
    pl.loop(1, 4)(within)
    turn(1)
    pl.loop(4, 5)(within)
    turn(2)
    pl.loop(5, 8)(within)

    for stage in range(3):
        with jax.named_scope("enterwait"):
            wait_all(enter_in.at[0:31, 0 : STATE // parts[stage]], 11 + stage)

        @pl.loop(0, 1 if stage else 2)
        @jax.named_scope("groups")
        def _(m):
            g = group_at(stage, m)
            decays = widen(misc_ref[...], g)[0:1]
            for k in range(2):
                rows = slice(k * BLOCK, (k + 1) * BLOCK)
                read = map_lanes(g, rows, 18)
                for j in range(4):
                    lanes = slice(j * 256, (j + 1) * 256)
                    pair = begin[stage] + 8 * m + 2 * j
                    enter = jnp.concatenate([enter_in[pair], enter_in[pair + 1]], axis=1)
                    if k == 1:
                        enter = decays[:, lanes] * enter.astype(F32) + first[g, :, lanes]
                        enter = enter.astype(BF16)
                    carried = jnp.dot(read, enter, preferred_element_type=F32) * jnp.dot(
                        e2_ref[rows], spread[g, :, lanes], preferred_element_type=F32
                    )
                    columns = pl.ds(pl.multiple_of(g * 1024 + j * 256, 256), 256)
                    out_ref[rows, columns] = (mix[g, rows, lanes] + carried).astype(BF16)

    with jax.named_scope("drain"):
        halo_copy.wait_send()
        for dim in range(2):
            for p in range(4):
                x_piece(dim, p).wait_send()
                for kind in range(3):
                    ring_out(dim, kind, p).wait_send()
        for k in range(2):
            x_direct(k).wait_send()
        for j in range(10):
            sib_copy(j).wait_send()
        for index in range(34):
            forward(index).wait_send()
        wait_all(totals.at[0:31], 0)
        for stage in range(3):
            wait_all(state_in[stage].at[0:31], 2 + stage)
            wait_all(state_in[stage].at[0:31], 8 + stage)


def mixer(tokens, in_weight, step_weight, bias, rate, skip, taps, filter_bias):
    vmem = pl.BlockSpec(memory_space=pltpu.VMEM)
    anywhere = pl.BlockSpec(memory_space=pl.ANY)
    dma = pltpu.SemaphoreType.DMA
    return pl.pallas_call(
        mixer_kernel,
        out_shape=pltpu.VMEM((ROWS, INNER), BF16),
        in_specs=[anywhere] * 8,
        out_specs=vmem,
        scratch_shapes=[
            pltpu.VMEM((4, XBC), F32),
            pltpu.VMEM((1, XBC), F32),
            *[pltpu.VMEM((1, HEADS), F32) for _ in range(3)],
            pltpu.VMEM((HALO + ROWS, D), BF16),
            pltpu.VMEM((40, D, 128), BF16),
            pltpu.VMEM((2, HALO + ROWS, 128), F32),
            pltpu.VMEM((20, ROWS, 256), BF16),
            pltpu.VMEM((128, D), BF16),
            pltpu.VMEM((8, 128), F32),
            pltpu.VMEM((GROUPS, ROWS, 128), F32),
            pltpu.VMEM((GROUPS, 16, ROWS), F32),
            pltpu.VMEM((GROUPS, 16, ROWS), F32),
            pltpu.VMEM((ROWS, 128), BF16),
            pltpu.VMEM((ROWS, 128), BF16),
            pltpu.VMEM((8, 128), BF16),
            pltpu.VMEM((GROUPS, 128, 1024), BF16),
            pltpu.VMEM((GROUPS, STATE, 1024), F32),
            pltpu.VMEM((GROUPS, ROWS, 1024), F32),
            pltpu.VMEM((3, 128, 128), F32),
            pltpu.VMEM((32, 8, 128), BF16),
            pltpu.VMEM((32, 8, 128), F32),
            *[pltpu.VMEM((32, rows, 128), BF16) for rows in (64, 32, 32) * 3],
            pltpu.VMEM((32, STATE, 128), BF16),
            dma((20,)), dma, dma((6,)), dma((2,)), dma((10,)),
            dma((10,)), dma((10,)), dma((24,)), dma((24,)), dma((34,)), dma((34,)), dma((14,)),
        ],
        compiler_params=pltpu.CompilerParams(
            collective_id=0, has_side_effects=True, vmem_limit_bytes=54 * 2**20
        ),
        name="mixer",
    )(tokens, in_weight, step_weight, bias, rate, skip, taps, filter_bias)


def norm_kernel(mixed_ref, gain_ref, out_ref, rows_out, sem):
    tile = 64

    def copy(n):
        rows = slice(n * tile, (n + 1) * tile)
        return pltpu.make_async_copy(rows_out.at[rows], out_ref.at[rows], sem.at[n])

    for n in range(ROWS // tile):
        rows = slice(n * tile, (n + 1) * tile)
        for g in range(GROUPS):
            columns = slice(g * 1024, (g + 1) * 1024)
            mixed = mixed_ref[rows, columns].astype(F32)
            mean = jnp.mean(mixed * mixed, axis=1, keepdims=True)
            normed = mixed * lax.rsqrt(mean + 1e-05) * gain_ref[:, columns]
            rows_out[rows, columns] = normed.astype(BF16)
        copy(n).start()
    for n in range(ROWS // tile):
        copy(n).wait()


def group_norm(mixed, gain):
    vmem = pl.BlockSpec(memory_space=pltpu.VMEM)
    return pl.pallas_call(
        norm_kernel,
        out_shape=jax.ShapeDtypeStruct((ROWS, INNER), BF16),
        in_specs=[vmem, vmem],
        out_specs=pl.BlockSpec(memory_space=pl.ANY),
        scratch_shapes=[pltpu.VMEM((ROWS, INNER), BF16), pltpu.SemaphoreType.DMA((8,))],
        compiler_params=pltpu.CompilerParams(vmem_limit_bytes=24 * 2**20),
        name="group_norm",
    )(mixed, gain)


def per_device(
    tokens,
    in_weight,
    step_weight,
    step_bias,
    decay_rate,
    skip_gain,
    filter_taps,
    filter_bias,
    norm_gain,
):
    mixed = mixer(
        tokens, in_weight, step_weight.T, step_bias[None], decay_rate[None], skip_gain[None],
        filter_taps, filter_bias[None],
    )
    return group_norm(mixed, norm_gain[None])[None]


def solution(mesh):
    in_specs = (P("dp", "ctx", None), P(None, "dp"), P(), P(), P(), P(), P(), P(), P())
    out_specs = P("dp", "ctx", None)
    return jax.shard_map(
        per_device, mesh=mesh, in_specs=in_specs, out_specs=out_specs, check_vma=False
    )
```
